8 devices in a mesh: dp: 1 (over z), dim: 2 (over y), heads: 4 (over x, core).
Axes of the slice: x: 2, y: 2, z: 1, core: 2. Of those that a mesh axis runs over, the one named last changes fastest.
Arguments:
- tokens: bfloat16 [128, 5120], P('dp')
- ln_attn: float32 [5120], replicated
- w_query: bfloat16 [5120, 64, 128], P(None, 'heads', 'dim')
- w_key: bfloat16 [5120, 8, 128], P(None, 'heads', 'dim')
- w_value: bfloat16 [5120, 8, 128], P(None, 'heads', 'dim')
- q_gain: float32 [128], P('dim')
- k_gain: float32 [128], P('dim')
- w_out: bfloat16 [64, 128, 5120], P('heads', 'dim')
- ln_mlp: float32 [5120], replicated
- w_gate: bfloat16 [5120, 25600], P(None, ('heads', 'dim'))
- w_up: bfloat16 [5120, 25600], P(None, ('heads', 'dim'))
- w_down: bfloat16 [25600, 5120], P(('heads', 'dim'))
- k_cache: bfloat16 [128, 1024, 8, 128], P('dp', None, 'heads', 'dim')
- v_cache: bfloat16 [128, 1024, 8, 128], P('dp', None, 'heads', 'dim')
- positions: int32 [128], P('dp')
Outputs:
- output 1: bfloat16 [128, 5120], P('dp')
- output 2: bfloat16 [128, 8, 128], P('dp', 'heads', 'dim')
- output 3: bfloat16 [128, 8, 128], P('dp', 'heads', 'dim')
All inputs are finite; a program needn't handle non-finite values.
Results may differ from the reference program's by a relative error of at most 0.00674652.
Values sent between devices are 32-bit elements.
A program may use at most 1 GiB of HBM per device.

```python
import jax
import jax.numpy as jnp
from jax import lax

BATCH_SEQS = 128
CACHE_LEN = 1024
D_MODEL = 5120
N_HEADS = 64
KV_HEADS = 8
HEAD_DIM = 128
FFN_DIM = 25600
EPS = 1e-6
ROPE_BASE = 1000000.0


def weight_draw(key, shape, fan_in):
    return (jax.random.normal(key, shape, jnp.float32) * fan_in ** -0.5).astype(jnp.bfloat16)


def setup_inputs(seed: int = 0, part: int = 0) -> dict:
    base_key = jax.random.key(seed)
    shared_keys = jax.random.split(base_key, 11)
    part_keys = jax.random.split(jax.random.fold_in(base_key, part), 4)
    positions = jax.random.randint(part_keys[3], (BATCH_SEQS,), CACHE_LEN // 2, CACHE_LEN, dtype=jnp.int32)
    positions = positions.at[0].set(CACHE_LEN - 1).at[1].set(CACHE_LEN // 2)
    return {
        'tokens': jax.random.normal(part_keys[0], (BATCH_SEQS, D_MODEL), jnp.float32).astype(jnp.bfloat16),
        'ln_attn': 1.0 + 0.2 * jax.random.normal(shared_keys[0], (D_MODEL,), jnp.float32),
        'w_query': weight_draw(shared_keys[1], (D_MODEL, N_HEADS, HEAD_DIM), D_MODEL),
        'w_key': weight_draw(shared_keys[2], (D_MODEL, KV_HEADS, HEAD_DIM), D_MODEL),
        'w_value': weight_draw(shared_keys[3], (D_MODEL, KV_HEADS, HEAD_DIM), D_MODEL),
        'q_gain': 2.0 + 0.4 * jax.random.normal(shared_keys[4], (HEAD_DIM,), jnp.float32),
        'k_gain': 1.5 + 0.3 * jax.random.normal(shared_keys[5], (HEAD_DIM,), jnp.float32),
        'w_out': weight_draw(shared_keys[6], (N_HEADS, HEAD_DIM, D_MODEL), N_HEADS * HEAD_DIM),
        'ln_mlp': 1.0 + 0.2 * jax.random.normal(shared_keys[7], (D_MODEL,), jnp.float32),
        'w_gate': weight_draw(shared_keys[8], (D_MODEL, FFN_DIM), D_MODEL),
        'w_up': weight_draw(shared_keys[9], (D_MODEL, FFN_DIM), D_MODEL),
        'w_down': weight_draw(shared_keys[10], (FFN_DIM, D_MODEL), FFN_DIM),
        'k_cache': (1.5 * jax.random.normal(part_keys[1], (BATCH_SEQS, CACHE_LEN, KV_HEADS, HEAD_DIM), jnp.float32)).astype(jnp.bfloat16),
        'v_cache': jax.random.normal(part_keys[2], (BATCH_SEQS, CACHE_LEN, KV_HEADS, HEAD_DIM), jnp.float32).astype(jnp.bfloat16),
        'positions': positions,
    }


def rms_scale(values, gain):
    mean_sq = jnp.mean(values * values, axis=-1, keepdims=True)
    return values * lax.rsqrt(mean_sq + EPS) * gain


def rope_tables(positions):
    half_dim = HEAD_DIM // 2
    inv_freq = ROPE_BASE ** (-jnp.arange(half_dim, dtype=jnp.float32) * 2.0 / HEAD_DIM)
    rot_angle = positions.astype(jnp.float32)[:, None] * inv_freq[None, :]
    cos_t = jnp.cos(rot_angle)
    sin_t = jnp.sin(rot_angle)
    return jnp.concatenate([cos_t, cos_t], axis=-1)[:, None, :], jnp.concatenate([sin_t, sin_t], axis=-1)[:, None, :]


def rotate_half(values, cos_t, sin_t):
    half_dim = HEAD_DIM // 2
    swapped = jnp.concatenate([-values[..., half_dim:], values[..., :half_dim]], axis=-1)
    return values * cos_t + swapped * sin_t


def attend_one(row_args):
    q_row, k_row, v_row, k_rows, v_rows, position = row_args
    keys_all = lax.dynamic_update_slice_in_dim(k_rows, k_row[None], position, axis=0)
    values_all = lax.dynamic_update_slice_in_dim(v_rows, v_row[None], position, axis=0)
    scores = jnp.einsum('kgd,tkd->kgt', q_row.astype(jnp.float32), keys_all.astype(jnp.float32)) * HEAD_DIM ** -0.5
    slot_ids = jnp.arange(CACHE_LEN)
    scores = jnp.where((slot_ids <= position)[None, None, :], scores, -jnp.inf)
    exp_scores = jnp.exp(scores - jnp.max(scores, axis=-1, keepdims=True))
    attn_prob = (exp_scores / jnp.sum(exp_scores, axis=-1, keepdims=True)).astype(jnp.bfloat16)
    return jnp.einsum('kgt,tkd->kgd', attn_prob.astype(jnp.float32), values_all.astype(jnp.float32)).astype(jnp.bfloat16)


def reference(tokens, ln_attn, w_query, w_key, w_value, q_gain, k_gain, w_out, ln_mlp, w_gate, w_up, w_down, k_cache, v_cache, positions):
    q_group = N_HEADS // KV_HEADS
    tok_f32 = tokens.astype(jnp.float32)
    hidden = rms_scale(tok_f32, ln_attn).astype(jnp.bfloat16)
    q_proj = jnp.dot(hidden, w_query.reshape(D_MODEL, N_HEADS * HEAD_DIM), preferred_element_type=jnp.float32).reshape(BATCH_SEQS, N_HEADS, HEAD_DIM)
    k_proj = jnp.dot(hidden, w_key.reshape(D_MODEL, KV_HEADS * HEAD_DIM), preferred_element_type=jnp.float32).reshape(BATCH_SEQS, KV_HEADS, HEAD_DIM)
    v_new = jnp.dot(hidden, w_value.reshape(D_MODEL, KV_HEADS * HEAD_DIM), preferred_element_type=jnp.float32).reshape(BATCH_SEQS, KV_HEADS, HEAD_DIM).astype(jnp.bfloat16)
    cos_t, sin_t = rope_tables(positions)
    q_rot = rotate_half(rms_scale(q_proj, q_gain), cos_t, sin_t).astype(jnp.bfloat16)
    k_new = rotate_half(rms_scale(k_proj, k_gain), cos_t, sin_t).astype(jnp.bfloat16)
    q_grouped = q_rot.reshape(BATCH_SEQS, KV_HEADS, q_group, HEAD_DIM)
    attn_vals = lax.map(attend_one, (q_grouped, k_new, v_new, k_cache, v_cache, positions))
    attn_flat = attn_vals.reshape(BATCH_SEQS, N_HEADS * HEAD_DIM)
    attn_out = jnp.dot(attn_flat, w_out.reshape(N_HEADS * HEAD_DIM, D_MODEL), preferred_element_type=jnp.float32)
    resid_f32 = (tok_f32 + attn_out).astype(jnp.bfloat16).astype(jnp.float32)
    hidden2 = rms_scale(resid_f32, ln_mlp).astype(jnp.bfloat16)
    gate_val = jnp.dot(hidden2, w_gate, preferred_element_type=jnp.float32)
    up_val = jnp.dot(hidden2, w_up, preferred_element_type=jnp.float32)
    mlp_act = (jax.nn.silu(gate_val) * up_val).astype(jnp.bfloat16)
    mlp_out = jnp.dot(mlp_act, w_down, preferred_element_type=jnp.float32)
    return (resid_f32 + mlp_out).astype(jnp.bfloat16), k_new, v_new
```

```python
import functools

import jax
import jax.numpy as jnp
from jax import lax
from jax.experimental import pallas as pl
from jax.experimental.pallas import tpu as pltpu
from jax.sharding import PartitionSpec as P

EPS = 1e-6
ROPE_BASE = 1000000.0
MESH = pl.DeviceIdType.MESH

BLK = 128
LOW = 512
CH = 4
UCH = 16
SLOTS = 4
FIRST = 8
LEAD = 4
UP_SIZES = (320, 336, 352, 512)


def rms_scale(values, gain):
    mean_sq = jnp.mean(values * values, axis=-1, keepdims=True)
    return values * lax.rsqrt(mean_sq + EPS) * gain


def attn_kernel(n_up, scale, pos_ref, off_ref, idx_ref, qd_ref, qf_ref, kf_ref, vn_ref, k_hbm, v_hbm, o_ref,
                kbuf, vbuf, own_lo, own_up, pack, rlo, rup, ksem, vsem, slo_s, slo_r, sup_s, sup_r):
    partner = {"dim": 1 - lax.axis_index("dim")}
    rows = qd_ref.shape[0]
    n_ch = rows // CH
    n_uch = n_up // UCH
    up_blocks = own_up.shape[0] // rows

    def kcopy(c):
        return pltpu.make_async_copy(k_hbm.at[pl.ds(c * CH, CH)], kbuf.at[lax.rem(c, SLOTS)], ksem.at[lax.rem(c, SLOTS)])

    def vcopy(c):
        return pltpu.make_async_copy(v_hbm.at[pl.ds(c * CH, CH)], vbuf.at[lax.rem(c, SLOTS)], vsem.at[lax.rem(c, SLOTS)])

    def lo_copy(c):
        part = pl.ds(c * CH, CH)
        return pltpu.make_async_remote_copy(src_ref=own_lo.at[part], dst_ref=rlo.at[part], send_sem=slo_s.at[c],
                                            recv_sem=slo_r.at[c], device_id=partner, device_id_type=MESH)

    def up_copy(c):
        part = pl.ds(c * UCH, UCH)
        return pltpu.make_async_remote_copy(src_ref=pack.at[part], dst_ref=rup.at[part], send_sem=sup_s.at[c],
                                            recv_sem=sup_r.at[c], device_id=partner, device_id_type=MESH)

    for c in range(SLOTS):
        kcopy(c).start()
    barrier = pltpu.get_barrier_semaphore()
    pl.semaphore_signal(barrier, inc=1, device_id=partner, device_id_type=MESH)
    pl.semaphore_wait(barrier, 1)
    for c in range(SLOTS):
        vcopy(c).start()

    @pl.loop(0, n_ch)
    def _(c):
        kcopy(c).wait()
        for r in range(CH):
            b = c * CH + r
            s = jnp.dot(qd_ref[b], kbuf[lax.rem(c, SLOTS), r], preferred_element_type=jnp.float32)
            own_lo[b] = s[:, :LOW]
            for j in range(up_blocks):
                own_up[b * up_blocks + j] = s[:, LOW + j * BLK:LOW + (j + 1) * BLK]

        @pl.when(c + SLOTS < n_ch)
        def _():
            kcopy(c + SLOTS).start()

        @pl.when((c >= 1) & (c <= FIRST))
        def _():
            lo_copy(c - 1).start()

    @pl.loop(0, n_uch + 1)
    def _(c):
        @pl.when(c < n_uch)
        def _():
            for r in range(UCH):
                j = c * UCH + r
                pack[j] = own_up[idx_ref[j]]

        @pl.when(c >= 1)
        def _():
            up_copy(c - 1).start()

    @pl.loop(FIRST, FIRST + LEAD)
    def _(c):
        lo_copy(c).start()

    @pl.loop(0, n_uch)
    def _(c):
        up_copy(c).wait_recv()

    lane = lax.broadcasted_iota(jnp.int32, (8, 2 * 64), 1)
    t_up = lax.broadcasted_iota(jnp.int32, (16, BLK), 1) + LOW

    @pl.loop(0, n_ch)
    def _(c):
        @pl.when(c + FIRST + LEAD < n_ch)
        def _():
            lo_copy(c + FIRST + LEAD).start()

        vcopy(c).wait()
        lo_copy(c).wait_recv()
        for r in range(CH):
            b = c * CH + r
            pos = pos_ref[b]
            off = off_ref[b]
            parts = [(own_lo[b] + rlo[b]) * scale]
            for j in range(up_blocks):
                total = (own_up[b * up_blocks + j] + rup[jnp.minimum(off + j, n_up - 1)]) * scale
                parts.append(jnp.where(t_up + j * BLK < pos, total, -jnp.inf))
            s = jnp.concatenate(parts, axis=1)
            kf = kf_ref[b]
            k_rows = jnp.concatenate([jnp.broadcast_to(kf[0:1], (8, 128)), jnp.broadcast_to(kf[1:2], (8, 128))], axis=0)
            s_new = jnp.sum(qf_ref[b].astype(jnp.float32) * k_rows, axis=1, keepdims=True) * scale
            m = jnp.maximum(jnp.max(s, axis=1, keepdims=True), s_new)
            e = jnp.exp(s - m)
            e_new = jnp.exp(s_new - m)
            inv = 1.0 / (jnp.sum(e, axis=1, keepdims=True) + e_new)
            p = (e * inv).astype(jnp.bfloat16)
            p_new = (e_new * inv).astype(jnp.bfloat16).astype(jnp.float32)
            o = lax.dot_general(p, vbuf[lax.rem(c, SLOTS), r], (((1,), (1,)), ((), ())), preferred_element_type=jnp.float32)
            o = o + p_new * vn_ref[pl.ds(b, 1), :]
            o_ref[b] = jnp.where(lane < 64, o[0:8], o[8:16]).astype(jnp.bfloat16)

        @pl.when(c + SLOTS < n_ch)
        def _():
            vcopy(c + SLOTS).start()

    @pl.loop(0, n_ch)
    def _(c):
        lo_copy(c).wait_send()

    @pl.loop(0, n_uch)
    def _(c):
        up_copy(c).wait_send()


def attend(n_up, cid, scale, pos, off, idx, qd, qf, kf, vn, k_t, v_t):
    rows = qd.shape[0]
    n_ch = rows // CH
    n_uch = n_up // UCH
    cache_len = k_t.shape[2]
    up_blocks = (cache_len - LOW) // BLK
    smem = pl.BlockSpec(memory_space=pltpu.SMEM)
    vmem = pl.BlockSpec(memory_space=pltpu.VMEM)
    hbm = pl.BlockSpec(memory_space=pl.ANY)
    return pl.pallas_call(
        functools.partial(attn_kernel, n_up, scale),
        out_shape=jax.ShapeDtypeStruct((rows, 8, 128), jnp.bfloat16),
        in_specs=[smem, smem, smem, vmem, vmem, vmem, vmem, hbm, hbm],
        out_specs=vmem,
        scratch_shapes=[
            pltpu.VMEM((SLOTS, CH, 128, cache_len), jnp.bfloat16),
            pltpu.VMEM((SLOTS, CH, 128, cache_len), jnp.bfloat16),
            pltpu.VMEM((rows, 16, LOW), jnp.float32),
            pltpu.VMEM((rows * up_blocks, 16, BLK), jnp.float32),
            pltpu.VMEM((n_up, 16, BLK), jnp.float32),
            pltpu.VMEM((rows, 16, LOW), jnp.float32),
            pltpu.VMEM((n_up, 16, BLK), jnp.float32),
            pltpu.SemaphoreType.DMA((SLOTS,)),
            pltpu.SemaphoreType.DMA((SLOTS,)),
            pltpu.SemaphoreType.DMA((n_ch,)),
            pltpu.SemaphoreType.DMA((n_ch,)),
            pltpu.SemaphoreType.DMA((n_uch,)),
            pltpu.SemaphoreType.DMA((n_uch,)),
        ],
        compiler_params=pltpu.CompilerParams(collective_id=cid, has_side_effects=True, vmem_limit_bytes=40 * 1024 * 1024),
        name=f"attend_{n_up}",
    )(pos, off, idx, qd, qf, kf, vn, k_t, v_t)


def solution(mesh):
    dim_count = mesh.shape['dim']
    mlp_axes = ('heads', 'dim')
    swap_perm = [(src, (src + dim_count // 2) % dim_count) for src in range(dim_count)]

    def layer_body(tokens, ln_attn, w_query, w_key, w_value, q_gain, k_gain, w_out, ln_mlp, w_gate, w_up, w_down, k_cache, v_cache, positions):
        rows = tokens.shape[0]
        heads_local = w_query.shape[1]
        kv_local = w_key.shape[1]
        slice_len = w_query.shape[2]
        head_dim = slice_len * dim_count
        half_dim = head_dim // 2
        q_group = heads_local // kv_local
        cache_len = k_cache.shape[1]
        up_blocks = (cache_len - LOW) // BLK
        dim_index = lax.axis_index('dim')

        tok_f32 = tokens.astype(jnp.float32)
        hidden = rms_scale(tok_f32, ln_attn).astype(jnp.bfloat16)
        q_part = jnp.einsum('bd,dhs->bhs', hidden, w_query, preferred_element_type=jnp.float32)
        k_part = jnp.einsum('bd,dhs->bhs', hidden, w_key, preferred_element_type=jnp.float32)
        v_new = jnp.einsum('bd,dhs->bhs', hidden, w_value, preferred_element_type=jnp.float32).astype(jnp.bfloat16)

        own = jnp.concatenate([q_part, k_part], axis=1)
        other = lax.ppermute(own, 'dim', swap_perm)
        gains = jnp.stack([q_gain, k_gain])
        gains_other = lax.ppermute(gains, 'dim', swap_perm)
        sq_total = jnp.sum(own * own, axis=-1, keepdims=True) + jnp.sum(other * other, axis=-1, keepdims=True)
        inv = lax.rsqrt(sq_total / head_dim + EPS)

        def spread(pair):
            return jnp.concatenate([jnp.broadcast_to(pair[0], (heads_local, slice_len)), jnp.broadcast_to(pair[1], (kv_local, slice_len))], axis=0)

        u_own = own * inv * spread(gains)
        u_other = other * inv * spread(gains_other)
        inv_freq = ROPE_BASE ** (-jnp.arange(half_dim, dtype=jnp.float32) * 2.0 / head_dim)
        rot_angle = positions.astype(jnp.float32)[:, None, None] * inv_freq
        cos_t = jnp.cos(rot_angle)
        sin_t = jnp.where(dim_index == 0, -1.0, 1.0) * jnp.sin(rot_angle)
        r_own = (u_own * cos_t + u_other * sin_t).astype(jnp.bfloat16)
        r_other = (u_other * cos_t - u_own * sin_t).astype(jnp.bfloat16)
        k_new = r_own[:, heads_local:]
        qf = jnp.concatenate([r_own[:, :heads_local], r_other[:, :heads_local]], axis=-1)
        kf = jnp.concatenate([k_new, r_other[:, heads_local:]], axis=-1).astype(jnp.float32)
        zeros = jnp.zeros((rows, q_group, slice_len), jnp.bfloat16)
        qd = jnp.concatenate([
            jnp.concatenate([r_own[:, :q_group], zeros], axis=-1),
            jnp.concatenate([zeros, r_own[:, q_group:heads_local]], axis=-1)], axis=1)
        vn = v_new.reshape(rows, kv_local * slice_len).astype(jnp.float32)

        n_blk = (positions - LOW + BLK - 1) // BLK
        cum = jnp.cumsum(n_blk)
        off = cum - n_blk
        slot = jnp.arange(rows * up_blocks)
        row_of = jnp.sum((cum[None, :] <= slot[:, None]).astype(jnp.int32), axis=1)
        off_of = jnp.sum(jnp.where(row_of[:, None] == jnp.arange(rows)[None, :], off[None, :], 0), axis=1)
        idx = jnp.where(row_of < rows, row_of * up_blocks + slot - off_of, 0)

        k_t = k_cache.transpose(0, 2, 3, 1).reshape(rows, kv_local * slice_len, cache_len)
        v_t = v_cache.transpose(0, 2, 3, 1).reshape(rows, kv_local * slice_len, cache_len)
        which = jnp.sum((cum[-1] > jnp.array(UP_SIZES[:-1])).astype(jnp.int32))
        branches = [functools.partial(attend, n, i, head_dim ** -0.5) for i, n in enumerate(UP_SIZES)]
        attn = lax.switch(which, branches, positions, off, idx, qd, qf, kf, vn, k_t, v_t)
        attn_vals = attn.reshape(rows, q_group, kv_local, slice_len).transpose(0, 2, 1, 3).reshape(rows, heads_local, slice_len)

        attn_out = lax.psum(jnp.einsum('bhs,hsd->bd', attn_vals, w_out, preferred_element_type=jnp.float32), mlp_axes)
        resid_f32 = (tok_f32 + attn_out).astype(jnp.bfloat16).astype(jnp.float32)
        hidden2 = rms_scale(resid_f32, ln_mlp).astype(jnp.bfloat16)
        gate_val = jnp.dot(hidden2, w_gate, preferred_element_type=jnp.float32)
        up_val = jnp.dot(hidden2, w_up, preferred_element_type=jnp.float32)
        mlp_act = (jax.nn.silu(gate_val) * up_val).astype(jnp.bfloat16)
        mlp_out = lax.psum(jnp.dot(mlp_act, w_down, preferred_element_type=jnp.float32), mlp_axes)
        return (resid_f32 + mlp_out).astype(jnp.bfloat16), k_new, v_new

    row_spec = P('dp', None)
    head_spec = P(None, 'heads', 'dim')
    cache_spec = P('dp', None, 'heads', 'dim')
    new_spec = P('dp', 'heads', 'dim')
    in_specs = (row_spec, P(None), head_spec, head_spec, head_spec, P('dim'), P('dim'), P('heads', 'dim', None), P(None), P(None, mlp_axes), P(None, mlp_axes), P(mlp_axes, None), cache_spec, cache_spec, P('dp'))
    out_specs = (row_spec, new_spec, new_spec)
    return jax.shard_map(layer_body, mesh=mesh, in_specs=in_specs, out_specs=out_specs, check_vma=False)
```

```python
import functools

import jax
import jax.numpy as jnp
from jax import lax
from jax.experimental import pallas as pl
from jax.experimental.pallas import tpu as pltpu
from jax.sharding import PartitionSpec as P

EPS = 1e-6
ROPE_BASE = 1000000.0
MESH = pl.DeviceIdType.MESH

BLK = 128
LOW = 512
CH = 4
UCH = 16
SLOTS = 4
FIRST = 8
LEAD = 4
UP_SIZES = (320, 336, 352, 512)


def rms_scale(values, gain):
    mean_sq = jnp.mean(values * values, axis=-1, keepdims=True)
    return values * lax.rsqrt(mean_sq + EPS) * gain


def attn_kernel(n_up, scale, pos_ref, off_ref, idx_ref, qd_ref, qf_ref, kf_ref, vn_ref, k_hbm, v_hbm, o_ref,
                kbuf, vbuf, own_lo, own_up, pack, rlo, rup, ksem, vsem, slo_s, slo_r, sup_s, sup_r):
    partner = {"dim": 1 - lax.axis_index("dim")}
    rows = qd_ref.shape[0]
    n_ch = rows // CH
    n_uch = n_up // UCH
    up_blocks = own_up.shape[0] // rows

    def kcopy(c):
        return pltpu.make_async_copy(k_hbm.at[pl.ds(c * CH, CH)], kbuf.at[lax.rem(c, SLOTS)], ksem.at[lax.rem(c, SLOTS)])

    def vcopy(c):
        return pltpu.make_async_copy(v_hbm.at[pl.ds(c * CH, CH)], vbuf.at[lax.rem(c, SLOTS)], vsem.at[lax.rem(c, SLOTS)])

    def lo_copy(c):
        part = pl.ds(c * CH, CH)
        return pltpu.make_async_remote_copy(src_ref=own_lo.at[part], dst_ref=rlo.at[part], send_sem=slo_s.at[c],
                                            recv_sem=slo_r.at[c], device_id=partner, device_id_type=MESH)

    def up_copy(c):
        part = pl.ds(c * UCH, UCH)
        return pltpu.make_async_remote_copy(src_ref=pack.at[part], dst_ref=rup.at[part], send_sem=sup_s.at[c],
                                            recv_sem=sup_r.at[c], device_id=partner, device_id_type=MESH)

    for c in range(SLOTS):
        kcopy(c).start()
    barrier = pltpu.get_barrier_semaphore()
    pl.semaphore_signal(barrier, inc=1, device_id=partner, device_id_type=MESH)
    pl.semaphore_wait(barrier, 1)
    for c in range(SLOTS):
        vcopy(c).start()

    @pl.loop(0, n_ch)
    def _(c):
        kcopy(c).wait()
        for r in range(CH):
            b = c * CH + r
            s = jnp.dot(qd_ref[b], kbuf[lax.rem(c, SLOTS), r], preferred_element_type=jnp.float32)
            own_lo[b] = s[:, :LOW]
            for j in range(up_blocks):
                own_up[b * up_blocks + j] = s[:, LOW + j * BLK:LOW + (j + 1) * BLK]

        @pl.when(c + SLOTS < n_ch)
        def _():
            kcopy(c + SLOTS).start()

        @pl.when((c >= 1) & (c <= FIRST))
        def _():
            lo_copy(c - 1).start()

    @pl.loop(0, n_uch + 1)
    def _(c):
        @pl.when(c < n_uch)
        def _():
            for r in range(UCH):
                j = c * UCH + r
                pack[j] = own_up[idx_ref[j]]

        @pl.when(c >= 1)
        def _():
            up_copy(c - 1).start()

    @pl.loop(FIRST, FIRST + LEAD)
    def _(c):
        lo_copy(c).start()

    @pl.loop(0, n_uch)
    def _(c):
        up_copy(c).wait_recv()

    lane = lax.broadcasted_iota(jnp.int32, (8, 2 * 64), 1)
    t_up = lax.broadcasted_iota(jnp.int32, (16, BLK), 1) + LOW

    @pl.loop(0, n_ch)
    def _(c):
        @pl.when(c + FIRST + LEAD < n_ch)
        def _():
            lo_copy(c + FIRST + LEAD).start()

        vcopy(c).wait()
        lo_copy(c).wait_recv()
        for r in range(CH):
            b = c * CH + r
            pos = pos_ref[b]
            off = off_ref[b]
            parts = [(own_lo[b] + rlo[b]) * scale]
            for j in range(up_blocks):
                total = (own_up[b * up_blocks + j] + rup[jnp.minimum(off + j, n_up - 1)]) * scale
                parts.append(jnp.where(t_up + j * BLK < pos, total, -jnp.inf))
            s = jnp.concatenate(parts, axis=1)
            kf = kf_ref[b]
            k_rows = jnp.concatenate([jnp.broadcast_to(kf[0:1], (8, 128)), jnp.broadcast_to(kf[1:2], (8, 128))], axis=0)
            s_new = jnp.sum(qf_ref[b].astype(jnp.float32) * k_rows, axis=1, keepdims=True) * scale
            m = jnp.maximum(jnp.max(s, axis=1, keepdims=True), s_new)
            e = jnp.exp(s - m)
            e_new = jnp.exp(s_new - m)
            inv = 1.0 / (jnp.sum(e, axis=1, keepdims=True) + e_new)
            p = (e * inv).astype(jnp.bfloat16)
            p_new = (e_new * inv).astype(jnp.bfloat16).astype(jnp.float32)
            o = lax.dot_general(p, vbuf[lax.rem(c, SLOTS), r], (((1,), (1,)), ((), ())), preferred_element_type=jnp.float32)
            o = o + p_new * vn_ref[pl.ds(b, 1), :]
            o_ref[b] = jnp.where(lane < 64, o[0:8], o[8:16]).astype(jnp.bfloat16)

        @pl.when(c + SLOTS < n_ch)
        def _():
            vcopy(c + SLOTS).start()

    @pl.loop(0, n_ch)
    def _(c):
        lo_copy(c).wait_send()

    @pl.loop(0, n_uch)
    def _(c):
        up_copy(c).wait_send()


def attend(n_up, cid, scale, pos, off, idx, qd, qf, kf, vn, k_t, v_t):
    rows = qd.shape[0]
    n_ch = rows // CH
    n_uch = n_up // UCH
    cache_len = k_t.shape[2]
    up_blocks = (cache_len - LOW) // BLK
    smem = pl.BlockSpec(memory_space=pltpu.SMEM)
    vmem = pl.BlockSpec(memory_space=pltpu.VMEM)
    hbm = pl.BlockSpec(memory_space=pl.ANY)
    return pl.pallas_call(
        functools.partial(attn_kernel, n_up, scale),
        out_shape=jax.ShapeDtypeStruct((rows, 8, 128), jnp.bfloat16),
        in_specs=[smem, smem, smem, vmem, vmem, vmem, vmem, hbm, hbm],
        out_specs=vmem,
        scratch_shapes=[
            pltpu.VMEM((SLOTS, CH, 128, cache_len), jnp.bfloat16),
            pltpu.VMEM((SLOTS, CH, 128, cache_len), jnp.bfloat16),
            pltpu.VMEM((rows, 16, LOW), jnp.float32),
            pltpu.VMEM((rows * up_blocks, 16, BLK), jnp.float32),
            pltpu.VMEM((n_up, 16, BLK), jnp.float32),
            pltpu.VMEM((rows, 16, LOW), jnp.float32),
            pltpu.VMEM((n_up, 16, BLK), jnp.float32),
            pltpu.SemaphoreType.DMA((SLOTS,)),
            pltpu.SemaphoreType.DMA((SLOTS,)),
            pltpu.SemaphoreType.DMA((n_ch,)),
            pltpu.SemaphoreType.DMA((n_ch,)),
            pltpu.SemaphoreType.DMA((n_uch,)),
            pltpu.SemaphoreType.DMA((n_uch,)),
        ],
        compiler_params=pltpu.CompilerParams(collective_id=cid, has_side_effects=True, vmem_limit_bytes=40 * 1024 * 1024),
        name=f"attend_{n_up}",
    )(pos, off, idx, qd, qf, kf, vn, k_t, v_t)


Q = 10
WO_SLOTS = 4
GU_SLOTS = 4
WD_SLOTS = 4


def tail_kernel(x_ref, tok_ref, ln_ref, wo_hbm, wg_hbm, wu_hbm, wd_hbm, out_ref,
                part, r1, r2, r3, full, xres, acc_g, acc_u, mact, wo, wg, wu, wd,
                wo_s, wg_s, wu_s, wd_s, snd, rcv):
    heads = lax.axis_index("heads")
    core, cx, cy = lax.rem(heads, 2), heads // 2, lax.axis_index("dim")
    sib = {"heads": 2 * cx + 1 - core}
    xn = {"heads": 2 * (1 - cx) + core}
    yn = {"dim": 1 - cy}
    width = part.shape[3]
    rows = 16 * 8
    f32 = jnp.float32

    def cols(q):
        return pl.ds(pl.multiple_of(q * width, width), width)

    def wo_copy(q):
        s = lax.rem(q, WO_SLOTS)
        return [pltpu.make_async_copy(wo_hbm.at[:, cols(q)], wo.at[s], wo_s.at[s])]

    def gu_copy(q):
        s = lax.rem(q, GU_SLOTS)
        return [pltpu.make_async_copy(wg_hbm.at[cols(q)], wg.at[s], wg_s.at[s]),
                pltpu.make_async_copy(wu_hbm.at[cols(q)], wu.at[s], wu_s.at[s])]

    def wd_copy(q):
        s = lax.rem(q, WD_SLOTS)
        return [pltpu.make_async_copy(wd_hbm.at[:, cols(q)], wd.at[s], wd_s.at[s])]

    def start(copies):
        for cp in copies:
            cp.start()

    def wait(copies):
        for cp in copies:
            cp.wait()

    def remote(ph, st, q, src, dst, dev):
        return pltpu.make_async_remote_copy(src_ref=src, dst_ref=dst, send_sem=snd.at[ph, st], recv_sem=rcv.at[ph, st, q],
                                            device_id=dev, device_id_type=MESH)

    def stage(ph, k, q, sem_q):
        if k == 0:
            return [remote(ph, 0, sem_q, part.at[q, pl.ds(8 * (1 - core), 8)], r1.at[q], sib)]
        if k == 1:
            return [remote(ph, 1, sem_q, r1.at[q, pl.ds(2 * (1 - cx), 2)], r2.at[q, pl.ds(0, 2)], xn),
                    remote(ph, 2, sem_q, r1.at[q, pl.ds(4 + 2 * (1 - cy), 2)], r2.at[q, pl.ds(2, 2)], yn)]
        if k == 2:
            return [remote(ph, 3, sem_q, r2.at[q, pl.ds(1 - cy, 1)], r3.at[q, pl.ds(0, 1)], yn),
                    remote(ph, 4, sem_q, r2.at[q, pl.ds(2 + 1 - cx, 1)], r3.at[q, pl.ds(1, 1)], xn)]
        blk_a, blk_b = core * 8, core * 8 + 4
        if k == 3:
            a, b = full.at[q, pl.ds(blk_a + 2 * cx + cy, 1)], full.at[q, pl.ds(blk_b + 2 * cy + cx, 1)]
            return [remote(ph, 5, sem_q, a, a, yn), remote(ph, 6, sem_q, b, b, xn)]
        if k == 4:
            a, b = full.at[q, pl.ds(blk_a + 2 * cx, 2)], full.at[q, pl.ds(blk_b + 2 * cy, 2)]
            return [remote(ph, 7, sem_q, a, a, xn), remote(ph, 8, sem_q, b, b, yn)]
        a = full.at[q, pl.ds(blk_a, 8)]
        return [remote(ph, 9, sem_q, a, a, sib)]

    def one(ph, k, q):
        return stage(ph, k, q, q)

    def drain(ph, ks):
        for k in ks:
            for cp in stage(ph, k, slice(None), 0):
                cp.wait_send()

    def arrived(ph, k, q):
        for cp in one(ph, k, q):
            cp.wait_recv()

    def when(t, lo):
        return pl.when((t >= lo) & (t < lo + Q))

    def reduce_steps(ph, t, finish):
        @when(t, 1)
        def _():
            start(one(ph, 0, t - 1))

        @when(t, 2)
        def _():
            u = t - 2
            arrived(ph, 0, u)
            r1[u] = r1[u] + part[u, pl.ds(8 * core, 8)]
            start(one(ph, 1, u))

        @when(t, 4)
        def _():
            u = t - 4
            arrived(ph, 1, u)
            r2[u, pl.ds(0, 2)] = r2[u, pl.ds(0, 2)] + r1[u, pl.ds(2 * cx, 2)]
            r2[u, pl.ds(2, 2)] = r2[u, pl.ds(2, 2)] + r1[u, pl.ds(4 + 2 * cy, 2)]
            start(one(ph, 2, u))

        @when(t, 6)
        def _():
            u = t - 6
            arrived(ph, 2, u)
            finish(u, r3[u, 0] + r2[u, cy], r3[u, 1] + r2[u, 2 + cx])

    def gather_steps(ph, t, finish):
        @when(t, 0)
        def _():
            start(one(ph, 3, t))

        @when(t, 2)
        def _():
            arrived(ph, 3, t - 2)
            start(one(ph, 4, t - 2))

        @when(t, 4)
        def _():
            arrived(ph, 4, t - 4)
            start(one(ph, 5, t - 4))

        @when(t, 5)
        def _():
            arrived(ph, 5, t - 5)
            finish(t - 5)

    for q in range(WO_SLOTS):
        start(wo_copy(q))
    barrier = pltpu.get_barrier_semaphore()
    for dev in (sib, xn, yn):
        pl.semaphore_signal(barrier, inc=1, device_id=dev, device_id_type=MESH)
    pl.semaphore_wait(barrier, 3)

    def finish_attn(u, a, b):
        xres[u, 0] = (tok_ref[u, 0] + a).astype(jnp.bfloat16).astype(f32)
        xres[u, 1] = (tok_ref[u, 1] + b).astype(jnp.bfloat16).astype(f32)

    @pl.loop(0, Q + 6)
    def _(t):
        @when(t, 0)
        def _():
            wait(wo_copy(t))
            part[t] = jnp.dot(x_ref[...], wo[lax.rem(t, WO_SLOTS)], preferred_element_type=f32).reshape(16, 8, width)

            @pl.when(t + WO_SLOTS < Q)
            def _():
                start(wo_copy(t + WO_SLOTS))

            @pl.when(t < GU_SLOTS)
            def _():
                start(gu_copy(t))

            @pl.when((t >= GU_SLOTS) & (t < GU_SLOTS + WD_SLOTS))
            def _():
                start(wd_copy(t - GU_SLOTS))
        reduce_steps(0, t, finish_attn)

    drain(0, (0, 1, 2))
    sq = jnp.zeros((2, 8, 1), f32)
    for q in range(Q):
        sq = sq + jnp.sum(xres[q] * xres[q], axis=-1, keepdims=True)
    inv = lax.rsqrt(sq / (Q * width) + EPS)
    blk_a, blk_b = core * 8 + 2 * cx + cy, core * 8 + 4 + 2 * cy + cx
    for q in range(Q):
        h = (xres[q] * inv * ln_ref[q]).astype(jnp.bfloat16).astype(f32)
        full[q, blk_a] = h[0]
        full[q, blk_b] = h[1]
    acc_g[...] = jnp.zeros_like(acc_g)
    acc_u[...] = jnp.zeros_like(acc_u)

    def finish_gather(u):
        wait(gu_copy(u))
        s = lax.rem(u, GU_SLOTS)
        h = full[u].reshape(rows, width).astype(jnp.bfloat16)
        inner = acc_g.shape[1]
        step = 512

        @pl.loop(0, inner // step)
        def _(n):
            c = pl.ds(pl.multiple_of(n * step, step), step)
            acc_g[:, c] += jnp.dot(h, wg[s, :, c], preferred_element_type=f32)
            acc_u[:, c] += jnp.dot(h, wu[s, :, c], preferred_element_type=f32)
        c = pl.ds(inner // step * step, inner % step)
        acc_g[:, c] += jnp.dot(h, wg[s, :, c], preferred_element_type=f32)
        acc_u[:, c] += jnp.dot(h, wu[s, :, c], preferred_element_type=f32)

        @pl.when(u + GU_SLOTS < Q)
        def _():
            start(gu_copy(u + GU_SLOTS))

    @pl.loop(0, Q + 5)
    def _(t):
        gather_steps(0, t, finish_gather)

    drain(0, (3, 4, 5))

    @pl.loop(0, acc_g.shape[1] // 640)
    def _(n):
        c = pl.ds(pl.multiple_of(n * 640, 640), 640)
        mact[:, c] = (jax.nn.silu(acc_g[:, c]) * acc_u[:, c]).astype(jnp.bfloat16)

    def finish_mlp(u, a, b):
        full[u, blk_a] = (xres[u, 0] + a).astype(jnp.bfloat16).astype(f32)
        full[u, blk_b] = (xres[u, 1] + b).astype(jnp.bfloat16).astype(f32)

    @pl.loop(0, Q + 6)
    def _(t):
        @when(t, 0)
        def _():
            wait(wd_copy(t))
            part[t] = jnp.dot(mact[...], wd[lax.rem(t, WD_SLOTS)], preferred_element_type=f32).reshape(16, 8, width)

            @pl.when(t + WD_SLOTS < Q)
            def _():
                start(wd_copy(t + WD_SLOTS))
        reduce_steps(1, t, finish_mlp)

    def finish_out(u):
        out_ref[:, cols(u)] = full[u].reshape(rows, width).astype(jnp.bfloat16)

    @pl.loop(0, Q + 5)
    def _(t):
        gather_steps(1, t, finish_out)

    drain(1, (0, 1, 2, 3, 4, 5))


def tail(cid, attn_vals, tok_own, ln, w_out, w_gate, w_up, w_down):
    rows, depth = attn_vals.shape
    d_model, inner = w_gate.shape
    width = d_model // Q
    vmem = pl.BlockSpec(memory_space=pltpu.VMEM)
    hbm = pl.BlockSpec(memory_space=pl.ANY)
    f32, bf16 = jnp.float32, jnp.bfloat16
    dma = pltpu.SemaphoreType.DMA
    return pl.pallas_call(
        tail_kernel,
        out_shape=jax.ShapeDtypeStruct((rows, d_model), bf16),
        in_specs=[vmem, vmem, vmem, hbm, hbm, hbm, hbm],
        out_specs=vmem,
        scratch_shapes=[
            pltpu.VMEM((Q, 16, 8, width), f32),
            pltpu.VMEM((Q, 8, 8, width), f32),
            pltpu.VMEM((Q, 4, 8, width), f32),
            pltpu.VMEM((Q, 2, 8, width), f32),
            pltpu.VMEM((Q, 16, 8, width), f32),
            pltpu.VMEM((Q, 2, 8, width), f32),
            pltpu.VMEM((rows, inner), f32),
            pltpu.VMEM((rows, inner), f32),
            pltpu.VMEM((rows, inner), bf16),
            pltpu.VMEM((WO_SLOTS, depth, width), bf16),
            pltpu.VMEM((GU_SLOTS, width, inner), bf16),
            pltpu.VMEM((GU_SLOTS, width, inner), bf16),
            pltpu.VMEM((WD_SLOTS, inner, width), bf16),
            dma((WO_SLOTS,)), dma((GU_SLOTS,)), dma((GU_SLOTS,)), dma((WD_SLOTS,)),
            dma((2, 10)), dma((2, 10, Q)),
        ],
        compiler_params=pltpu.CompilerParams(collective_id=cid, has_side_effects=True, vmem_limit_bytes=62 * 1024 * 1024),
        name="tail",
    )(attn_vals, tok_own, ln, w_out, w_gate, w_up, w_down)


def solution(mesh):
    dim_count = mesh.shape['dim']
    mlp_axes = ('heads', 'dim')
    swap_perm = [(src, (src + dim_count // 2) % dim_count) for src in range(dim_count)]

    def layer_body(tokens, ln_attn, w_query, w_key, w_value, q_gain, k_gain, w_out, ln_mlp, w_gate, w_up, w_down, k_cache, v_cache, positions):
        rows = tokens.shape[0]
        heads_local = w_query.shape[1]
        kv_local = w_key.shape[1]
        slice_len = w_query.shape[2]
        head_dim = slice_len * dim_count
        half_dim = head_dim // 2
        q_group = heads_local // kv_local
        cache_len = k_cache.shape[1]
        up_blocks = (cache_len - LOW) // BLK
        dim_index = lax.axis_index('dim')

        hidden = rms_scale(tokens.astype(jnp.float32), ln_attn).astype(jnp.bfloat16)
        q_part = jnp.einsum('bd,dhs->bhs', hidden, w_query, preferred_element_type=jnp.float32)
        k_part = jnp.einsum('bd,dhs->bhs', hidden, w_key, preferred_element_type=jnp.float32)
        v_new = jnp.einsum('bd,dhs->bhs', hidden, w_value, preferred_element_type=jnp.float32).astype(jnp.bfloat16)

        own = jnp.concatenate([q_part, k_part], axis=1)
        other = lax.ppermute(own, 'dim', swap_perm)
        gains = jnp.stack([q_gain, k_gain])
        gains_other = lax.ppermute(gains, 'dim', swap_perm)
        sq_total = jnp.sum(own * own, axis=-1, keepdims=True) + jnp.sum(other * other, axis=-1, keepdims=True)
        inv = lax.rsqrt(sq_total / head_dim + EPS)

        def spread(pair):
            return jnp.concatenate([jnp.broadcast_to(pair[0], (heads_local, slice_len)), jnp.broadcast_to(pair[1], (kv_local, slice_len))], axis=0)

        u_own = own * inv * spread(gains)
        u_other = other * inv * spread(gains_other)
        inv_freq = ROPE_BASE ** (-jnp.arange(half_dim, dtype=jnp.float32) * 2.0 / head_dim)
        rot_angle = positions.astype(jnp.float32)[:, None, None] * inv_freq
        cos_t = jnp.cos(rot_angle)
        sin_t = jnp.where(dim_index == 0, -1.0, 1.0) * jnp.sin(rot_angle)
        r_own = (u_own * cos_t + u_other * sin_t).astype(jnp.bfloat16)
        r_other = (u_other * cos_t - u_own * sin_t).astype(jnp.bfloat16)
        k_new = r_own[:, heads_local:]
        qf = jnp.concatenate([r_own[:, :heads_local], r_other[:, :heads_local]], axis=-1)
        kf = jnp.concatenate([k_new, r_other[:, heads_local:]], axis=-1).astype(jnp.float32)
        zeros = jnp.zeros((rows, q_group, slice_len), jnp.bfloat16)
        qd = jnp.concatenate([
            jnp.concatenate([r_own[:, :q_group], zeros], axis=-1),
            jnp.concatenate([zeros, r_own[:, q_group:heads_local]], axis=-1)], axis=1)
        vn = v_new.reshape(rows, kv_local * slice_len).astype(jnp.float32)

        n_blk = (positions - LOW + BLK - 1) // BLK
        cum = jnp.cumsum(n_blk)
        off = cum - n_blk
        slot = jnp.arange(rows * up_blocks)
        row_of = jnp.sum((cum[None, :] <= slot[:, None]).astype(jnp.int32), axis=1)
        off_of = jnp.sum(jnp.where(row_of[:, None] == jnp.arange(rows)[None, :], off[None, :], 0), axis=1)
        idx = jnp.where(row_of < rows, row_of * up_blocks + slot - off_of, 0)

        k_t = k_cache.transpose(0, 2, 3, 1).reshape(rows, kv_local * slice_len, cache_len)
        v_t = v_cache.transpose(0, 2, 3, 1).reshape(rows, kv_local * slice_len, cache_len)
        which = jnp.sum((cum[-1] > jnp.array(UP_SIZES[:-1])).astype(jnp.int32))
        branches = [functools.partial(attend, n, i, head_dim ** -0.5) for i, n in enumerate(UP_SIZES)]
        attn = lax.switch(which, branches, positions, off, idx, qd, qf, kf, vn, k_t, v_t)
        attn_vals = attn.reshape(rows, q_group, kv_local, slice_len).transpose(0, 2, 1, 3).reshape(rows, heads_local, slice_len)

        attn_vals = attn_vals.reshape(rows, heads_local * slice_len)
        heads_index = lax.axis_index('heads')
        core, cx = heads_index % 2, heads_index // 2
        tok_blocks = tokens.reshape(16, 8, Q, -1)
        tok_own = jnp.stack([lax.dynamic_index_in_dim(tok_blocks, core * 8 + 2 * cx + dim_index, 0, keepdims=False),
                             lax.dynamic_index_in_dim(tok_blocks, core * 8 + 4 + 2 * dim_index + cx, 0, keepdims=False)])
        tok_own = tok_own.astype(jnp.float32).transpose(2, 0, 1, 3)
        out = tail(len(UP_SIZES), attn_vals, tok_own, ln_mlp.reshape(Q, 1, -1), w_out.reshape(heads_local * slice_len, -1), w_gate, w_up, w_down)
        return out, k_new, v_new

    row_spec = P('dp', None)
    head_spec = P(None, 'heads', 'dim')
    cache_spec = P('dp', None, 'heads', 'dim')
    new_spec = P('dp', 'heads', 'dim')
    in_specs = (row_spec, P(None), head_spec, head_spec, head_spec, P('dim'), P('dim'), P('heads', 'dim', None), P(None), P(None, mlp_axes), P(None, mlp_axes), P(mlp_axes, None), cache_spec, cache_spec, P('dp'))
    out_specs = (row_spec, new_spec, new_spec)
    return jax.shard_map(layer_body, mesh=mesh, in_specs=in_specs, out_specs=out_specs, check_vma=False)
```

```python
import functools

import jax
import jax.numpy as jnp
from jax import lax
from jax.experimental import pallas as pl
from jax.experimental.pallas import tpu as pltpu
from jax.sharding import PartitionSpec as P

EPS = 1e-6
ROPE_BASE = 1000000.0
MESH = pl.DeviceIdType.MESH

BLK = 128
LOW = 512
CH = 4
UCH = 16
SLOTS = 4
FIRST = 8
LEAD = 4
UP_SIZES = (320, 336, 352, 512)


def rms_scale(values, gain):
    mean_sq = jnp.mean(values * values, axis=-1, keepdims=True)
    return values * lax.rsqrt(mean_sq + EPS) * gain


def attn_kernel(n_up, scale, pos_ref, off_ref, idx_ref, qd_ref, qf_ref, kf_ref, vn_ref, k_hbm, v_hbm, o_ref,
                kbuf, vbuf, own_lo, own_up, pack, rlo, rup, ksem, vsem, slo_s, slo_r, sup_s, sup_r):
    partner = {"dim": 1 - lax.axis_index("dim")}
    rows = qd_ref.shape[0]
    n_ch = rows // CH
    n_uch = n_up // UCH
    up_blocks = own_up.shape[0] // rows

    def kcopy(c):
        return pltpu.make_async_copy(k_hbm.at[pl.ds(c * CH, CH)], kbuf.at[lax.rem(c, SLOTS)], ksem.at[lax.rem(c, SLOTS)])

    def vcopy(c):
        return pltpu.make_async_copy(v_hbm.at[pl.ds(c * CH, CH)], vbuf.at[lax.rem(c, SLOTS)], vsem.at[lax.rem(c, SLOTS)])

    def lo_copy(c):
        part = pl.ds(c * CH, CH)
        return pltpu.make_async_remote_copy(src_ref=own_lo.at[part], dst_ref=rlo.at[part], send_sem=slo_s.at[c],
                                            recv_sem=slo_r.at[c], device_id=partner, device_id_type=MESH)

    def up_copy(c):
        part = pl.ds(c * UCH, UCH)
        return pltpu.make_async_remote_copy(src_ref=pack.at[part], dst_ref=rup.at[part], send_sem=sup_s.at[c],
                                            recv_sem=sup_r.at[c], device_id=partner, device_id_type=MESH)

    for c in range(SLOTS):
        kcopy(c).start()
    barrier = pltpu.get_barrier_semaphore()
    pl.semaphore_signal(barrier, inc=1, device_id=partner, device_id_type=MESH)
    pl.semaphore_wait(barrier, 1)
    for c in range(SLOTS):
        vcopy(c).start()

    @pl.loop(0, n_ch)
    def _(c):
        kcopy(c).wait()
        for r in range(CH):
            b = c * CH + r
            s = jnp.dot(qd_ref[b], kbuf[lax.rem(c, SLOTS), r], preferred_element_type=jnp.float32)
            own_lo[b] = s[:, :LOW]
            for j in range(up_blocks):
                own_up[b * up_blocks + j] = s[:, LOW + j * BLK:LOW + (j + 1) * BLK]

        @pl.when(c + SLOTS < n_ch)
        def _():
            kcopy(c + SLOTS).start()

        @pl.when((c >= 1) & (c <= FIRST))
        def _():
            lo_copy(c - 1).start()

    @pl.loop(0, n_uch + 1)
    def _(c):
        @pl.when(c < n_uch)
        def _():
            for r in range(UCH):
                j = c * UCH + r
                pack[j] = own_up[idx_ref[j]]

        @pl.when(c >= 1)
        def _():
            up_copy(c - 1).start()

    @pl.loop(FIRST, FIRST + LEAD)
    def _(c):
        lo_copy(c).start()

    @pl.loop(0, n_uch)
    def _(c):
        up_copy(c).wait_recv()

    lane = lax.broadcasted_iota(jnp.int32, (8, 2 * 64), 1)
    t_up = lax.broadcasted_iota(jnp.int32, (16, BLK), 1) + LOW

    @pl.loop(0, n_ch)
    def _(c):
        @pl.when(c + FIRST + LEAD < n_ch)
        def _():
            lo_copy(c + FIRST + LEAD).start()

        vcopy(c).wait()
        lo_copy(c).wait_recv()
        for r in range(CH):
            b = c * CH + r
            pos = pos_ref[b]
            off = off_ref[b]
            parts = [(own_lo[b] + rlo[b]) * scale]
            for j in range(up_blocks):
                total = (own_up[b * up_blocks + j] + rup[jnp.minimum(off + j, n_up - 1)]) * scale
                parts.append(jnp.where(t_up + j * BLK < pos, total, -jnp.inf))
            s = jnp.concatenate(parts, axis=1)
            kf = kf_ref[b]
            k_rows = jnp.concatenate([jnp.broadcast_to(kf[0:1], (8, 128)), jnp.broadcast_to(kf[1:2], (8, 128))], axis=0)
            s_new = jnp.sum(qf_ref[b].astype(jnp.float32) * k_rows, axis=1, keepdims=True) * scale
            m = jnp.maximum(jnp.max(s, axis=1, keepdims=True), s_new)
            e = jnp.exp(s - m)
            e_new = jnp.exp(s_new - m)
            inv = 1.0 / (jnp.sum(e, axis=1, keepdims=True) + e_new)
            p = (e * inv).astype(jnp.bfloat16)
            p_new = (e_new * inv).astype(jnp.bfloat16).astype(jnp.float32)
            o = lax.dot_general(p, vbuf[lax.rem(c, SLOTS), r], (((1,), (1,)), ((), ())), preferred_element_type=jnp.float32)
            o = o + p_new * vn_ref[pl.ds(b, 1), :]
            o_ref[b] = jnp.where(lane < 64, o[0:8], o[8:16]).astype(jnp.bfloat16)

        @pl.when(c + SLOTS < n_ch)
        def _():
            vcopy(c + SLOTS).start()

    @pl.loop(0, n_ch)
    def _(c):
        lo_copy(c).wait_send()

    @pl.loop(0, n_uch)
    def _(c):
        up_copy(c).wait_send()


def attend(n_up, cid, scale, pos, off, idx, qd, qf, kf, vn, k_t, v_t):
    rows = qd.shape[0]
    n_ch = rows // CH
    n_uch = n_up // UCH
    cache_len = k_t.shape[2]
    up_blocks = (cache_len - LOW) // BLK
    smem = pl.BlockSpec(memory_space=pltpu.SMEM)
    vmem = pl.BlockSpec(memory_space=pltpu.VMEM)
    hbm = pl.BlockSpec(memory_space=pl.ANY)
    return pl.pallas_call(
        functools.partial(attn_kernel, n_up, scale),
        out_shape=jax.ShapeDtypeStruct((rows, 8, 128), jnp.bfloat16),
        in_specs=[smem, smem, smem, vmem, vmem, vmem, vmem, hbm, hbm],
        out_specs=vmem,
        scratch_shapes=[
            pltpu.VMEM((SLOTS, CH, 128, cache_len), jnp.bfloat16),
            pltpu.VMEM((SLOTS, CH, 128, cache_len), jnp.bfloat16),
            pltpu.VMEM((rows, 16, LOW), jnp.float32),
            pltpu.VMEM((rows * up_blocks, 16, BLK), jnp.float32),
            pltpu.VMEM((n_up, 16, BLK), jnp.float32),
            pltpu.VMEM((rows, 16, LOW), jnp.float32),
            pltpu.VMEM((n_up, 16, BLK), jnp.float32),
            pltpu.SemaphoreType.DMA((SLOTS,)),
            pltpu.SemaphoreType.DMA((SLOTS,)),
            pltpu.SemaphoreType.DMA((n_ch,)),
            pltpu.SemaphoreType.DMA((n_ch,)),
            pltpu.SemaphoreType.DMA((n_uch,)),
            pltpu.SemaphoreType.DMA((n_uch,)),
        ],
        compiler_params=pltpu.CompilerParams(collective_id=cid, has_side_effects=True, vmem_limit_bytes=40 * 1024 * 1024),
        name=f"attend_{n_up}",
    )(pos, off, idx, qd, qf, kf, vn, k_t, v_t)


Q = 10
WO_SLOTS = 4
GU_SLOTS = 4
WD_SLOTS = 4


def tail_kernel(x_ref, tok_ref, ln_ref, wo_hbm, wg_hbm, wu_hbm, wd_hbm, out_ref,
                part, r1, r2, r3, full, xres, acc_g, acc_u, mact, wo, wg, wu, wd,
                wo_s, wg_s, wu_s, wd_s, snd, rcv):
    heads = lax.axis_index("heads")
    core, cx, cy = lax.rem(heads, 2), heads // 2, lax.axis_index("dim")
    sib = {"heads": 2 * cx + 1 - core}
    xn = {"heads": 2 * (1 - cx) + core}
    yn = {"dim": 1 - cy}
    width = part.shape[3]
    rows = 16 * 8
    f32 = jnp.float32

    def cols(q):
        return pl.ds(pl.multiple_of(q * width, width), width)

    def wo_copy(q):
        s = lax.rem(q, WO_SLOTS)
        return [pltpu.make_async_copy(wo_hbm.at[:, cols(q)], wo.at[s], wo_s.at[s])]

    def gu_copy(q):
        s = lax.rem(q, GU_SLOTS)
        return [pltpu.make_async_copy(wg_hbm.at[cols(q)], wg.at[s], wg_s.at[s]),
                pltpu.make_async_copy(wu_hbm.at[cols(q)], wu.at[s], wu_s.at[s])]

    def wd_copy(q):
        s = lax.rem(q, WD_SLOTS)
        return [pltpu.make_async_copy(wd_hbm.at[:, cols(q)], wd.at[s], wd_s.at[s])]

    def start(copies):
        for cp in copies:
            cp.start()

    def wait(copies):
        for cp in copies:
            cp.wait()

    def remote(ph, st, q, src, dst, dev):
        return pltpu.make_async_remote_copy(src_ref=src, dst_ref=dst, send_sem=snd.at[ph, st], recv_sem=rcv.at[ph, st, q],
                                            device_id=dev, device_id_type=MESH)

    def stage(ph, k, q, sem_q):
        if k == 0:
            return [remote(ph, 0, sem_q, part.at[q, pl.ds(8 * (1 - core), 8)], r1.at[q], sib)]
        if k == 1:
            return [remote(ph, 1, sem_q, r1.at[q, pl.ds(2 * (1 - cx), 2)], r2.at[q, pl.ds(0, 2)], xn),
                    remote(ph, 2, sem_q, r1.at[q, pl.ds(4 + 2 * (1 - cy), 2)], r2.at[q, pl.ds(2, 2)], yn)]
        if k == 2:
            return [remote(ph, 3, sem_q, r2.at[q, pl.ds(1 - cy, 1)], r3.at[q, pl.ds(0, 1)], yn),
                    remote(ph, 4, sem_q, r2.at[q, pl.ds(2 + 1 - cx, 1)], r3.at[q, pl.ds(1, 1)], xn)]
        blk_a, blk_b = core * 8, core * 8 + 4
        if k == 3:
            a, b = full.at[q, pl.ds(blk_a + 2 * cx + cy, 1)], full.at[q, pl.ds(blk_b + 2 * cy + cx, 1)]
            return [remote(ph, 5, sem_q, a, a, yn), remote(ph, 6, sem_q, b, b, xn)]
        if k == 4:
            a, b = full.at[q, pl.ds(blk_a + 2 * cx, 2)], full.at[q, pl.ds(blk_b + 2 * cy, 2)]
            return [remote(ph, 7, sem_q, a, a, xn), remote(ph, 8, sem_q, b, b, yn)]
        a = full.at[q, pl.ds(blk_a, 8)]
        return [remote(ph, 9, sem_q, a, a, sib)]

    def one(ph, k, q):
        return stage(ph, k, q, q)

    def drain(ph, ks):
        for k in ks:
            for cp in stage(ph, k, slice(None), 0):
                cp.wait_send()

    def arrived(ph, k, q):
        for cp in one(ph, k, q):
            cp.wait_recv()

    def when(t, lo):
        return pl.when((t >= lo) & (t < lo + Q))

    def reduce_steps(ph, t, finish):
        @when(t, 1)
        def _():
            start(one(ph, 0, t - 1))

        @when(t, 2)
        def _():
            u = t - 2
            arrived(ph, 0, u)
            r1[u] = r1[u] + part[u, pl.ds(8 * core, 8)]
            start(one(ph, 1, u))

        @when(t, 4)
        def _():
            u = t - 4
            arrived(ph, 1, u)
            r2[u, pl.ds(0, 2)] = r2[u, pl.ds(0, 2)] + r1[u, pl.ds(2 * cx, 2)]
            r2[u, pl.ds(2, 2)] = r2[u, pl.ds(2, 2)] + r1[u, pl.ds(4 + 2 * cy, 2)]
            start(one(ph, 2, u))

        @when(t, 6)
        def _():
            u = t - 6
            arrived(ph, 2, u)
            finish(u, r3[u, 0] + r2[u, cy], r3[u, 1] + r2[u, 2 + cx])

    def gather_steps(ph, t, finish):
        @when(t, 0)
        def _():
            start(one(ph, 3, t))

        @when(t, 2)
        def _():
            arrived(ph, 3, t - 2)
            start(one(ph, 4, t - 2))

        @when(t, 4)
        def _():
            arrived(ph, 4, t - 4)
            start(one(ph, 5, t - 4))

        @when(t, 5)
        def _():
            arrived(ph, 5, t - 5)
            finish(t - 5)

    for q in range(WO_SLOTS):
        start(wo_copy(q))
    barrier = pltpu.get_barrier_semaphore()
    for dev in (sib, xn, yn):
        pl.semaphore_signal(barrier, inc=1, device_id=dev, device_id_type=MESH)
    pl.semaphore_wait(barrier, 3)
    acc_g[...] = jnp.zeros_like(acc_g)
    acc_u[...] = jnp.zeros_like(acc_u)

    def finish_attn(u, a, b):
        xres[u, 0] = (tok_ref[u, 0] + a).astype(jnp.bfloat16).astype(f32)
        xres[u, 1] = (tok_ref[u, 1] + b).astype(jnp.bfloat16).astype(f32)

    @pl.loop(0, Q + 6)
    def _(t):
        @when(t, 0)
        def _():
            wait(wo_copy(t))
            part[t] = jnp.dot(x_ref[...], wo[lax.rem(t, WO_SLOTS)], preferred_element_type=f32).reshape(16, 8, width)

            @pl.when(t + WO_SLOTS < Q)
            def _():
                start(wo_copy(t + WO_SLOTS))

            @pl.when(t < GU_SLOTS)
            def _():
                start(gu_copy(t))

            @pl.when((t >= GU_SLOTS) & (t < GU_SLOTS + WD_SLOTS))
            def _():
                start(wd_copy(t - GU_SLOTS))
        reduce_steps(0, t, finish_attn)

    drain(0, (0, 1, 2))
    sq = jnp.zeros((2, 8, 1), f32)
    for q in range(Q):
        sq = sq + jnp.sum(xres[q] * xres[q], axis=-1, keepdims=True)
    inv = lax.rsqrt(sq / (Q * width) + EPS)
    blk_a, blk_b = core * 8 + 2 * cx + cy, core * 8 + 4 + 2 * cy + cx
    for q in range(Q):
        h = (xres[q] * inv * ln_ref[q]).astype(jnp.bfloat16).astype(f32)
        full[q, blk_a] = h[0]
        full[q, blk_b] = h[1]

    def finish_gather(u):
        wait(gu_copy(u))
        s = lax.rem(u, GU_SLOTS)
        h = full[u].reshape(rows, width).astype(jnp.bfloat16)
        acc_g[...] += jnp.dot(h, wg[s], preferred_element_type=f32)
        acc_u[...] += jnp.dot(h, wu[s], preferred_element_type=f32)

        @pl.when(u + GU_SLOTS < Q)
        def _():
            start(gu_copy(u + GU_SLOTS))

    @pl.loop(0, Q + 5)
    def _(t):
        gather_steps(0, t, finish_gather)

    drain(0, (3, 4, 5))

    @pl.loop(0, acc_g.shape[1] // 640)
    def _(n):
        c = pl.ds(pl.multiple_of(n * 640, 640), 640)
        mact[:, c] = (jax.nn.silu(acc_g[:, c]) * acc_u[:, c]).astype(jnp.bfloat16)

    def finish_mlp(u, a, b):
        full[u, blk_a] = (xres[u, 0] + a).astype(jnp.bfloat16).astype(f32)
        full[u, blk_b] = (xres[u, 1] + b).astype(jnp.bfloat16).astype(f32)

    def finish_out(u):
        out_ref[:, cols(u)] = full[u].reshape(rows, width).astype(jnp.bfloat16)

    @pl.loop(0, Q + 12)
    def _(t):
        @when(t, 0)
        def _():
            wait(wd_copy(t))
            part[t] = jnp.dot(mact[...], wd[lax.rem(t, WD_SLOTS)], preferred_element_type=f32).reshape(16, 8, width)

            @pl.when(t + WD_SLOTS < Q)
            def _():
                start(wd_copy(t + WD_SLOTS))
        reduce_steps(1, t, finish_mlp)
        gather_steps(1, t - 7, finish_out)

    drain(1, (0, 1, 2, 3, 4, 5))


def tail(cid, attn_vals, tok_own, ln, w_out, w_gate, w_up, w_down):
    rows, depth = attn_vals.shape
    d_model, inner = w_gate.shape
    width = d_model // Q
    vmem = pl.BlockSpec(memory_space=pltpu.VMEM)
    hbm = pl.BlockSpec(memory_space=pl.ANY)
    f32, bf16 = jnp.float32, jnp.bfloat16
    dma = pltpu.SemaphoreType.DMA
    return pl.pallas_call(
        tail_kernel,
        out_shape=jax.ShapeDtypeStruct((rows, d_model), bf16),
        in_specs=[vmem, vmem, vmem, hbm, hbm, hbm, hbm],
        out_specs=vmem,
        scratch_shapes=[
            pltpu.VMEM((Q, 16, 8, width), f32),
            pltpu.VMEM((Q, 8, 8, width), f32),
            pltpu.VMEM((Q, 4, 8, width), f32),
            pltpu.VMEM((Q, 2, 8, width), f32),
            pltpu.VMEM((Q, 16, 8, width), f32),
            pltpu.VMEM((Q, 2, 8, width), f32),
            pltpu.VMEM((rows, inner), f32),
            pltpu.VMEM((rows, inner), f32),
            pltpu.VMEM((rows, inner), bf16),
            pltpu.VMEM((WO_SLOTS, depth, width), bf16),
            pltpu.VMEM((GU_SLOTS, width, inner), bf16),
            pltpu.VMEM((GU_SLOTS, width, inner), bf16),
            pltpu.VMEM((WD_SLOTS, inner, width), bf16),
            dma((WO_SLOTS,)), dma((GU_SLOTS,)), dma((GU_SLOTS,)), dma((WD_SLOTS,)),
            dma((2, 10)), dma((2, 10, Q)),
        ],
        compiler_params=pltpu.CompilerParams(collective_id=cid, has_side_effects=True, vmem_limit_bytes=62 * 1024 * 1024),
        name="tail",
    )(attn_vals, tok_own, ln, w_out, w_gate, w_up, w_down)


def solution(mesh):
    dim_count = mesh.shape['dim']
    mlp_axes = ('heads', 'dim')
    swap_perm = [(src, (src + dim_count // 2) % dim_count) for src in range(dim_count)]

    def layer_body(tokens, ln_attn, w_query, w_key, w_value, q_gain, k_gain, w_out, ln_mlp, w_gate, w_up, w_down, k_cache, v_cache, positions):
        rows = tokens.shape[0]
        heads_local = w_query.shape[1]
        kv_local = w_key.shape[1]
        slice_len = w_query.shape[2]
        head_dim = slice_len * dim_count
        half_dim = head_dim // 2
        q_group = heads_local // kv_local
        cache_len = k_cache.shape[1]
        up_blocks = (cache_len - LOW) // BLK
        dim_index = lax.axis_index('dim')

        hidden = rms_scale(tokens.astype(jnp.float32), ln_attn).astype(jnp.bfloat16)
        q_part = jnp.einsum('bd,dhs->bhs', hidden, w_query, preferred_element_type=jnp.float32)
        k_part = jnp.einsum('bd,dhs->bhs', hidden, w_key, preferred_element_type=jnp.float32)
        v_new = jnp.einsum('bd,dhs->bhs', hidden, w_value, preferred_element_type=jnp.float32).astype(jnp.bfloat16)

        own = jnp.concatenate([q_part, k_part], axis=1)
        other = lax.ppermute(own, 'dim', swap_perm)
        gains = jnp.stack([q_gain, k_gain])
        gains_other = lax.ppermute(gains, 'dim', swap_perm)
        sq_total = jnp.sum(own * own, axis=-1, keepdims=True) + jnp.sum(other * other, axis=-1, keepdims=True)
        inv = lax.rsqrt(sq_total / head_dim + EPS)

        def spread(pair):
            return jnp.concatenate([jnp.broadcast_to(pair[0], (heads_local, slice_len)), jnp.broadcast_to(pair[1], (kv_local, slice_len))], axis=0)

        u_own = own * inv * spread(gains)
        u_other = other * inv * spread(gains_other)
        inv_freq = ROPE_BASE ** (-jnp.arange(half_dim, dtype=jnp.float32) * 2.0 / head_dim)
        rot_angle = positions.astype(jnp.float32)[:, None, None] * inv_freq
        cos_t = jnp.cos(rot_angle)
        sin_t = jnp.where(dim_index == 0, -1.0, 1.0) * jnp.sin(rot_angle)
        r_own = (u_own * cos_t + u_other * sin_t).astype(jnp.bfloat16)
        r_other = (u_other * cos_t - u_own * sin_t).astype(jnp.bfloat16)
        k_new = r_own[:, heads_local:]
        qf = jnp.concatenate([r_own[:, :heads_local], r_other[:, :heads_local]], axis=-1)
        kf = jnp.concatenate([k_new, r_other[:, heads_local:]], axis=-1).astype(jnp.float32)
        zeros = jnp.zeros((rows, q_group, slice_len), jnp.bfloat16)
        qd = jnp.concatenate([
            jnp.concatenate([r_own[:, :q_group], zeros], axis=-1),
            jnp.concatenate([zeros, r_own[:, q_group:heads_local]], axis=-1)], axis=1)
        vn = v_new.reshape(rows, kv_local * slice_len).astype(jnp.float32)

        n_blk = (positions - LOW + BLK - 1) // BLK
        cum = jnp.cumsum(n_blk)
        off = cum - n_blk
        slot = jnp.arange(rows * up_blocks)
        row_of = jnp.sum((cum[None, :] <= slot[:, None]).astype(jnp.int32), axis=1)
        off_of = jnp.sum(jnp.where(row_of[:, None] == jnp.arange(rows)[None, :], off[None, :], 0), axis=1)
        idx = jnp.where(row_of < rows, row_of * up_blocks + slot - off_of, 0)

        k_t = k_cache.transpose(0, 2, 3, 1).reshape(rows, kv_local * slice_len, cache_len)
        v_t = v_cache.transpose(0, 2, 3, 1).reshape(rows, kv_local * slice_len, cache_len)
        which = jnp.sum((cum[-1] > jnp.array(UP_SIZES[:-1])).astype(jnp.int32))
        branches = [functools.partial(attend, n, i, head_dim ** -0.5) for i, n in enumerate(UP_SIZES)]
        attn = lax.switch(which, branches, positions, off, idx, qd, qf, kf, vn, k_t, v_t)
        attn_vals = attn.reshape(rows, q_group, kv_local, slice_len).transpose(0, 2, 1, 3).reshape(rows, heads_local, slice_len)

        attn_vals = attn_vals.reshape(rows, heads_local * slice_len)
        heads_index = lax.axis_index('heads')
        core, cx = heads_index % 2, heads_index // 2
        tok_blocks = tokens.reshape(16, 8, Q, -1)
        tok_own = jnp.stack([lax.dynamic_index_in_dim(tok_blocks, core * 8 + 2 * cx + dim_index, 0, keepdims=False),
                             lax.dynamic_index_in_dim(tok_blocks, core * 8 + 4 + 2 * dim_index + cx, 0, keepdims=False)])
        tok_own = tok_own.astype(jnp.float32).transpose(2, 0, 1, 3)
        out = tail(len(UP_SIZES), attn_vals, tok_own, ln_mlp.reshape(Q, 1, -1), w_out.reshape(heads_local * slice_len, -1), w_gate, w_up, w_down)
        return out, k_new, v_new

    row_spec = P('dp', None)
    head_spec = P(None, 'heads', 'dim')
    cache_spec = P('dp', None, 'heads', 'dim')
    new_spec = P('dp', 'heads', 'dim')
    in_specs = (row_spec, P(None), head_spec, head_spec, head_spec, P('dim'), P('dim'), P('heads', 'dim', None), P(None), P(None, mlp_axes), P(None, mlp_axes), P(mlp_axes, None), cache_spec, cache_spec, P('dp'))
    out_specs = (row_spec, new_spec, new_spec)
    return jax.shard_map(layer_body, mesh=mesh, in_specs=in_specs, out_specs=out_specs, check_vma=False)
```

```python
import functools

import jax
import jax.numpy as jnp
from jax import lax
from jax.experimental import pallas as pl
from jax.experimental.pallas import tpu as pltpu
from jax.sharding import PartitionSpec as P

EPS = 1e-6
ROPE_BASE = 1000000.0
MESH = pl.DeviceIdType.MESH

BLK = 128
LOW = 512
CH = 4
UCH = 8
UNIT = 32
SLOTS = 4
FIRST = 8
LEAD = 4
UP_SIZES = (240, 256, 264, 272, 280, 288, 304, 512)


def qkv_kernel(group, tok_ref, ln_ref, cos_ref, sin_ref, gain_ref, wq_hbm, wk_hbm, wv_hbm, qd_ref, sn_ref, vn_ref, kn_ref,
               hid, wq, wk, wv, own, other, gain_other, wsem, snd, rcv):
    partner = {"dim": 1 - lax.axis_index("dim")}
    rows, depth = tok_ref.shape
    n_q = own.shape[0] - 1
    steps = n_q // 2
    f32, bf16 = jnp.float32, jnp.bfloat16
    half = BLK // 2
    per_step = wq.shape[0] // steps

    def wq_copy(c):
        part = pl.ds(pl.multiple_of(c * per_step, per_step), per_step)
        return pltpu.make_async_copy(wq_hbm.at[part], wq.at[part], wsem.at[c])

    k_load = pltpu.make_async_copy(wk_hbm, wk, wsem.at[steps])
    v_load = pltpu.make_async_copy(wv_hbm, wv, wsem.at[steps + 1])

    def remote(src, dst, i):
        return pltpu.make_async_remote_copy(src_ref=src, dst_ref=dst, send_sem=snd.at[i], recv_sem=rcv.at[i],
                                            device_id=partner, device_id_type=MESH)

    def q_copy(c):
        part = pl.ds(2 * c, 2)
        return remote(own.at[part], other.at[part], c)

    k_copy = remote(own.at[pl.ds(n_q, 1)], other.at[pl.ds(n_q, 1)], steps)
    g_copy = remote(gain_ref, gain_other, steps + 1)

    k_load.start()
    for c in range(steps):
        wq_copy(c).start()
    v_load.start()
    barrier = pltpu.get_barrier_semaphore()
    pl.semaphore_signal(barrier, inc=1, device_id=partner, device_id_type=MESH)
    pl.semaphore_wait(barrier, 1)
    g_copy.start()

    @pl.loop(0, rows // 16)
    def _(i):
        part = pl.ds(pl.multiple_of(i * 16, 16), 16)
        x = tok_ref[part, :].astype(f32)
        inv = lax.rsqrt(jnp.mean(x * x, axis=-1, keepdims=True) + EPS)
        hid[part, :] = (x * inv * ln_ref[...]).astype(bf16)

    def project(w):
        return lax.dot_general(hid[...], w, (((1,), (1,)), ((), ())), preferred_element_type=f32)

    k_load.wait()
    own[n_q] = project(wk[...])

    @pl.loop(0, steps)
    def _(c):
        wq_copy(c).wait()
        u = project(wq[pl.ds(pl.multiple_of(c * per_step, per_step), per_step), :])

        @pl.when(c == 0)
        def _():
            k_copy.start()

        own[2 * c] = u[:, :BLK]
        own[2 * c + 1] = u[:, BLK:]
        q_copy(c).start()

    v_load.wait()
    vn_ref[...] = project(wv[...]).astype(bf16).astype(f32)
    low = lax.broadcasted_iota(jnp.int32, (rows, BLK), 1) < half
    cos_t, sin_t = cos_ref[...], sin_ref[...]

    def halves(x):
        return (jnp.sum(jnp.where(low, x, 0.0), axis=-1, keepdims=True), jnp.sum(jnp.where(low, 0.0, x), axis=-1, keepdims=True))

    def rotate(i, g):
        a, b = own[i], other[i]
        s_lo, s_hi = halves(a * a + b * b)
        inv = jnp.where(low, lax.rsqrt(s_lo / BLK + EPS), lax.rsqrt(s_hi / BLK + EPS))
        a, b = a * inv * gain_ref[g:g + 1, :], b * inv * gain_other[g:g + 1, :]
        return (a * cos_t + b * sin_t).astype(bf16).astype(f32), (b * cos_t - a * sin_t).astype(bf16).astype(f32)

    g_copy.wait_recv()
    k_copy.wait_recv()
    k_own, k_oth = rotate(n_q, 1)
    kn_ref[...] = k_own.astype(bf16)
    kr_own, kr_oth = pltpu.roll(k_own, half, 1), pltpu.roll(k_oth, half, 1)
    kk = [(jnp.where(low, k_own, kr_own), jnp.where(low, k_oth, kr_oth)),
          (jnp.where(low, kr_own, k_own), jnp.where(low, kr_oth, k_oth))]
    for i in range(n_q):
        if i % 2 == 0:
            q_copy(i // 2).wait_recv()
        q_own, q_oth = rotate(i, 0)
        kv = 2 * i // group
        new = halves(q_own * kk[kv][0] + q_oth * kk[kv][1])
        turned = pltpu.roll(q_own, half, 1)
        for e in range(2):
            sn_ref[:, 2 * i + e, :] = jnp.broadcast_to(new[e], (rows, BLK))
            val = q_own if e == kv else turned
            qd_ref[:, 2 * i + e, :] = jnp.where(low, val, 0.0) if kv == 0 else jnp.where(low, 0.0, val)
    for c in range(steps):
        q_copy(c).wait_send()
    k_copy.wait_send()
    g_copy.wait_send()


def qkv(cid, group, tokens, ln, cos_t, sin_t, gain, w_q, w_k, w_v):
    rows, depth = tokens.shape
    n_q = w_q.shape[0] // BLK
    steps = n_q // 2
    vmem = pl.BlockSpec(memory_space=pltpu.VMEM)
    hbm = pl.BlockSpec(memory_space=pl.ANY)
    f32, bf16 = jnp.float32, jnp.bfloat16
    heads = 2 * n_q
    dma = pltpu.SemaphoreType.DMA
    return pl.pallas_call(
        functools.partial(qkv_kernel, group),
        out_shape=(jax.ShapeDtypeStruct((rows, heads, BLK), f32), jax.ShapeDtypeStruct((rows, heads, BLK), f32),
                   jax.ShapeDtypeStruct((rows, BLK), f32), jax.ShapeDtypeStruct((rows, BLK), bf16)),
        in_specs=[vmem] * 5 + [hbm] * 3,
        out_specs=(vmem,) * 4,
        scratch_shapes=[
            pltpu.VMEM((rows, depth), bf16),
            pltpu.VMEM(w_q.shape, bf16),
            pltpu.VMEM(w_k.shape, bf16),
            pltpu.VMEM(w_v.shape, bf16),
            pltpu.VMEM((n_q + 1, rows, BLK), f32),
            pltpu.VMEM((n_q + 1, rows, BLK), f32),
            pltpu.VMEM(gain.shape, f32),
            dma((steps + 2,)), dma((steps + 2,)), dma((steps + 2,)),
        ],
        compiler_params=pltpu.CompilerParams(collective_id=cid, has_side_effects=True, vmem_limit_bytes=32 * 1024 * 1024),
        name="qkv",
    )(tokens, ln, cos_t, sin_t, gain, w_q, w_k, w_v)


def attn_kernel(n_up, scale, pos_ref, off_ref, idx_ref, qd_ref, sn_ref, vn_ref, k_hbm, v_hbm, o_ref,
                kbuf, vbuf, own_lo, own_up, pack, rlo, rup, ksem, vsem, slo_s, slo_r, sup_s, sup_r):
    partner = {"dim": 1 - lax.axis_index("dim")}
    rows = qd_ref.shape[0]
    n_ch = rows // CH
    n_uch = n_up // UCH
    up_blocks = own_up.shape[0] // rows
    per_blk = BLK // UNIT
    lane_up = lax.broadcasted_iota(jnp.int32, (16, BLK), 1)

    def kcopy(c):
        return pltpu.make_async_copy(k_hbm.at[pl.ds(c * CH, CH)], kbuf.at[lax.rem(c, SLOTS)], ksem.at[lax.rem(c, SLOTS)])

    def vcopy(c):
        return pltpu.make_async_copy(v_hbm.at[pl.ds(c * CH, CH)], vbuf.at[lax.rem(c, SLOTS)], vsem.at[lax.rem(c, SLOTS)])

    def lo_copy(c):
        part = pl.ds(c * CH, CH)
        return pltpu.make_async_remote_copy(src_ref=own_lo.at[part], dst_ref=rlo.at[part], send_sem=slo_s.at[c],
                                            recv_sem=slo_r.at[c], device_id=partner, device_id_type=MESH)

    def up_copy(c):
        part = pl.ds(c * UCH, UCH)
        return pltpu.make_async_remote_copy(src_ref=pack.at[part], dst_ref=rup.at[part], send_sem=sup_s.at[c],
                                            recv_sem=sup_r.at[c], device_id=partner, device_id_type=MESH)

    for c in range(SLOTS):
        kcopy(c).start()
    barrier = pltpu.get_barrier_semaphore()
    pl.semaphore_signal(barrier, inc=1, device_id=partner, device_id_type=MESH)
    pl.semaphore_wait(barrier, 1)
    for c in range(SLOTS):
        vcopy(c).start()

    @pl.loop(0, n_ch)
    def _(c):
        kcopy(c).wait()
        for r in range(CH):
            b = c * CH + r
            s = jnp.dot(qd_ref[b].astype(jnp.bfloat16), kbuf[lax.rem(c, SLOTS), r], preferred_element_type=jnp.float32)
            own_lo[b] = s[:, :LOW]
            for j in range(up_blocks):
                own_up[b * up_blocks + j] = s[:, LOW + j * BLK:LOW + (j + 1) * BLK]

        @pl.when(c + SLOTS < n_ch)
        def _():
            kcopy(c + SLOTS).start()

        @pl.when((c >= 1) & (c <= FIRST))
        def _():
            lo_copy(c - 1).start()

    @pl.loop(0, n_uch + 1)
    def _(c):
        @pl.when(c < n_uch)
        def _():
            for r in range(UCH):
                j = c * UCH + r
                block = None
                for k in range(per_blk):
                    src = idx_ref[j * per_blk + k]
                    piece = pltpu.roll(own_up[src // per_blk], (k + per_blk - src % per_blk) % per_blk * UNIT, 1)
                    block = piece if k == 0 else jnp.where(lane_up >= k * UNIT, piece, block)
                pack[j] = block

        @pl.when(c >= 1)
        def _():
            up_copy(c - 1).start()

    @pl.loop(FIRST, FIRST + LEAD)
    def _(c):
        lo_copy(c).start()

    @pl.loop(0, n_uch)
    def _(c):
        up_copy(c).wait_recv()

    lane = lax.broadcasted_iota(jnp.int32, (8, 2 * 64), 1)
    t_up = lane_up + LOW

    @pl.loop(0, n_ch)
    def _(c):
        @pl.when(c + FIRST + LEAD < n_ch)
        def _():
            lo_copy(c + FIRST + LEAD).start()

        vcopy(c).wait()
        lo_copy(c).wait_recv()
        for r in range(CH):
            b = c * CH + r
            pos = pos_ref[b]
            off = off_ref[b]
            parts = [(own_lo[b] + rlo[b]) * scale]
            skew = off % per_blk * UNIT
            slots = [pltpu.roll(rup[jnp.minimum(off // per_blk + j, n_up - 1)], (BLK - skew) % BLK, 1) for j in range(up_blocks + 1)]
            for j in range(up_blocks):
                got = jnp.where(lane_up < BLK - skew, slots[j], slots[j + 1])
                total = (own_up[b * up_blocks + j] + got) * scale
                parts.append(jnp.where(t_up + j * BLK < pos, total, -jnp.inf))
            s = jnp.concatenate(parts, axis=1)
            s_new = sn_ref[b][:, 0:1] * scale
            m = jnp.maximum(jnp.max(s, axis=1, keepdims=True), s_new)
            e = jnp.exp(s - m)
            e_new = jnp.exp(s_new - m)
            inv = 1.0 / (jnp.sum(e, axis=1, keepdims=True) + e_new)
            p = (e * inv).astype(jnp.bfloat16)
            p_new = (e_new * inv).astype(jnp.bfloat16).astype(jnp.float32)
            o = lax.dot_general(p, vbuf[lax.rem(c, SLOTS), r], (((1,), (1,)), ((), ())), preferred_element_type=jnp.float32)
            o = o + p_new * vn_ref[pl.ds(b, 1), :]
            o_ref[b] = jnp.where(lane < 64, o[0:8], o[8:16]).astype(jnp.bfloat16)

        @pl.when(c + SLOTS < n_ch)
        def _():
            vcopy(c + SLOTS).start()

    @pl.loop(0, n_ch)
    def _(c):
        lo_copy(c).wait_send()

    @pl.loop(0, n_uch)
    def _(c):
        up_copy(c).wait_send()


def attend(n_up, cid, scale, pos, off, idx, qd, sn, vn, k_t, v_t):
    rows = qd.shape[0]
    n_ch = rows // CH
    n_uch = n_up // UCH
    cache_len = k_t.shape[2]
    up_blocks = (cache_len - LOW) // BLK
    smem = pl.BlockSpec(memory_space=pltpu.SMEM)
    vmem = pl.BlockSpec(memory_space=pltpu.VMEM)
    hbm = pl.BlockSpec(memory_space=pl.ANY)
    return pl.pallas_call(
        functools.partial(attn_kernel, n_up, scale),
        out_shape=jax.ShapeDtypeStruct((rows, 8, 128), jnp.bfloat16),
        in_specs=[smem, smem, smem, vmem, vmem, vmem, hbm, hbm],
        out_specs=vmem,
        scratch_shapes=[
            pltpu.VMEM((SLOTS, CH, 128, cache_len), jnp.bfloat16),
            pltpu.VMEM((SLOTS, CH, 128, cache_len), jnp.bfloat16),
            pltpu.VMEM((rows, 16, LOW), jnp.float32),
            pltpu.VMEM((rows * up_blocks, 16, BLK), jnp.float32),
            pltpu.VMEM((n_up, 16, BLK), jnp.float32),
            pltpu.VMEM((rows, 16, LOW), jnp.float32),
            pltpu.VMEM((n_up, 16, BLK), jnp.float32),
            pltpu.SemaphoreType.DMA((SLOTS,)),
            pltpu.SemaphoreType.DMA((SLOTS,)),
            pltpu.SemaphoreType.DMA((n_ch,)),
            pltpu.SemaphoreType.DMA((n_ch,)),
            pltpu.SemaphoreType.DMA((n_uch,)),
            pltpu.SemaphoreType.DMA((n_uch,)),
        ],
        compiler_params=pltpu.CompilerParams(collective_id=cid, has_side_effects=True, vmem_limit_bytes=40 * 1024 * 1024),
        name=f"attend_{n_up}",
    )(pos, off, idx, qd, sn, vn, k_t, v_t)


Q = 10
WO_SLOTS = 4
GU_SLOTS = 4
WD_SLOTS = 4


def tail_kernel(x_ref, tok_ref, ln_ref, wo_hbm, wg_hbm, wu_hbm, wd_hbm, out_ref,
                part, r1, r2, r3, full, xres, acc_g, acc_u, mact, wo, wg, wu, wd,
                wo_s, wg_s, wu_s, wd_s, snd, rcv):
    heads = lax.axis_index("heads")
    core, cx, cy = lax.rem(heads, 2), heads // 2, lax.axis_index("dim")
    sib = {"heads": 2 * cx + 1 - core}
    xn = {"heads": 2 * (1 - cx) + core}
    yn = {"dim": 1 - cy}
    width = part.shape[3]
    rows = 16 * 8
    f32 = jnp.float32

    def cols(q):
        return pl.ds(pl.multiple_of(q * width, width), width)

    def wo_copy(q):
        s = lax.rem(q, WO_SLOTS)
        return [pltpu.make_async_copy(wo_hbm.at[:, cols(q)], wo.at[s], wo_s.at[s])]

    def gu_copy(q):
        s = lax.rem(q, GU_SLOTS)
        return [pltpu.make_async_copy(wg_hbm.at[cols(q)], wg.at[s], wg_s.at[s]),
                pltpu.make_async_copy(wu_hbm.at[cols(q)], wu.at[s], wu_s.at[s])]

    def wd_copy(q):
        s = lax.rem(q, WD_SLOTS)
        return [pltpu.make_async_copy(wd_hbm.at[:, cols(q)], wd.at[s], wd_s.at[s])]

    def start(copies):
        for cp in copies:
            cp.start()

    def wait(copies):
        for cp in copies:
            cp.wait()

    def remote(ph, st, q, src, dst, dev):
        return pltpu.make_async_remote_copy(src_ref=src, dst_ref=dst, send_sem=snd.at[ph, st], recv_sem=rcv.at[ph, st, q],
                                            device_id=dev, device_id_type=MESH)

    def stage(ph, k, q, sem_q):
        if k == 0:
            return [remote(ph, 0, sem_q, part.at[q, pl.ds(8 * (1 - core), 8)], r1.at[q], sib)]
        if k == 1:
            return [remote(ph, 1, sem_q, r1.at[q, pl.ds(2 * (1 - cx), 2)], r2.at[q, pl.ds(0, 2)], xn),
                    remote(ph, 2, sem_q, r1.at[q, pl.ds(4 + 2 * (1 - cy), 2)], r2.at[q, pl.ds(2, 2)], yn)]
        if k == 2:
            return [remote(ph, 3, sem_q, r2.at[q, pl.ds(1 - cy, 1)], r3.at[q, pl.ds(0, 1)], yn),
                    remote(ph, 4, sem_q, r2.at[q, pl.ds(2 + 1 - cx, 1)], r3.at[q, pl.ds(1, 1)], xn)]
        blk_a, blk_b = core * 8, core * 8 + 4
        if k == 3:
            a, b = full.at[q, pl.ds(blk_a + 2 * cx + cy, 1)], full.at[q, pl.ds(blk_b + 2 * cy + cx, 1)]
            return [remote(ph, 5, sem_q, a, a, yn), remote(ph, 6, sem_q, b, b, xn)]
        if k == 4:
            a, b = full.at[q, pl.ds(blk_a + 2 * cx, 2)], full.at[q, pl.ds(blk_b + 2 * cy, 2)]
            return [remote(ph, 7, sem_q, a, a, xn), remote(ph, 8, sem_q, b, b, yn)]
        a = full.at[q, pl.ds(blk_a, 8)]
        return [remote(ph, 9, sem_q, a, a, sib)]

    def one(ph, k, q):
        return stage(ph, k, q, q)

    def drain(ph, ks):
        for k in ks:
            for cp in stage(ph, k, slice(None), 0):
                cp.wait_send()

    def arrived(ph, k, q):
        for cp in one(ph, k, q):
            cp.wait_recv()

    def when(t, lo):
        return pl.when((t >= lo) & (t < lo + Q))

    def reduce_steps(ph, t, finish):
        @when(t, 1)
        def _():
            start(one(ph, 0, t - 1))

        @when(t, 2)
        def _():
            u = t - 2
            arrived(ph, 0, u)
            r1[u] = r1[u] + part[u, pl.ds(8 * core, 8)]
            start(one(ph, 1, u))

        @when(t, 4)
        def _():
            u = t - 4
            arrived(ph, 1, u)
            r2[u, pl.ds(0, 2)] = r2[u, pl.ds(0, 2)] + r1[u, pl.ds(2 * cx, 2)]
            r2[u, pl.ds(2, 2)] = r2[u, pl.ds(2, 2)] + r1[u, pl.ds(4 + 2 * cy, 2)]
            start(one(ph, 2, u))

        @when(t, 6)
        def _():
            u = t - 6
            arrived(ph, 2, u)
            finish(u, r3[u, 0] + r2[u, cy], r3[u, 1] + r2[u, 2 + cx])

    def gather_steps(ph, t, finish):
        @when(t, 0)
        def _():
            start(one(ph, 3, t))

        @when(t, 2)
        def _():
            arrived(ph, 3, t - 2)
            start(one(ph, 4, t - 2))

        @when(t, 4)
        def _():
            arrived(ph, 4, t - 4)
            start(one(ph, 5, t - 4))

        @when(t, 5)
        def _():
            arrived(ph, 5, t - 5)
            finish(t - 5)

    for q in range(WO_SLOTS):
        start(wo_copy(q))
    barrier = pltpu.get_barrier_semaphore()
    for dev in (sib, xn, yn):
        pl.semaphore_signal(barrier, inc=1, device_id=dev, device_id_type=MESH)
    pl.semaphore_wait(barrier, 3)
    acc_g[...] = jnp.zeros_like(acc_g)
    acc_u[...] = jnp.zeros_like(acc_u)

    def finish_attn(u, a, b):
        xres[u, 0] = (tok_ref[u, 0] + a).astype(jnp.bfloat16).astype(f32)
        xres[u, 1] = (tok_ref[u, 1] + b).astype(jnp.bfloat16).astype(f32)

    @pl.loop(0, Q + 6)
    def _(t):
        @when(t, 0)
        def _():
            wait(wo_copy(t))
            part[t] = jnp.dot(x_ref[...], wo[lax.rem(t, WO_SLOTS)], preferred_element_type=f32).reshape(16, 8, width)

            @pl.when(t + WO_SLOTS < Q)
            def _():
                start(wo_copy(t + WO_SLOTS))

            @pl.when(t < GU_SLOTS)
            def _():
                start(gu_copy(t))

            @pl.when((t >= GU_SLOTS) & (t < GU_SLOTS + WD_SLOTS))
            def _():
                start(wd_copy(t - GU_SLOTS))
        reduce_steps(0, t, finish_attn)

    drain(0, (0, 1, 2))
    sq = jnp.zeros((2, 8, 1), f32)
    for q in range(Q):
        sq = sq + jnp.sum(xres[q] * xres[q], axis=-1, keepdims=True)
    inv = lax.rsqrt(sq / (Q * width) + EPS)
    blk_a, blk_b = core * 8 + 2 * cx + cy, core * 8 + 4 + 2 * cy + cx
    for q in range(Q):
        h = (xres[q] * inv * ln_ref[q]).astype(jnp.bfloat16).astype(f32)
        full[q, blk_a] = h[0]
        full[q, blk_b] = h[1]

    def finish_gather(u):
        wait(gu_copy(u))
        s = lax.rem(u, GU_SLOTS)
        h = full[u].reshape(rows, width).astype(jnp.bfloat16)
        acc_g[...] += jnp.dot(h, wg[s], preferred_element_type=f32)
        acc_u[...] += jnp.dot(h, wu[s], preferred_element_type=f32)

        @pl.when(u + GU_SLOTS < Q)
        def _():
            start(gu_copy(u + GU_SLOTS))

    @pl.loop(0, Q + 5)
    def _(t):
        gather_steps(0, t, finish_gather)

    drain(0, (3, 4, 5))

    @pl.loop(0, acc_g.shape[1] // 640)
    def _(n):
        c = pl.ds(pl.multiple_of(n * 640, 640), 640)
        mact[:, c] = (jax.nn.silu(acc_g[:, c]) * acc_u[:, c]).astype(jnp.bfloat16)

    def finish_mlp(u, a, b):
        full[u, blk_a] = (xres[u, 0] + a).astype(jnp.bfloat16).astype(f32)
        full[u, blk_b] = (xres[u, 1] + b).astype(jnp.bfloat16).astype(f32)

    def finish_out(u):
        out_ref[:, cols(u)] = full[u].reshape(rows, width).astype(jnp.bfloat16)

    @pl.loop(0, Q + 12)
    def _(t):
        @when(t, 0)
        def _():
            wait(wd_copy(t))
            part[t] = jnp.dot(mact[...], wd[lax.rem(t, WD_SLOTS)], preferred_element_type=f32).reshape(16, 8, width)

            @pl.when(t + WD_SLOTS < Q)
            def _():
                start(wd_copy(t + WD_SLOTS))
        reduce_steps(1, t, finish_mlp)
        gather_steps(1, t - 7, finish_out)

    drain(1, (0, 1, 2, 3, 4, 5))


def tail(cid, attn_vals, tok_own, ln, w_out, w_gate, w_up, w_down):
    rows, depth = attn_vals.shape
    d_model, inner = w_gate.shape
    width = d_model // Q
    vmem = pl.BlockSpec(memory_space=pltpu.VMEM)
    hbm = pl.BlockSpec(memory_space=pl.ANY)
    f32, bf16 = jnp.float32, jnp.bfloat16
    dma = pltpu.SemaphoreType.DMA
    return pl.pallas_call(
        tail_kernel,
        out_shape=jax.ShapeDtypeStruct((rows, d_model), bf16),
        in_specs=[vmem, vmem, vmem, hbm, hbm, hbm, hbm],
        out_specs=vmem,
        scratch_shapes=[
            pltpu.VMEM((Q, 16, 8, width), f32),
            pltpu.VMEM((Q, 8, 8, width), f32),
            pltpu.VMEM((Q, 4, 8, width), f32),
            pltpu.VMEM((Q, 2, 8, width), f32),
            pltpu.VMEM((Q, 16, 8, width), f32),
            pltpu.VMEM((Q, 2, 8, width), f32),
            pltpu.VMEM((rows, inner), f32),
            pltpu.VMEM((rows, inner), f32),
            pltpu.VMEM((rows, inner), bf16),
            pltpu.VMEM((WO_SLOTS, depth, width), bf16),
            pltpu.VMEM((GU_SLOTS, width, inner), bf16),
            pltpu.VMEM((GU_SLOTS, width, inner), bf16),
            pltpu.VMEM((WD_SLOTS, inner, width), bf16),
            dma((WO_SLOTS,)), dma((GU_SLOTS,)), dma((GU_SLOTS,)), dma((WD_SLOTS,)),
            dma((2, 10)), dma((2, 10, Q)),
        ],
        compiler_params=pltpu.CompilerParams(collective_id=cid, has_side_effects=True, vmem_limit_bytes=62 * 1024 * 1024),
        name="tail",
    )(attn_vals, tok_own, ln, w_out, w_gate, w_up, w_down)


def solution(mesh):
    dim_count = mesh.shape['dim']
    mlp_axes = ('heads', 'dim')

    def layer_body(tokens, ln_attn, w_query, w_key, w_value, q_gain, k_gain, w_out, ln_mlp, w_gate, w_up, w_down, k_cache, v_cache, positions):
        rows = tokens.shape[0]
        heads_local = w_query.shape[1]
        kv_local = w_key.shape[1]
        slice_len = w_query.shape[2]
        head_dim = slice_len * dim_count
        half_dim = head_dim // 2
        q_group = heads_local // kv_local
        cache_len = k_cache.shape[1]
        up_blocks = (cache_len - LOW) // BLK
        dim_index = lax.axis_index('dim')

        inv_freq = ROPE_BASE ** (-jnp.arange(half_dim, dtype=jnp.float32) * 2.0 / head_dim)
        rot_angle = positions.astype(jnp.float32)[:, None] * jnp.tile(inv_freq, 2)
        cos_t = jnp.cos(rot_angle)
        sin_t = jnp.where(dim_index == 0, -1.0, 1.0) * jnp.sin(rot_angle)
        gain = jnp.concatenate([jnp.stack([jnp.tile(q_gain, 2), jnp.tile(k_gain, 2)]), jnp.zeros((6, head_dim), jnp.float32)])

        def by_column(w):
            return w.transpose(1, 2, 0).reshape(-1, w.shape[0])

        qd, sn, vn, kn = qkv(len(UP_SIZES) + 1, q_group, tokens, ln_attn[None], cos_t, sin_t, gain,
                             by_column(w_query), by_column(w_key), by_column(w_value))
        k_new = kn.reshape(rows, kv_local, slice_len)
        v_new = vn.astype(jnp.bfloat16).reshape(rows, kv_local, slice_len)

        row_units = up_blocks * BLK // UNIT
        n_units = (positions - LOW + UNIT - 1) // UNIT
        cum = jnp.cumsum(n_units)
        off = cum - n_units
        unit = jnp.arange(rows * row_units)
        row_of = jnp.sum((cum[None, :] <= unit[:, None]).astype(jnp.int32), axis=1)
        off_of = jnp.sum(jnp.where(row_of[:, None] == jnp.arange(rows)[None, :], off[None, :], 0), axis=1)
        idx = jnp.where(row_of < rows, row_of * row_units + unit - off_of, 0)

        k_t = k_cache.transpose(0, 2, 3, 1).reshape(rows, kv_local * slice_len, cache_len)
        v_t = v_cache.transpose(0, 2, 3, 1).reshape(rows, kv_local * slice_len, cache_len)
        which = jnp.sum((cum[-1] > jnp.array(UP_SIZES[:-1]) * (BLK // UNIT)).astype(jnp.int32))
        branches = [functools.partial(attend, n, i, head_dim ** -0.5) for i, n in enumerate(UP_SIZES)]
        attn = lax.switch(which, branches, positions, off, idx, qd, sn, vn, k_t, v_t)
        attn_vals = attn.reshape(rows, q_group, kv_local, slice_len).transpose(0, 2, 1, 3).reshape(rows, heads_local, slice_len)

        attn_vals = attn_vals.reshape(rows, heads_local * slice_len)
        heads_index = lax.axis_index('heads')
        core, cx = heads_index % 2, heads_index // 2
        tok_blocks = tokens.reshape(16, 8, Q, -1)
        tok_own = jnp.stack([lax.dynamic_index_in_dim(tok_blocks, core * 8 + 2 * cx + dim_index, 0, keepdims=False),
                             lax.dynamic_index_in_dim(tok_blocks, core * 8 + 4 + 2 * dim_index + cx, 0, keepdims=False)])
        tok_own = tok_own.astype(jnp.float32).transpose(2, 0, 1, 3)
        out = tail(len(UP_SIZES), attn_vals, tok_own, ln_mlp.reshape(Q, 1, -1), w_out.reshape(heads_local * slice_len, -1), w_gate, w_up, w_down)
        return out, k_new, v_new

    row_spec = P('dp', None)
    head_spec = P(None, 'heads', 'dim')
    cache_spec = P('dp', None, 'heads', 'dim')
    new_spec = P('dp', 'heads', 'dim')
    in_specs = (row_spec, P(None), head_spec, head_spec, head_spec, P('dim'), P('dim'), P('heads', 'dim', None), P(None), P(None, mlp_axes), P(None, mlp_axes), P(mlp_axes, None), cache_spec, cache_spec, P('dp'))
    out_specs = (row_spec, new_spec, new_spec)
    return jax.shard_map(layer_body, mesh=mesh, in_specs=in_specs, out_specs=out_specs, check_vma=False)
```

```python
import functools

import jax
import jax.numpy as jnp
import numpy as np
from jax import lax
from jax.experimental import pallas as pl
from jax.experimental.pallas import tpu as pltpu
from jax.sharding import PartitionSpec as P

EPS = 1e-6
ROPE_BASE = 1000000.0
MESH = pl.DeviceIdType.MESH

BLK = 128
LOW = 512
CH = 4
UCH = 8
UNIT = 32
SLOTS = 4
FIRST = 8
LEAD = 4
UP_SIZES = (240, 256, 264, 272, 280, 288, 304, 512)


def qkv_kernel(group, tok_ref, ln_ref, angle_ref, qg_ref, kg_ref, wq_hbm, wk_hbm, wv_hbm, qd_ref, sn_ref, vn_ref, kn_ref,
               hid, wq, wk, wv, own, other, gain_ref, gain_other, wsem, snd, rcv):
    partner = {"dim": 1 - lax.axis_index("dim")}
    rows, depth = tok_ref.shape
    n_q = own.shape[0] - 1
    steps = n_q // 2
    f32, bf16 = jnp.float32, jnp.bfloat16
    half = BLK // 2
    per_step = wq.shape[0] // steps

    def wq_copy(c):
        part = pl.ds(pl.multiple_of(c * per_step, per_step), per_step)
        return pltpu.make_async_copy(wq_hbm.at[part], wq.at[part], wsem.at[c])

    k_load = pltpu.make_async_copy(wk_hbm, wk, wsem.at[steps])
    v_load = pltpu.make_async_copy(wv_hbm, wv, wsem.at[steps + 1])

    def remote(src, dst, i):
        return pltpu.make_async_remote_copy(src_ref=src, dst_ref=dst, send_sem=snd.at[i], recv_sem=rcv.at[i],
                                            device_id=partner, device_id_type=MESH)

    def q_copy(c):
        part = pl.ds(2 * c, 2)
        return remote(own.at[part], other.at[part], c)

    k_copy = remote(own.at[pl.ds(n_q, 1)], other.at[pl.ds(n_q, 1)], steps)
    g_copy = remote(gain_ref, gain_other, steps + 1)

    k_load.start()
    for c in range(steps):
        wq_copy(c).start()
    v_load.start()
    barrier = pltpu.get_barrier_semaphore()
    pl.semaphore_signal(barrier, inc=1, device_id=partner, device_id_type=MESH)
    gain_ref[...] = jnp.zeros_like(gain_ref)
    for row, ref in enumerate((qg_ref, kg_ref)):
        gain_ref[row:row + 1, :half] = ref[...]
        gain_ref[row:row + 1, half:] = ref[...]
    pl.semaphore_wait(barrier, 1)

    @pl.loop(0, rows // 16)
    def _(i):
        part = pl.ds(pl.multiple_of(i * 16, 16), 16)
        x = tok_ref[part, :].astype(f32)
        inv = lax.rsqrt(jnp.mean(x * x, axis=-1, keepdims=True) + EPS)
        hid[part, :] = (x * inv * ln_ref[...]).astype(bf16)

    def project(w):
        return lax.dot_general(hid[...], w, (((1,), (1,)), ((), ())), preferred_element_type=f32)

    g_copy.start()
    k_load.wait()
    own[n_q] = project(wk[...])

    @pl.loop(0, steps)
    def _(c):
        wq_copy(c).wait()
        u = project(wq[pl.ds(pl.multiple_of(c * per_step, per_step), per_step), :])

        @pl.when(c == 0)
        def _():
            k_copy.start()

        own[2 * c] = u[:, :BLK]
        own[2 * c + 1] = u[:, BLK:]
        q_copy(c).start()

    v_load.wait()
    vn_ref[...] = project(wv[...]).astype(bf16).astype(f32)
    low = lax.broadcasted_iota(jnp.int32, (rows, BLK), 1) < half
    cos_t = jnp.cos(angle_ref[...])
    sin_t = jnp.sin(angle_ref[...]) * jnp.where(lax.axis_index("dim") == 0, -1.0, 1.0)

    def halves(x):
        return (jnp.sum(jnp.where(low, x, 0.0), axis=-1, keepdims=True), jnp.sum(jnp.where(low, 0.0, x), axis=-1, keepdims=True))

    def rotate(i, g):
        a, b = own[i], other[i]
        s_lo, s_hi = halves(a * a + b * b)
        inv = jnp.where(low, lax.rsqrt(s_lo / BLK + EPS), lax.rsqrt(s_hi / BLK + EPS))
        a, b = a * inv * gain_ref[g:g + 1, :], b * inv * gain_other[g:g + 1, :]
        return (a * cos_t + b * sin_t).astype(bf16).astype(f32), (b * cos_t - a * sin_t).astype(bf16).astype(f32)

    g_copy.wait_recv()
    k_copy.wait_recv()
    k_own, k_oth = rotate(n_q, 1)
    kn_ref[...] = k_own.astype(bf16)
    kr_own, kr_oth = pltpu.roll(k_own, half, 1), pltpu.roll(k_oth, half, 1)
    kk = [(jnp.where(low, k_own, kr_own), jnp.where(low, k_oth, kr_oth)),
          (jnp.where(low, kr_own, k_own), jnp.where(low, kr_oth, k_oth))]
    for i in range(n_q):
        if i % 2 == 0:
            q_copy(i // 2).wait_recv()
        q_own, q_oth = rotate(i, 0)
        kv = 2 * i // group
        new = halves(q_own * kk[kv][0] + q_oth * kk[kv][1])
        turned = pltpu.roll(q_own, half, 1)
        for e in range(2):
            row = i + n_q * e
            sn_ref[:, row, :] = jnp.broadcast_to(new[e], (rows, BLK))
            val = q_own if e == kv else turned
            qd_ref[:, row, :] = jnp.where(low, val, 0.0) if kv == 0 else jnp.where(low, 0.0, val)
    for c in range(steps):
        q_copy(c).wait_send()
    k_copy.wait_send()
    g_copy.wait_send()


def qkv(cid, group, tokens, ln, angle, q_gain, k_gain, w_q, w_k, w_v):
    rows, depth = tokens.shape
    n_q = w_q.shape[0] // BLK
    steps = n_q // 2
    vmem = pl.BlockSpec(memory_space=pltpu.VMEM)
    hbm = pl.BlockSpec(memory_space=pl.ANY)
    f32, bf16 = jnp.float32, jnp.bfloat16
    heads = 2 * n_q
    dma = pltpu.SemaphoreType.DMA
    return pl.pallas_call(
        functools.partial(qkv_kernel, group),
        out_shape=(jax.ShapeDtypeStruct((rows, heads, BLK), f32), jax.ShapeDtypeStruct((rows, heads, BLK), f32),
                   jax.ShapeDtypeStruct((rows, BLK), f32), jax.ShapeDtypeStruct((rows, BLK), bf16)),
        in_specs=[vmem] * 5 + [hbm] * 3,
        out_specs=(vmem,) * 4,
        scratch_shapes=[
            pltpu.VMEM((rows, depth), bf16),
            pltpu.VMEM(w_q.shape, bf16),
            pltpu.VMEM(w_k.shape, bf16),
            pltpu.VMEM(w_v.shape, bf16),
            pltpu.VMEM((n_q + 1, rows, BLK), f32),
            pltpu.VMEM((n_q + 1, rows, BLK), f32),
            pltpu.VMEM((8, BLK), f32),
            pltpu.VMEM((8, BLK), f32),
            dma((steps + 2,)), dma((steps + 2,)), dma((steps + 2,)),
        ],
        compiler_params=pltpu.CompilerParams(collective_id=cid, has_side_effects=True, vmem_limit_bytes=62 * 1024 * 1024),
        name="qkv",
    )(tokens, ln, angle, q_gain, k_gain, w_q, w_k, w_v)


def attn_kernel(n_up, scale, pos_ref, off_ref, idx_ref, qd_ref, sn_ref, vn_ref, k_hbm, v_hbm, o_ref,
                kbuf, vbuf, own_lo, own_up, pack, rlo, rup, ksem, vsem, slo_s, slo_r, sup_s, sup_r):
    partner = {"dim": 1 - lax.axis_index("dim")}
    rows = qd_ref.shape[0]
    n_ch = rows // CH
    n_uch = n_up // UCH
    up_blocks = own_up.shape[0] // rows
    per_blk = BLK // UNIT
    lane_up = lax.broadcasted_iota(jnp.int32, (16, BLK), 1)

    def kcopy(c):
        return pltpu.make_async_copy(k_hbm.at[pl.ds(c * CH, CH)], kbuf.at[lax.rem(c, SLOTS)], ksem.at[lax.rem(c, SLOTS)])

    def vcopy(c):
        return pltpu.make_async_copy(v_hbm.at[pl.ds(c * CH, CH)], vbuf.at[lax.rem(c, SLOTS)], vsem.at[lax.rem(c, SLOTS)])

    def lo_copy(c):
        part = pl.ds(c * CH, CH)
        return pltpu.make_async_remote_copy(src_ref=own_lo.at[part], dst_ref=rlo.at[part], send_sem=slo_s.at[c],
                                            recv_sem=slo_r.at[c], device_id=partner, device_id_type=MESH)

    def up_copy(c):
        part = pl.ds(c * UCH, UCH)
        return pltpu.make_async_remote_copy(src_ref=pack.at[part], dst_ref=rup.at[part], send_sem=sup_s.at[c],
                                            recv_sem=sup_r.at[c], device_id=partner, device_id_type=MESH)

    for c in range(SLOTS):
        kcopy(c).start()
    barrier = pltpu.get_barrier_semaphore()
    pl.semaphore_signal(barrier, inc=1, device_id=partner, device_id_type=MESH)
    pl.semaphore_wait(barrier, 1)
    for c in range(SLOTS):
        vcopy(c).start()

    @pl.loop(0, n_ch)
    def _(c):
        kcopy(c).wait()
        for r in range(CH):
            b = c * CH + r
            s = jnp.dot(qd_ref[b].astype(jnp.bfloat16), kbuf[lax.rem(c, SLOTS), r], preferred_element_type=jnp.float32)
            own_lo[b] = s[:, :LOW]
            for j in range(up_blocks):
                own_up[b * up_blocks + j] = s[:, LOW + j * BLK:LOW + (j + 1) * BLK]

        @pl.when(c + SLOTS < n_ch)
        def _():
            kcopy(c + SLOTS).start()

        @pl.when((c >= 1) & (c <= FIRST))
        def _():
            lo_copy(c - 1).start()

    @pl.loop(0, n_uch + 1)
    def _(c):
        @pl.when(c < n_uch)
        def _():
            for r in range(UCH):
                j = c * UCH + r
                block = None
                for k in range(per_blk):
                    row = idx_ref[j * per_blk + k]
                    src = jnp.minimum(row * (up_blocks * per_blk) + j * per_blk + k - off_ref[row], rows * up_blocks * per_blk - 1)
                    piece = pltpu.roll(own_up[src // per_blk], (k + per_blk - src % per_blk) % per_blk * UNIT, 1)
                    block = piece if k == 0 else jnp.where(lane_up >= k * UNIT, piece, block)
                pack[j] = block

        @pl.when(c >= 1)
        def _():
            up_copy(c - 1).start()

    @pl.loop(FIRST, FIRST + LEAD)
    def _(c):
        lo_copy(c).start()

    @pl.loop(0, n_uch)
    def _(c):
        up_copy(c).wait_recv()

    lane = lax.broadcasted_iota(jnp.int32, (8, 2 * 64), 1)
    first = lax.broadcasted_iota(jnp.int32, (8, 2 * 64), 0) < 4
    t_up = lane_up + LOW

    @pl.loop(0, n_ch)
    def _(c):
        @pl.when(c + FIRST + LEAD < n_ch)
        def _():
            lo_copy(c + FIRST + LEAD).start()

        vcopy(c).wait()
        lo_copy(c).wait_recv()
        for r in range(CH):
            b = c * CH + r
            pos = pos_ref[b]
            off = off_ref[b]
            parts = [(own_lo[b] + rlo[b]) * scale]
            skew = off % per_blk * UNIT
            slots = [pltpu.roll(rup[jnp.minimum(off // per_blk + j, n_up - 1)], (BLK - skew) % BLK, 1) for j in range(up_blocks + 1)]
            for j in range(up_blocks):
                got = jnp.where(lane_up < BLK - skew, slots[j], slots[j + 1])
                total = (own_up[b * up_blocks + j] + got) * scale
                parts.append(jnp.where(t_up + j * BLK < pos, total, -jnp.inf))
            s = jnp.concatenate(parts, axis=1)
            s_new = sn_ref[b][:, 0:1] * scale
            m = jnp.maximum(jnp.max(s, axis=1, keepdims=True), s_new)
            e = jnp.exp(s - m)
            e_new = jnp.exp(s_new - m)
            inv = 1.0 / (jnp.sum(e, axis=1, keepdims=True) + e_new)
            p = (e * inv).astype(jnp.bfloat16)
            p_new = (e_new * inv).astype(jnp.bfloat16).astype(jnp.float32)
            o = lax.dot_general(p, vbuf[lax.rem(c, SLOTS), r], (((1,), (1,)), ((), ())), preferred_element_type=jnp.float32)
            o = o + p_new * vn_ref[pl.ds(b, 1), :]
            even, odd = o[0:8], o[8:16]
            o_ref[b] = jnp.where(lane < 64, jnp.where(first, even, pltpu.roll(even, 64, 1)), jnp.where(first, pltpu.roll(odd, 64, 1), odd))

        @pl.when(c + SLOTS < n_ch)
        def _():
            vcopy(c + SLOTS).start()

    @pl.loop(0, n_ch)
    def _(c):
        lo_copy(c).wait_send()

    @pl.loop(0, n_uch)
    def _(c):
        up_copy(c).wait_send()


def attend(n_up, cid, scale, pos, off, idx, qd, sn, vn, k_t, v_t):
    rows = qd.shape[0]
    n_ch = rows // CH
    n_uch = n_up // UCH
    cache_len = k_t.shape[2]
    up_blocks = (cache_len - LOW) // BLK
    smem = pl.BlockSpec(memory_space=pltpu.SMEM)
    vmem = pl.BlockSpec(memory_space=pltpu.VMEM)
    hbm = pl.BlockSpec(memory_space=pl.ANY)
    return pl.pallas_call(
        functools.partial(attn_kernel, n_up, scale),
        out_shape=jax.ShapeDtypeStruct((rows, 8, 128), jnp.float32),
        in_specs=[smem, smem, smem, vmem, vmem, vmem, hbm, hbm],
        out_specs=vmem,
        scratch_shapes=[
            pltpu.VMEM((SLOTS, CH, 128, cache_len), jnp.bfloat16),
            pltpu.VMEM((SLOTS, CH, 128, cache_len), jnp.bfloat16),
            pltpu.VMEM((rows, 16, LOW), jnp.float32),
            pltpu.VMEM((rows * up_blocks, 16, BLK), jnp.float32),
            pltpu.VMEM((n_up, 16, BLK), jnp.float32),
            pltpu.VMEM((rows, 16, LOW), jnp.float32),
            pltpu.VMEM((n_up, 16, BLK), jnp.float32),
            pltpu.SemaphoreType.DMA((SLOTS,)),
            pltpu.SemaphoreType.DMA((SLOTS,)),
            pltpu.SemaphoreType.DMA((n_ch,)),
            pltpu.SemaphoreType.DMA((n_ch,)),
            pltpu.SemaphoreType.DMA((n_uch,)),
            pltpu.SemaphoreType.DMA((n_uch,)),
        ],
        compiler_params=pltpu.CompilerParams(collective_id=cid, has_side_effects=True, vmem_limit_bytes=40 * 1024 * 1024),
        name=f"attend_{n_up}",
    )(pos, off, idx, qd, sn, vn, k_t, v_t)


Q = 10
WO_SLOTS = 4
GU_SLOTS = 4
WD_SLOTS = 4


def tail_kernel(attn_ref, tok_hbm, ln_ref, wo_hbm, wg_hbm, wu_hbm, wd_hbm, out_ref,
                x_ref, tok_ref, part, r1, r2, r3, full, xres, acc_g, acc_u, mact, wo, wg, wu, wd,
                tok_s, wo_s, wg_s, wu_s, wd_s, snd, rcv):
    heads = lax.axis_index("heads")
    core, cx, cy = lax.rem(heads, 2), heads // 2, lax.axis_index("dim")
    sib = {"heads": 2 * cx + 1 - core}
    xn = {"heads": 2 * (1 - cx) + core}
    yn = {"dim": 1 - cy}
    width = part.shape[3]
    rows = 16 * 8
    f32 = jnp.float32

    def cols(q):
        return pl.ds(pl.multiple_of(q * width, width), width)

    def wo_copy(q):
        s = lax.rem(q, WO_SLOTS)
        return [pltpu.make_async_copy(wo_hbm.at[:, cols(q)], wo.at[s], wo_s.at[s])]

    def gu_copy(q):
        s = lax.rem(q, GU_SLOTS)
        return [pltpu.make_async_copy(wg_hbm.at[cols(q)], wg.at[s], wg_s.at[s]),
                pltpu.make_async_copy(wu_hbm.at[cols(q)], wu.at[s], wu_s.at[s])]

    def wd_copy(q):
        s = lax.rem(q, WD_SLOTS)
        return [pltpu.make_async_copy(wd_hbm.at[:, cols(q)], wd.at[s], wd_s.at[s])]

    def start(copies):
        for cp in copies:
            cp.start()

    def wait(copies):
        for cp in copies:
            cp.wait()

    def remote(ph, st, q, src, dst, dev):
        return pltpu.make_async_remote_copy(src_ref=src, dst_ref=dst, send_sem=snd.at[ph, st], recv_sem=rcv.at[ph, st, q],
                                            device_id=dev, device_id_type=MESH)

    def stage(ph, k, q, sem_q):
        if k == 0:
            return [remote(ph, 0, sem_q, part.at[q, pl.ds(8 * (1 - core), 8)], r1.at[q], sib)]
        if k == 1:
            return [remote(ph, 1, sem_q, r1.at[q, pl.ds(2 * (1 - cx), 2)], r2.at[q, pl.ds(0, 2)], xn),
                    remote(ph, 2, sem_q, r1.at[q, pl.ds(4 + 2 * (1 - cy), 2)], r2.at[q, pl.ds(2, 2)], yn)]
        if k == 2:
            return [remote(ph, 3, sem_q, r2.at[q, pl.ds(1 - cy, 1)], r3.at[q, pl.ds(0, 1)], yn),
                    remote(ph, 4, sem_q, r2.at[q, pl.ds(2 + 1 - cx, 1)], r3.at[q, pl.ds(1, 1)], xn)]
        blk_a, blk_b = core * 8, core * 8 + 4
        if k == 3:
            a, b = full.at[q, pl.ds(blk_a + 2 * cx + cy, 1)], full.at[q, pl.ds(blk_b + 2 * cy + cx, 1)]
            return [remote(ph, 5, sem_q, a, a, yn), remote(ph, 6, sem_q, b, b, xn)]
        if k == 4:
            a, b = full.at[q, pl.ds(blk_a + 2 * cx, 2)], full.at[q, pl.ds(blk_b + 2 * cy, 2)]
            return [remote(ph, 7, sem_q, a, a, xn), remote(ph, 8, sem_q, b, b, yn)]
        a = full.at[q, pl.ds(blk_a, 8)]
        return [remote(ph, 9, sem_q, a, a, sib)]

    def one(ph, k, q):
        return stage(ph, k, q, q)

    def drain(ph, ks):
        for k in ks:
            for cp in stage(ph, k, slice(None), 0):
                cp.wait_send()

    def arrived(ph, k, q):
        for cp in one(ph, k, q):
            cp.wait_recv()

    def when(t, lo):
        return pl.when((t >= lo) & (t < lo + Q))

    def reduce_steps(ph, t, finish):
        @when(t, 1)
        def _():
            start(one(ph, 0, t - 1))

        @when(t, 2)
        def _():
            u = t - 2
            arrived(ph, 0, u)
            r1[u] = r1[u] + part[u, pl.ds(8 * core, 8)]
            start(one(ph, 1, u))

        @when(t, 4)
        def _():
            u = t - 4
            arrived(ph, 1, u)
            r2[u, pl.ds(0, 2)] = r2[u, pl.ds(0, 2)] + r1[u, pl.ds(2 * cx, 2)]
            r2[u, pl.ds(2, 2)] = r2[u, pl.ds(2, 2)] + r1[u, pl.ds(4 + 2 * cy, 2)]
            start(one(ph, 2, u))

        @when(t, 6)
        def _():
            u = t - 6
            arrived(ph, 2, u)
            finish(u, r3[u, 0] + r2[u, cy], r3[u, 1] + r2[u, 2 + cx])

    def gather_steps(ph, t, finish):
        @when(t, 0)
        def _():
            start(one(ph, 3, t))

        @when(t, 2)
        def _():
            arrived(ph, 3, t - 2)
            start(one(ph, 4, t - 2))

        @when(t, 4)
        def _():
            arrived(ph, 4, t - 4)
            start(one(ph, 5, t - 4))

        @when(t, 5)
        def _():
            arrived(ph, 5, t - 5)
            finish(t - 5)

    blk_a, blk_b = core * 8 + 2 * cx + cy, core * 8 + 4 + 2 * cy + cx
    tok_loads = [pltpu.make_async_copy(tok_hbm.at[blk], tok_ref.at[i], tok_s.at[i]) for i, blk in enumerate((blk_a, blk_b))]
    for q in range(WO_SLOTS):
        start(wo_copy(q))
    start(tok_loads)
    barrier = pltpu.get_barrier_semaphore()
    for dev in (sib, xn, yn):
        pl.semaphore_signal(barrier, inc=1, device_id=dev, device_id_type=MESH)
    pl.semaphore_wait(barrier, 3)
    acc_g[...] = jnp.zeros_like(acc_g)
    acc_u[...] = jnp.zeros_like(acc_u)
    for i in range(attn_ref.shape[1]):
        x_ref[:, i * BLK:(i + 1) * BLK] = attn_ref[:, i, :].astype(jnp.bfloat16)
    wait(tok_loads)

    def finish_attn(u, a, b):
        xres[u, 0] = (tok_ref[0, :, cols(u)].astype(f32) + a).astype(jnp.bfloat16).astype(f32)
        xres[u, 1] = (tok_ref[1, :, cols(u)].astype(f32) + b).astype(jnp.bfloat16).astype(f32)

    @pl.loop(0, Q + 6)
    def _(t):
        @when(t, 0)
        def _():
            wait(wo_copy(t))
            part[t] = jnp.dot(x_ref[...], wo[lax.rem(t, WO_SLOTS)], preferred_element_type=f32).reshape(16, 8, width)

            @pl.when(t + WO_SLOTS < Q)
            def _():
                start(wo_copy(t + WO_SLOTS))

            @pl.when(t < GU_SLOTS)
            def _():
                start(gu_copy(t))

            @pl.when((t >= GU_SLOTS) & (t < GU_SLOTS + WD_SLOTS))
            def _():
                start(wd_copy(t - GU_SLOTS))
        reduce_steps(0, t, finish_attn)

    drain(0, (0, 1, 2))
    sq = jnp.zeros((2, 8, 1), f32)
    for q in range(Q):
        sq = sq + jnp.sum(xres[q] * xres[q], axis=-1, keepdims=True)
    inv = lax.rsqrt(sq / (Q * width) + EPS)
    for q in range(Q):
        h = (xres[q] * inv * ln_ref[q]).astype(jnp.bfloat16).astype(f32)
        full[q, blk_a] = h[0]
        full[q, blk_b] = h[1]

    def finish_gather(u):
        wait(gu_copy(u))
        s = lax.rem(u, GU_SLOTS)
        h = full[u].reshape(rows, width).astype(jnp.bfloat16)
        acc_g[...] += jnp.dot(h, wg[s], preferred_element_type=f32)
        acc_u[...] += jnp.dot(h, wu[s], preferred_element_type=f32)

        @pl.when(u + GU_SLOTS < Q)
        def _():
            start(gu_copy(u + GU_SLOTS))

    @pl.loop(0, Q + 5)
    def _(t):
        gather_steps(0, t, finish_gather)

    drain(0, (3, 4, 5))

    @pl.loop(0, acc_g.shape[1] // 640)
    def _(n):
        c = pl.ds(pl.multiple_of(n * 640, 640), 640)
        mact[:, c] = (jax.nn.silu(acc_g[:, c]) * acc_u[:, c]).astype(jnp.bfloat16)

    def finish_mlp(u, a, b):
        full[u, blk_a] = (xres[u, 0] + a).astype(jnp.bfloat16).astype(f32)
        full[u, blk_b] = (xres[u, 1] + b).astype(jnp.bfloat16).astype(f32)

    def finish_out(u):
        out_ref[:, cols(u)] = full[u].reshape(rows, width).astype(jnp.bfloat16)

    @pl.loop(0, Q + 12)
    def _(t):
        @when(t, 0)
        def _():
            wait(wd_copy(t))
            part[t] = jnp.dot(mact[...], wd[lax.rem(t, WD_SLOTS)], preferred_element_type=f32).reshape(16, 8, width)

            @pl.when(t + WD_SLOTS < Q)
            def _():
                start(wd_copy(t + WD_SLOTS))
        reduce_steps(1, t, finish_mlp)
        gather_steps(1, t - 7, finish_out)

    drain(1, (0, 1, 2, 3, 4, 5))


def tail(cid, attn, tok_blocks, ln, w_out, w_gate, w_up, w_down):
    rows = attn.shape[0]
    depth = w_out.shape[0]
    d_model, inner = w_gate.shape
    width = d_model // Q
    vmem = pl.BlockSpec(memory_space=pltpu.VMEM)
    hbm = pl.BlockSpec(memory_space=pl.ANY)
    f32, bf16 = jnp.float32, jnp.bfloat16
    dma = pltpu.SemaphoreType.DMA
    return pl.pallas_call(
        tail_kernel,
        out_shape=jax.ShapeDtypeStruct((rows, d_model), bf16),
        in_specs=[vmem, hbm, vmem, hbm, hbm, hbm, hbm],
        out_specs=vmem,
        scratch_shapes=[
            pltpu.VMEM((rows, depth), bf16),
            pltpu.VMEM((2, 8, d_model), bf16),
            pltpu.VMEM((Q, 16, 8, width), f32),
            pltpu.VMEM((Q, 8, 8, width), f32),
            pltpu.VMEM((Q, 4, 8, width), f32),
            pltpu.VMEM((Q, 2, 8, width), f32),
            pltpu.VMEM((Q, 16, 8, width), f32),
            pltpu.VMEM((Q, 2, 8, width), f32),
            pltpu.VMEM((rows, inner), f32),
            pltpu.VMEM((rows, inner), f32),
            pltpu.VMEM((rows, inner), bf16),
            pltpu.VMEM((WO_SLOTS, depth, width), bf16),
            pltpu.VMEM((GU_SLOTS, width, inner), bf16),
            pltpu.VMEM((GU_SLOTS, width, inner), bf16),
            pltpu.VMEM((WD_SLOTS, inner, width), bf16),
            dma((2,)), dma((WO_SLOTS,)), dma((GU_SLOTS,)), dma((GU_SLOTS,)), dma((WD_SLOTS,)),
            dma((2, 10)), dma((2, 10, Q)),
        ],
        compiler_params=pltpu.CompilerParams(collective_id=cid, has_side_effects=True, vmem_limit_bytes=59 * 1024 * 1024),
        name="tail",
    )(attn, tok_blocks, ln, w_out, w_gate, w_up, w_down)


def solution(mesh):
    dim_count = mesh.shape['dim']
    mlp_axes = ('heads', 'dim')

    def layer_body(tokens, ln_attn, w_query, w_key, w_value, q_gain, k_gain, w_out, ln_mlp, w_gate, w_up, w_down, k_cache, v_cache, positions):
        rows = tokens.shape[0]
        heads_local = w_query.shape[1]
        kv_local = w_key.shape[1]
        slice_len = w_query.shape[2]
        head_dim = slice_len * dim_count
        half_dim = head_dim // 2
        q_group = heads_local // kv_local
        cache_len = k_cache.shape[1]
        up_blocks = (cache_len - LOW) // BLK
        dim_index = lax.axis_index('dim')

        inv_freq = np.tile(ROPE_BASE ** (-np.arange(half_dim) * 2.0 / head_dim), 2).astype(np.float32)
        angle = positions.astype(jnp.float32)[:, None] * inv_freq

        def by_column(w):
            return w.transpose(1, 2, 0).reshape(-1, w.shape[0])

        qd, sn, vn, kn = qkv(len(UP_SIZES) + 1, q_group, tokens, ln_attn[None], angle, q_gain[None], k_gain[None],
                             by_column(w_query), by_column(w_key), by_column(w_value))
        k_new = kn.reshape(rows, kv_local, slice_len)
        v_new = vn.astype(jnp.bfloat16).reshape(rows, kv_local, slice_len)

        row_units = up_blocks * BLK // UNIT
        n_units = (positions - LOW + UNIT - 1) // UNIT
        seq = jnp.arange(rows)
        cum = jnp.sum(jnp.where(seq[:, None] >= seq[None, :], n_units[None, :], 0), axis=1)
        off = cum - n_units
        unit = jnp.arange(rows * row_units)
        row_of = jnp.sum((cum[None, :] <= unit[:, None]).astype(jnp.int32), axis=1)
        row_of = jnp.minimum(row_of, rows - 1)

        k_t = k_cache.transpose(0, 2, 3, 1).reshape(rows, kv_local * slice_len, cache_len)
        v_t = v_cache.transpose(0, 2, 3, 1).reshape(rows, kv_local * slice_len, cache_len)
        which = jnp.sum((jnp.sum(n_units) > np.array(UP_SIZES[:-1]) * (BLK // UNIT)).astype(jnp.int32))
        branches = [functools.partial(attend, n, i, head_dim ** -0.5) for i, n in enumerate(UP_SIZES)]
        attn = lax.switch(which, branches, positions, off, row_of, qd, sn, vn, k_t, v_t)
        out = tail(len(UP_SIZES), attn, tokens.reshape(16, 8, -1), ln_mlp.reshape(Q, 1, -1), w_out.reshape(heads_local * slice_len, -1), w_gate, w_up, w_down)
        return out, k_new, v_new

    row_spec = P('dp', None)
    head_spec = P(None, 'heads', 'dim')
    cache_spec = P('dp', None, 'heads', 'dim')
    new_spec = P('dp', 'heads', 'dim')
    in_specs = (row_spec, P(None), head_spec, head_spec, head_spec, P('dim'), P('dim'), P('heads', 'dim', None), P(None), P(None, mlp_axes), P(None, mlp_axes), P(mlp_axes, None), cache_spec, cache_spec, P('dp'))
    out_specs = (row_spec, new_spec, new_spec)
    return jax.shard_map(layer_body, mesh=mesh, in_specs=in_specs, out_specs=out_specs, check_vma=False)
```

```python
import functools

import jax
import jax.numpy as jnp
import numpy as np
from jax import lax
from jax.experimental import pallas as pl
from jax.experimental.pallas import tpu as pltpu
from jax.sharding import PartitionSpec as P

EPS = 1e-6
ROPE_BASE = 1000000.0
MESH = pl.DeviceIdType.MESH

BLK = 128
LOW = 512
CH = 2
UCH = 8
UNIT = 16
SLOTS = 6
FIRST = 16
LEAD = 8
UP_SIZES = (232, 248, 256, 264, 272, 280, 296, 512)


def qkv_kernel(group, tok_ref, ln_ref, pos_ref, freq_ref, qg_ref, kg_ref, wq_hbm, wk_hbm, wv_hbm, qd_ref, sn_ref, vn_ref, kt_ref, vt_ref,
               hid, wq, wk, wv, own, other, gain_ref, gain_other, wsem, snd, rcv):
    partner = {"dim": 1 - lax.axis_index("dim")}
    rows, depth = tok_ref.shape
    n_q = own.shape[0] - 1
    steps = n_q // 2
    f32, bf16 = jnp.float32, jnp.bfloat16
    half = BLK // 2
    per_step = wq.shape[0] // steps

    def wq_copy(c):
        part = pl.ds(pl.multiple_of(c * per_step, per_step), per_step)
        return pltpu.make_async_copy(wq_hbm.at[part], wq.at[part], wsem.at[c])

    k_load = pltpu.make_async_copy(wk_hbm, wk, wsem.at[steps])
    v_load = pltpu.make_async_copy(wv_hbm, wv, wsem.at[steps + 1])

    def remote(src, dst, i):
        return pltpu.make_async_remote_copy(src_ref=src, dst_ref=dst, send_sem=snd.at[i], recv_sem=rcv.at[i],
                                            device_id=partner, device_id_type=MESH)

    def q_copy(c):
        part = pl.ds(2 * c, 2)
        return remote(own.at[part], other.at[part], c)

    k_copy = remote(own.at[pl.ds(n_q, 1)], other.at[pl.ds(n_q, 1)], steps)
    g_copy = remote(gain_ref, gain_other, steps + 1)

    k_load.start()
    for c in range(steps):
        wq_copy(c).start()
    v_load.start()
    barrier = pltpu.get_barrier_semaphore()
    pl.semaphore_signal(barrier, inc=1, device_id=partner, device_id_type=MESH)
    gain_ref[...] = jnp.zeros_like(gain_ref)
    for row, ref in enumerate((qg_ref, kg_ref)):
        gain_ref[row:row + 1, :half] = ref[...]
        gain_ref[row:row + 1, half:] = ref[...]
    pl.semaphore_wait(barrier, 1)

    @pl.loop(0, rows // 16, unroll=4)
    def _(i):
        part = pl.ds(pl.multiple_of(i * 16, 16), 16)
        x = tok_ref[part, :].astype(f32)
        inv = lax.rsqrt(jnp.mean(x * x, axis=-1, keepdims=True) + EPS)
        hid[part, :] = (x * inv * ln_ref[...]).astype(bf16)

    def project(w):
        return lax.dot_general(hid[...], w, (((1,), (1,)), ((), ())), preferred_element_type=f32)

    g_copy.start()
    k_load.wait()
    own[n_q] = project(wk[...])
    k_copy.start()

    @pl.loop(0, steps)
    def _(c):
        wq_copy(c).wait()
        u = project(wq[pl.ds(pl.multiple_of(c * per_step, per_step), per_step), :])

        own[2 * c] = u[:, :BLK]
        own[2 * c + 1] = u[:, BLK:]
        q_copy(c).start()

    v_load.wait()
    v_row = project(wv[...]).astype(bf16).astype(f32)
    vn_ref[...] = v_row
    vt_ref[...] = v_row.T.astype(bf16)
    low = lax.broadcasted_iota(jnp.int32, (rows, BLK), 1) < half
    angle = jnp.broadcast_to(pos_ref[...], (rows, rows)).T * freq_ref[...]
    cos_t = jnp.cos(angle)
    sin_t = jnp.sin(angle) * jnp.where(lax.axis_index("dim") == 0, -1.0, 1.0)

    def halves(x):
        return (jnp.sum(jnp.where(low, x, 0.0), axis=-1, keepdims=True), jnp.sum(jnp.where(low, 0.0, x), axis=-1, keepdims=True))

    def rotate(i, g):
        a, b = own[i], other[i]
        s_lo, s_hi = halves(a * a + b * b)
        inv = jnp.where(low, lax.rsqrt(s_lo / BLK + EPS), lax.rsqrt(s_hi / BLK + EPS))
        a, b = a * inv * gain_ref[g:g + 1, :], b * inv * gain_other[g:g + 1, :]
        return (a * cos_t + b * sin_t).astype(bf16).astype(f32), (b * cos_t - a * sin_t).astype(bf16).astype(f32)

    g_copy.wait_recv()
    k_copy.wait_recv()
    k_own, k_oth = rotate(n_q, 1)
    kt_ref[...] = k_own.T.astype(bf16)
    kr_own, kr_oth = pltpu.roll(k_own, half, 1), pltpu.roll(k_oth, half, 1)
    kk = [(jnp.where(low, k_own, kr_own), jnp.where(low, k_oth, kr_oth)),
          (jnp.where(low, kr_own, k_own), jnp.where(low, kr_oth, k_oth))]
    for i in range(n_q):
        if i % 2 == 0:
            q_copy(i // 2).wait_recv()
        q_own, q_oth = rotate(i, 0)
        kv = 2 * i // group
        new = halves(q_own * kk[kv][0] + q_oth * kk[kv][1])
        turned = pltpu.roll(q_own, half, 1)
        for e in range(2):
            row = i + n_q * e
            sn_ref[:, row, :] = jnp.broadcast_to(new[e], (rows, BLK))
            val = q_own if e == kv else turned
            qd_ref[:, row, :] = jnp.where(low, val, 0.0) if kv == 0 else jnp.where(low, 0.0, val)
    for c in range(steps):
        q_copy(c).wait_send()
    k_copy.wait_send()
    g_copy.wait_send()


def qkv(cid, group, tokens, ln, pos, freq, q_gain, k_gain, w_q, w_k, w_v):
    rows, depth = tokens.shape
    n_q = w_q.shape[0] // BLK
    steps = n_q // 2
    vmem = pl.BlockSpec(memory_space=pltpu.VMEM)
    hbm = pl.BlockSpec(memory_space=pl.ANY)
    f32, bf16 = jnp.float32, jnp.bfloat16
    heads = 2 * n_q
    dma = pltpu.SemaphoreType.DMA
    return pl.pallas_call(
        functools.partial(qkv_kernel, group),
        out_shape=(jax.ShapeDtypeStruct((rows, heads, BLK), f32), jax.ShapeDtypeStruct((rows, heads, BLK), f32),
                   jax.ShapeDtypeStruct((rows, BLK), f32), jax.ShapeDtypeStruct((BLK, rows), bf16), jax.ShapeDtypeStruct((BLK, rows), bf16)),
        in_specs=[vmem] * 6 + [hbm] * 3,
        out_specs=(vmem,) * 5,
        scratch_shapes=[
            pltpu.VMEM((rows, depth), bf16),
            pltpu.VMEM(w_q.shape, bf16),
            pltpu.VMEM(w_k.shape, bf16),
            pltpu.VMEM(w_v.shape, bf16),
            pltpu.VMEM((n_q + 1, rows, BLK), f32),
            pltpu.VMEM((n_q + 1, rows, BLK), f32),
            pltpu.VMEM((8, BLK), f32),
            pltpu.VMEM((8, BLK), f32),
            dma((steps + 2,)), dma((steps + 2,)), dma((steps + 2,)),
        ],
        compiler_params=pltpu.CompilerParams(collective_id=cid, has_side_effects=True, vmem_limit_bytes=62 * 1024 * 1024),
        name="qkv",
    )(tokens, ln, pos, freq, q_gain, k_gain, w_q, w_k, w_v)


def attn_kernel(n_up, scale, pos_ref, qd_ref, sn_ref, vn_ref, k_hbm, v_hbm, o_ref,
                off_ref, kbuf, vbuf, own_lo, own_up, pack, rlo, rup, ksem, vsem, send, slo_r, sup_r):
    partner = {"dim": 1 - lax.axis_index("dim")}
    rows = qd_ref.shape[0]
    n_ch = rows // CH
    n_uch = n_up // UCH
    up_blocks = own_up.shape[0] // rows
    per_blk = BLK // UNIT
    lane_up = lax.broadcasted_iota(jnp.int32, (16, BLK), 1)

    def kcopy(c):
        return pltpu.make_async_copy(k_hbm.at[pl.ds(c * CH, CH)], kbuf.at[lax.rem(c, SLOTS)], ksem.at[lax.rem(c, SLOTS)])

    def vcopy(c):
        return pltpu.make_async_copy(v_hbm.at[pl.ds(c * CH, CH)], vbuf.at[lax.rem(c, SLOTS)], vsem.at[lax.rem(c, SLOTS)])

    def lo_copy(c):
        part = pl.ds(c * CH, CH)
        return pltpu.make_async_remote_copy(src_ref=own_lo.at[part], dst_ref=rlo.at[part], send_sem=send.at[0],
                                            recv_sem=slo_r.at[c], device_id=partner, device_id_type=MESH)

    def up_copy(c):
        part = pl.ds(c * UCH, UCH)
        return pltpu.make_async_remote_copy(src_ref=pack.at[part], dst_ref=rup.at[part], send_sem=send.at[1],
                                            recv_sem=sup_r.at[c], device_id=partner, device_id_type=MESH)

    for c in range(SLOTS):
        kcopy(c).start()
    barrier = pltpu.get_barrier_semaphore()
    pl.semaphore_signal(barrier, inc=1, device_id=partner, device_id_type=MESH)
    pl.semaphore_wait(barrier, 1)
    for c in range(SLOTS):
        vcopy(c).start()
    row_units = up_blocks * per_blk

    def place(b, total):
        off_ref[b] = total
        return total + jnp.maximum((pos_ref[b] - LOW + UNIT - 1) // UNIT, 1)

    lax.fori_loop(0, rows, place, jnp.int32(0))

    @pl.loop(0, n_ch)
    def _(c):
        kcopy(c).wait()
        for r in range(CH):
            b = c * CH + r
            s = jnp.dot(qd_ref[b].astype(jnp.bfloat16), kbuf[lax.rem(c, SLOTS), r], preferred_element_type=jnp.float32)
            own_lo[b] = s[:, :LOW]
            for j in range(up_blocks):
                own_up[b * up_blocks + j] = s[:, LOW + j * BLK:LOW + (j + 1) * BLK]

        @pl.when(c + SLOTS < n_ch)
        def _():
            kcopy(c + SLOTS).start()

        @pl.when((c >= 1) & (c <= FIRST))
        def _():
            lo_copy(c - 1).start()

    def fill(c, row):
        for r in range(UCH):
            j = c * UCH + r
            block = None
            for k in range(per_blk):
                unit = j * per_blk + k
                following = jnp.minimum(row + 1, rows - 1)
                row = jnp.where(unit >= off_ref[following], following, row)
                src = jnp.minimum(unit - off_ref[row], row_units - 1)
                piece = pltpu.roll(own_up[row * up_blocks + src // per_blk], (k + per_blk - src % per_blk) % per_blk * UNIT, 1)
                block = piece if k == 0 else jnp.where(lane_up >= k * UNIT, piece, block)
            pack[j] = block

        @pl.when(c >= 1)
        def _():
            up_copy(c - 1).start()
        return row

    lax.fori_loop(0, n_uch, fill, jnp.int32(0))
    up_copy(n_uch - 1).start()

    @pl.loop(FIRST, FIRST + LEAD)
    def _(c):
        lo_copy(c).start()

    @pl.loop(0, n_uch)
    def _(c):
        up_copy(c).wait_recv()

    lane = lax.broadcasted_iota(jnp.int32, (8, 2 * 64), 1)
    first = lax.broadcasted_iota(jnp.int32, (8, 2 * 64), 0) < 4
    t_up = lane_up + LOW

    @pl.loop(0, n_ch)
    def _(c):
        @pl.when(c + FIRST + LEAD < n_ch)
        def _():
            lo_copy(c + FIRST + LEAD).start()

        vcopy(c).wait()
        lo_copy(c).wait_recv()
        for r in range(CH):
            b = c * CH + r
            pos = pos_ref[b]
            off = off_ref[b]
            parts = [(own_lo[b] + rlo[b]) * scale]
            skew = off % per_blk * UNIT
            slots = [pltpu.roll(rup[jnp.minimum(off // per_blk + j, n_up - 1)], (BLK - skew) % BLK, 1) for j in range(up_blocks + 1)]
            for j in range(up_blocks):
                got = jnp.where(lane_up < BLK - skew, slots[j], slots[j + 1])
                total = (own_up[b * up_blocks + j] + got) * scale
                parts.append(jnp.where(t_up + j * BLK < pos, total, -jnp.inf))
            s = jnp.concatenate(parts, axis=1)
            s_new = sn_ref[b][:, 0:1] * scale
            m = jnp.maximum(jnp.max(s, axis=1, keepdims=True), s_new)
            e = jnp.exp(s - m)
            e_new = jnp.exp(s_new - m)
            inv = 1.0 / (jnp.sum(e, axis=1, keepdims=True) + e_new)
            p = (e * inv).astype(jnp.bfloat16)
            p_new = (e_new * inv).astype(jnp.bfloat16).astype(jnp.float32)
            o = lax.dot_general(p, vbuf[lax.rem(c, SLOTS), r], (((1,), (1,)), ((), ())), preferred_element_type=jnp.float32)
            o = o + p_new * vn_ref[pl.ds(b, 1), :]
            even, odd = o[0:8], o[8:16]
            o_ref[b] = jnp.where(lane < 64, jnp.where(first, even, pltpu.roll(even, 64, 1)), jnp.where(first, pltpu.roll(odd, 64, 1), odd))

        @pl.when(c + SLOTS < n_ch)
        def _():
            vcopy(c + SLOTS).start()

    pltpu.make_async_remote_copy(src_ref=own_lo, dst_ref=rlo, send_sem=send.at[0], recv_sem=slo_r.at[0],
                                 device_id=partner, device_id_type=MESH).wait_send()
    pltpu.make_async_remote_copy(src_ref=pack, dst_ref=rup, send_sem=send.at[1], recv_sem=sup_r.at[0],
                                 device_id=partner, device_id_type=MESH).wait_send()


def attend(n_up, cid, scale, pos, qd, sn, vn, k_t, v_t):
    rows = qd.shape[0]
    n_ch = rows // CH
    n_uch = n_up // UCH
    cache_len = k_t.shape[2]
    up_blocks = (cache_len - LOW) // BLK
    smem = pl.BlockSpec(memory_space=pltpu.SMEM)
    vmem = pl.BlockSpec(memory_space=pltpu.VMEM)
    hbm = pl.BlockSpec(memory_space=pl.ANY)
    return pl.pallas_call(
        functools.partial(attn_kernel, n_up, scale),
        out_shape=jax.ShapeDtypeStruct((rows, 8, 128), jnp.float32),
        in_specs=[smem, vmem, vmem, vmem, hbm, hbm],
        out_specs=vmem,
        scratch_shapes=[
            pltpu.SMEM((rows,), jnp.int32),
            pltpu.VMEM((SLOTS, CH, 128, cache_len), jnp.bfloat16),
            pltpu.VMEM((SLOTS, CH, 128, cache_len), jnp.bfloat16),
            pltpu.VMEM((rows, 16, LOW), jnp.float32),
            pltpu.VMEM((rows * up_blocks, 16, BLK), jnp.float32),
            pltpu.VMEM((n_up, 16, BLK), jnp.float32),
            pltpu.VMEM((rows, 16, LOW), jnp.float32),
            pltpu.VMEM((n_up, 16, BLK), jnp.float32),
            pltpu.SemaphoreType.DMA((SLOTS,)),
            pltpu.SemaphoreType.DMA((SLOTS,)),
            pltpu.SemaphoreType.DMA((2,)),
            pltpu.SemaphoreType.DMA((n_ch,)),
            pltpu.SemaphoreType.DMA((n_uch,)),
        ],
        compiler_params=pltpu.CompilerParams(collective_id=cid, has_side_effects=True, vmem_limit_bytes=40 * 1024 * 1024),
        name=f"attend_{n_up}",
    )(pos, qd, sn, vn, k_t, v_t)


Q = 10
WO_SLOTS = 4
GU_SLOTS = 4
WD_SLOTS = 3


def tail_kernel(attn_ref, tok_hbm, ln_ref, wo_hbm, wg_hbm, wu_hbm, wd_hbm, out_ref,
                x_ref, tok_ref, part, r1, r2, r3, full, xres, acc_g, acc_u, mact, wo, wg, wu, wd,
                tok_s, wo_s, wg_s, wu_s, wd_s, snd, rcv):
    heads = lax.axis_index("heads")
    core, cx, cy = lax.rem(heads, 2), heads // 2, lax.axis_index("dim")
    sib = {"heads": 2 * cx + 1 - core}
    xn = {"heads": 2 * (1 - cx) + core}
    yn = {"dim": 1 - cy}
    width = part.shape[3]
    rows = 16 * 8
    f32 = jnp.float32

    def cols(q):
        return pl.ds(pl.multiple_of(q * width, width), width)

    def wo_copy(q):
        s = lax.rem(q, WO_SLOTS)
        return [pltpu.make_async_copy(wo_hbm.at[:, cols(q)], wo.at[s], wo_s.at[s])]

    def gu_copy(q):
        s = lax.rem(q, GU_SLOTS)
        return [pltpu.make_async_copy(wg_hbm.at[cols(q)], wg.at[s], wg_s.at[s]),
                pltpu.make_async_copy(wu_hbm.at[cols(q)], wu.at[s], wu_s.at[s])]

    def wd_copy(q):
        s = lax.rem(q, WD_SLOTS)
        return [pltpu.make_async_copy(wd_hbm.at[:, cols(q)], wd.at[s], wd_s.at[s])]

    def start(copies):
        for cp in copies:
            cp.start()

    def wait(copies):
        for cp in copies:
            cp.wait()

    def remote(ph, st, q, src, dst, dev):
        return pltpu.make_async_remote_copy(src_ref=src, dst_ref=dst, send_sem=snd.at[ph, st], recv_sem=rcv.at[ph, st, q],
                                            device_id=dev, device_id_type=MESH)

    def stage(ph, k, q, sem_q):
        if k == 0:
            return [remote(ph, 0, sem_q, part.at[q, pl.ds(8 * (1 - core), 8)], r1.at[q], sib)]
        if k == 1:
            return [remote(ph, 1, sem_q, r1.at[q, pl.ds(2 * (1 - cx), 2)], r2.at[q, pl.ds(0, 2)], xn),
                    remote(ph, 2, sem_q, r1.at[q, pl.ds(4 + 2 * (1 - cy), 2)], r2.at[q, pl.ds(2, 2)], yn)]
        if k == 2:
            return [remote(ph, 3, sem_q, r2.at[q, pl.ds(1 - cy, 1)], r3.at[q, pl.ds(0, 1)], yn),
                    remote(ph, 4, sem_q, r2.at[q, pl.ds(2 + 1 - cx, 1)], r3.at[q, pl.ds(1, 1)], xn)]
        blk_a, blk_b = core * 8, core * 8 + 4
        if k == 3:
            a, b = full.at[q, pl.ds(blk_a + 2 * cx + cy, 1)], full.at[q, pl.ds(blk_b + 2 * cy + cx, 1)]
            return [remote(ph, 5, sem_q, a, a, yn), remote(ph, 6, sem_q, b, b, xn)]
        if k == 4:
            a, b = full.at[q, pl.ds(blk_a + 2 * cx, 2)], full.at[q, pl.ds(blk_b + 2 * cy, 2)]
            return [remote(ph, 7, sem_q, a, a, xn), remote(ph, 8, sem_q, b, b, yn)]
        a = full.at[q, pl.ds(blk_a, 8)]
        return [remote(ph, 9, sem_q, a, a, sib)]

    def one(ph, k, q):
        return stage(ph, k, q, q)

    def drain(ph, ks):
        for k in ks:
            for cp in stage(ph, k, slice(None), 0):
                cp.wait_send()

    def arrived(ph, k, q):
        for cp in one(ph, k, q):
            cp.wait_recv()

    def when(t, lo):
        return pl.when((t >= lo) & (t < lo + Q))

    def reduce_steps(ph, t, finish):
        @when(t, 1)
        def _():
            start(one(ph, 0, t - 1))

        @when(t, 2)
        def _():
            u = t - 2
            arrived(ph, 0, u)
            r1[u] = r1[u] + part[u, pl.ds(8 * core, 8)]
            start(one(ph, 1, u))

        @when(t, 4)
        def _():
            u = t - 4
            arrived(ph, 1, u)
            r2[u, pl.ds(0, 2)] = r2[u, pl.ds(0, 2)] + r1[u, pl.ds(2 * cx, 2)]
            r2[u, pl.ds(2, 2)] = r2[u, pl.ds(2, 2)] + r1[u, pl.ds(4 + 2 * cy, 2)]
            start(one(ph, 2, u))

        @when(t, 6)
        def _():
            u = t - 6
            arrived(ph, 2, u)
            finish(u, r3[u, 0] + r2[u, cy], r3[u, 1] + r2[u, 2 + cx])

    def gather_steps(ph, t, finish):
        @when(t, 0)
        def _():
            start(one(ph, 3, t))

        @when(t, 2)
        def _():
            arrived(ph, 3, t - 2)
            start(one(ph, 4, t - 2))

        @when(t, 4)
        def _():
            arrived(ph, 4, t - 4)
            start(one(ph, 5, t - 4))

        @when(t, 5)
        def _():
            arrived(ph, 5, t - 5)
            finish(t - 5)

    blk_a, blk_b = core * 8 + 2 * cx + cy, core * 8 + 4 + 2 * cy + cx
    tok_loads = [pltpu.make_async_copy(tok_hbm.at[blk], tok_ref.at[i], tok_s.at[i]) for i, blk in enumerate((blk_a, blk_b))]
    for q in range(WO_SLOTS):
        start(wo_copy(q))
    start(tok_loads)
    barrier = pltpu.get_barrier_semaphore()
    for dev in (sib, xn, yn):
        pl.semaphore_signal(barrier, inc=1, device_id=dev, device_id_type=MESH)
    pl.semaphore_wait(barrier, 3)
    acc_g[...] = jnp.zeros_like(acc_g)
    acc_u[...] = jnp.zeros_like(acc_u)
    for i in range(attn_ref.shape[1]):
        x_ref[:, i * BLK:(i + 1) * BLK] = attn_ref[:, i, :].astype(jnp.bfloat16)
    wait(tok_loads)

    def finish_attn(u, a, b):
        xres[u, 0] = (tok_ref[0, :, cols(u)].astype(f32) + a).astype(jnp.bfloat16).astype(f32)
        xres[u, 1] = (tok_ref[1, :, cols(u)].astype(f32) + b).astype(jnp.bfloat16).astype(f32)

    @pl.loop(0, Q + 6)
    def _(t):
        @when(t, 0)
        def _():
            wait(wo_copy(t))
            part[t] = jnp.dot(x_ref[...], wo[lax.rem(t, WO_SLOTS)], preferred_element_type=f32).reshape(16, 8, width)

            @pl.when(t + WO_SLOTS < Q)
            def _():
                start(wo_copy(t + WO_SLOTS))

            @pl.when(t < GU_SLOTS)
            def _():
                start(gu_copy(t))

            @pl.when((t >= GU_SLOTS) & (t < GU_SLOTS + WD_SLOTS))
            def _():
                start(wd_copy(t - GU_SLOTS))
        reduce_steps(0, t, finish_attn)

    drain(0, (0, 1, 2))
    sq = jnp.zeros((2, 8, 1), f32)
    for q in range(Q):
        sq = sq + jnp.sum(xres[q] * xres[q], axis=-1, keepdims=True)
    inv = lax.rsqrt(sq / (Q * width) + EPS)
    for q in range(Q):
        h = (xres[q] * inv * ln_ref[q]).astype(jnp.bfloat16).astype(f32)
        full[q, blk_a] = h[0]
        full[q, blk_b] = h[1]

    def finish_gather(u):
        wait(gu_copy(u))
        s = lax.rem(u, GU_SLOTS)
        h = full[u].reshape(rows, width).astype(jnp.bfloat16)
        acc_g[...] += jnp.dot(h, wg[s], preferred_element_type=f32)
        acc_u[...] += jnp.dot(h, wu[s], preferred_element_type=f32)

        @pl.when(u + GU_SLOTS < Q)
        def _():
            start(gu_copy(u + GU_SLOTS))

    @pl.loop(0, Q + 5)
    def _(t):
        gather_steps(0, t, finish_gather)

    drain(0, (3, 4, 5))

    @pl.loop(0, acc_g.shape[1] // 640)
    def _(n):
        c = pl.ds(pl.multiple_of(n * 640, 640), 640)
        mact[:, c] = (jax.nn.silu(acc_g[:, c]) * acc_u[:, c]).astype(jnp.bfloat16)

    def finish_mlp(u, a, b):
        full[u, blk_a] = (xres[u, 0] + a).astype(jnp.bfloat16).astype(f32)
        full[u, blk_b] = (xres[u, 1] + b).astype(jnp.bfloat16).astype(f32)

    def finish_out(u):
        out_ref[:, cols(u)] = full[u].reshape(rows, width).astype(jnp.bfloat16)

    @pl.loop(0, Q + 12)
    def _(t):
        @when(t, 0)
        def _():
            wait(wd_copy(t))
            part[t] = jnp.dot(mact[...], wd[lax.rem(t, WD_SLOTS)], preferred_element_type=f32).reshape(16, 8, width)

            @pl.when(t + WD_SLOTS < Q)
            def _():
                start(wd_copy(t + WD_SLOTS))
        reduce_steps(1, t, finish_mlp)
        gather_steps(1, t - 7, finish_out)

    drain(1, (0, 1, 2, 3, 4, 5))


def tail(cid, attn, tok_blocks, ln, w_out, w_gate, w_up, w_down):
    rows = attn.shape[0]
    depth = w_out.shape[0]
    d_model, inner = w_gate.shape
    width = d_model // Q
    vmem = pl.BlockSpec(memory_space=pltpu.VMEM)
    hbm = pl.BlockSpec(memory_space=pl.ANY)
    f32, bf16 = jnp.float32, jnp.bfloat16
    dma = pltpu.SemaphoreType.DMA
    return pl.pallas_call(
        tail_kernel,
        out_shape=jax.ShapeDtypeStruct((rows, d_model), bf16),
        in_specs=[vmem, hbm, vmem, hbm, hbm, hbm, hbm],
        out_specs=vmem,
        scratch_shapes=[
            pltpu.VMEM((rows, depth), bf16),
            pltpu.VMEM((2, 8, d_model), bf16),
            pltpu.VMEM((Q, 16, 8, width), f32),
            pltpu.VMEM((Q, 8, 8, width), f32),
            pltpu.VMEM((Q, 4, 8, width), f32),
            pltpu.VMEM((Q, 2, 8, width), f32),
            pltpu.VMEM((Q, 16, 8, width), f32),
            pltpu.VMEM((Q, 2, 8, width), f32),
            pltpu.VMEM((rows, inner), f32),
            pltpu.VMEM((rows, inner), f32),
            pltpu.VMEM((rows, inner), bf16),
            pltpu.VMEM((WO_SLOTS, depth, width), bf16),
            pltpu.VMEM((GU_SLOTS, width, inner), bf16),
            pltpu.VMEM((GU_SLOTS, width, inner), bf16),
            pltpu.VMEM((WD_SLOTS, inner, width), bf16),
            dma((2,)), dma((WO_SLOTS,)), dma((GU_SLOTS,)), dma((GU_SLOTS,)), dma((WD_SLOTS,)),
            dma((2, 10)), dma((2, 10, Q)),
        ],
        compiler_params=pltpu.CompilerParams(collective_id=cid, has_side_effects=True, vmem_limit_bytes=55 * 1024 * 1024),
        name="tail",
    )(attn, tok_blocks, ln, w_out, w_gate, w_up, w_down)


def solution(mesh):
    dim_count = mesh.shape['dim']
    mlp_axes = ('heads', 'dim')

    def layer_body(tokens, ln_attn, w_query, w_key, w_value, q_gain, k_gain, w_out, ln_mlp, w_gate, w_up, w_down, k_cache, v_cache, positions):
        rows = tokens.shape[0]
        heads_local = w_query.shape[1]
        kv_local = w_key.shape[1]
        slice_len = w_query.shape[2]
        head_dim = slice_len * dim_count
        half_dim = head_dim // 2
        q_group = heads_local // kv_local
        cache_len = k_cache.shape[1]
        dim_index = lax.axis_index('dim')

        inv_freq = np.tile(ROPE_BASE ** (-np.arange(half_dim) * 2.0 / head_dim), 2).astype(np.float32)

        def by_column(w):
            return w.transpose(1, 2, 0).reshape(-1, w.shape[0])

        qd, sn, vn, kt, vt = qkv(len(UP_SIZES) + 1, q_group, tokens, ln_attn[None], positions.astype(jnp.float32)[None], inv_freq[None], q_gain[None], k_gain[None],
                             by_column(w_query), by_column(w_key), by_column(w_value))
        k_new = kt.reshape(kv_local, slice_len, rows).transpose(2, 0, 1)
        v_new = vt.reshape(kv_local, slice_len, rows).transpose(2, 0, 1)

        n_units = jnp.maximum((positions - LOW + UNIT - 1) // UNIT, 1)
        k_t = k_cache.transpose(0, 2, 3, 1).reshape(rows, kv_local * slice_len, cache_len)
        v_t = v_cache.transpose(0, 2, 3, 1).reshape(rows, kv_local * slice_len, cache_len)
        which = jnp.sum((jnp.sum(n_units) > np.array(UP_SIZES[:-1]) * (BLK // UNIT)).astype(jnp.int32))
        branches = [functools.partial(attend, n, i, head_dim ** -0.5) for i, n in enumerate(UP_SIZES)]
        attn = lax.switch(which, branches, positions, qd, sn, vn, k_t, v_t)
        out = tail(len(UP_SIZES), attn, tokens.reshape(16, 8, -1), ln_mlp.reshape(Q, 1, -1), w_out.reshape(heads_local * slice_len, -1), w_gate, w_up, w_down)
        return out, k_new, v_new

    row_spec = P('dp', None)
    head_spec = P(None, 'heads', 'dim')
    cache_spec = P('dp', None, 'heads', 'dim')
    new_spec = P('dp', 'heads', 'dim')
    in_specs = (row_spec, P(None), head_spec, head_spec, head_spec, P('dim'), P('dim'), P('heads', 'dim', None), P(None), P(None, mlp_axes), P(None, mlp_axes), P(mlp_axes, None), cache_spec, cache_spec, P('dp'))
    out_specs = (row_spec, new_spec, new_spec)
    return jax.shard_map(layer_body, mesh=mesh, in_specs=in_specs, out_specs=out_specs, check_vma=False)
```

```python
import functools

import jax
import jax.numpy as jnp
import numpy as np
from jax import lax
from jax.experimental import pallas as pl
from jax.experimental.pallas import tpu as pltpu
from jax.sharding import PartitionSpec as P

EPS = 1e-6
ROPE_BASE = 1000000.0
MESH = pl.DeviceIdType.MESH

BLK = 128
LOW = 512
CH = 4
UCH = 8
UNIT = 16
SLOTS = 4
FIRST = 8
LEAD = 4
UP_SIZES = (232, 248, 256, 264, 272, 280, 296, 512)


def qkv_kernel(group, tok_ref, ln_ref, pos_ref, freq_ref, qg_ref, kg_ref, wq_hbm, wk_hbm, wv_hbm, qd_ref, sn_ref, vn_ref, kt_ref, vt_ref,
               hid, wq, wk, wv, own, other, gain_ref, gain_other, wsem, snd, rcv):
    partner = {"dim": 1 - lax.axis_index("dim")}
    rows, depth = tok_ref.shape
    n_q = own.shape[0] - 1
    steps = n_q // 2
    f32, bf16 = jnp.float32, jnp.bfloat16
    half = BLK // 2
    per_step = wq.shape[0] // steps

    def wq_copy(c):
        part = pl.ds(pl.multiple_of(c * per_step, per_step), per_step)
        return pltpu.make_async_copy(wq_hbm.at[part], wq.at[part], wsem.at[c])

    k_load = pltpu.make_async_copy(wk_hbm, wk, wsem.at[steps])
    v_load = pltpu.make_async_copy(wv_hbm, wv, wsem.at[steps + 1])

    def remote(src, dst, i):
        return pltpu.make_async_remote_copy(src_ref=src, dst_ref=dst, send_sem=snd.at[i], recv_sem=rcv.at[i],
                                            device_id=partner, device_id_type=MESH)

    def q_copy(c):
        part = pl.ds(2 * c, 2)
        return remote(own.at[part], other.at[part], c)

    k_copy = remote(own.at[pl.ds(n_q, 1)], other.at[pl.ds(n_q, 1)], steps)
    g_copy = remote(gain_ref, gain_other, steps + 1)

    k_load.start()
    for c in range(steps):
        wq_copy(c).start()
    v_load.start()
    barrier = pltpu.get_barrier_semaphore()
    pl.semaphore_signal(barrier, inc=1, device_id=partner, device_id_type=MESH)
    gain_ref[...] = jnp.zeros_like(gain_ref)
    for row, ref in enumerate((qg_ref, kg_ref)):
        gain_ref[row:row + 1, :half] = ref[...]
        gain_ref[row:row + 1, half:] = ref[...]
    pl.semaphore_wait(barrier, 1)

    @pl.loop(0, rows // 16, unroll=4)
    def _(i):
        part = pl.ds(pl.multiple_of(i * 16, 16), 16)
        x = tok_ref[part, :].astype(f32)
        inv = lax.rsqrt(jnp.mean(x * x, axis=-1, keepdims=True) + EPS)
        hid[part, :] = (x * inv * ln_ref[...]).astype(bf16)

    def project(w):
        return lax.dot_general(hid[...], w, (((1,), (1,)), ((), ())), preferred_element_type=f32)

    g_copy.start()
    k_load.wait()
    own[n_q] = project(wk[...])
    k_copy.start()

    @pl.loop(0, steps)
    def _(c):
        wq_copy(c).wait()
        u = project(wq[pl.ds(pl.multiple_of(c * per_step, per_step), per_step), :])

        own[2 * c] = u[:, :BLK]
        own[2 * c + 1] = u[:, BLK:]
        q_copy(c).start()

    v_load.wait()
    v_row = project(wv[...]).astype(bf16).astype(f32)
    vn_ref[...] = v_row
    vt_ref[...] = v_row.T.astype(bf16)
    low = lax.broadcasted_iota(jnp.int32, (rows, BLK), 1) < half
    angle = jnp.broadcast_to(pos_ref[...].astype(f32), (rows, rows)).T * freq_ref[...]
    cos_t = jnp.cos(angle)
    sin_t = jnp.sin(angle) * jnp.where(lax.axis_index("dim") == 0, -1.0, 1.0)

    def halves(x):
        return (jnp.sum(jnp.where(low, x, 0.0), axis=-1, keepdims=True), jnp.sum(jnp.where(low, 0.0, x), axis=-1, keepdims=True))

    def rotate(i, g):
        a, b = own[i], other[i]
        s_lo, s_hi = halves(a * a + b * b)
        inv = jnp.where(low, lax.rsqrt(s_lo / BLK + EPS), lax.rsqrt(s_hi / BLK + EPS))
        a, b = a * inv * gain_ref[g:g + 1, :], b * inv * gain_other[g:g + 1, :]
        return (a * cos_t + b * sin_t).astype(bf16).astype(f32), (b * cos_t - a * sin_t).astype(bf16).astype(f32)

    g_copy.wait_recv()
    k_copy.wait_recv()
    k_own, k_oth = rotate(n_q, 1)
    kt_ref[...] = k_own.T.astype(bf16)
    kr_own, kr_oth = pltpu.roll(k_own, half, 1), pltpu.roll(k_oth, half, 1)
    kk = [(jnp.where(low, k_own, kr_own), jnp.where(low, k_oth, kr_oth)),
          (jnp.where(low, kr_own, k_own), jnp.where(low, kr_oth, k_oth))]
    for i in range(n_q):
        if i % 2 == 0:
            q_copy(i // 2).wait_recv()
        q_own, q_oth = rotate(i, 0)
        kv = 2 * i // group
        new = halves(q_own * kk[kv][0] + q_oth * kk[kv][1])
        turned = pltpu.roll(q_own, half, 1)
        for e in range(2):
            row = i + n_q * e
            sn_ref[:, row, :] = jnp.broadcast_to(new[e], (rows, BLK))
            val = q_own if e == kv else turned
            qd_ref[:, row, :] = jnp.where(low, val, 0.0) if kv == 0 else jnp.where(low, 0.0, val)
    for c in range(steps):
        q_copy(c).wait_send()
    k_copy.wait_send()
    g_copy.wait_send()


def qkv(cid, group, tokens, ln, pos, freq, q_gain, k_gain, w_q, w_k, w_v):
    rows, depth = tokens.shape
    n_q = w_q.shape[0] // BLK
    steps = n_q // 2
    vmem = pl.BlockSpec(memory_space=pltpu.VMEM)
    hbm = pl.BlockSpec(memory_space=pl.ANY)
    f32, bf16 = jnp.float32, jnp.bfloat16
    heads = 2 * n_q
    dma = pltpu.SemaphoreType.DMA
    return pl.pallas_call(
        functools.partial(qkv_kernel, group),
        out_shape=(jax.ShapeDtypeStruct((rows, heads, BLK), f32), jax.ShapeDtypeStruct((rows, heads, BLK), f32),
                   jax.ShapeDtypeStruct((rows, BLK), f32), jax.ShapeDtypeStruct((BLK, rows), bf16), jax.ShapeDtypeStruct((BLK, rows), bf16)),
        in_specs=[vmem] * 6 + [hbm] * 3,
        out_specs=(vmem,) * 5,
        scratch_shapes=[
            pltpu.VMEM((rows, depth), bf16),
            pltpu.VMEM(w_q.shape, bf16),
            pltpu.VMEM(w_k.shape, bf16),
            pltpu.VMEM(w_v.shape, bf16),
            pltpu.VMEM((n_q + 1, rows, BLK), f32),
            pltpu.VMEM((n_q + 1, rows, BLK), f32),
            pltpu.VMEM((8, BLK), f32),
            pltpu.VMEM((8, BLK), f32),
            dma((steps + 2,)), dma((steps + 2,)), dma((steps + 2,)),
        ],
        compiler_params=pltpu.CompilerParams(collective_id=cid, has_side_effects=True, vmem_limit_bytes=62 * 1024 * 1024),
        name="qkv",
    )(tokens, ln, pos, freq, q_gain, k_gain, w_q, w_k, w_v)


def attn_kernel(n_up, scale, pos_ref, qd_ref, sn_ref, vn_ref, k_hbm, v_hbm, o_ref,
                off_ref, kbuf, vbuf, own_lo, own_up, pack, rlo, rup, ksem, vsem, send, slo_r, sup_r):
    partner = {"dim": 1 - lax.axis_index("dim")}
    rows = qd_ref.shape[0]
    n_ch = rows // CH
    n_uch = n_up // UCH
    up_blocks = own_up.shape[0] // rows
    per_blk = BLK // UNIT
    lane_up = lax.broadcasted_iota(jnp.int32, (16, BLK), 1)

    def kcopy(c):
        return pltpu.make_async_copy(k_hbm.at[pl.ds(c * CH, CH)], kbuf.at[lax.rem(c, SLOTS)], ksem.at[lax.rem(c, SLOTS)])

    def vcopy(c):
        return pltpu.make_async_copy(v_hbm.at[pl.ds(c * CH, CH)], vbuf.at[lax.rem(c, SLOTS)], vsem.at[lax.rem(c, SLOTS)])

    def lo_copy(c):
        part = pl.ds(c * CH, CH)
        return pltpu.make_async_remote_copy(src_ref=own_lo.at[part], dst_ref=rlo.at[part], send_sem=send.at[0],
                                            recv_sem=slo_r.at[c], device_id=partner, device_id_type=MESH)

    def up_copy(c):
        part = pl.ds(c * UCH, UCH)
        return pltpu.make_async_remote_copy(src_ref=pack.at[part], dst_ref=rup.at[part], send_sem=send.at[1],
                                            recv_sem=sup_r.at[c], device_id=partner, device_id_type=MESH)

    for c in range(SLOTS):
        kcopy(c).start()
    barrier = pltpu.get_barrier_semaphore()
    pl.semaphore_signal(barrier, inc=1, device_id=partner, device_id_type=MESH)
    pl.semaphore_wait(barrier, 1)
    for c in range(SLOTS):
        vcopy(c).start()
    row_units = up_blocks * per_blk

    def place(b, total):
        off_ref[b] = total
        return total + jnp.maximum((pos_ref[b] - LOW + UNIT - 1) // UNIT, 1)

    lax.fori_loop(0, rows, place, jnp.int32(0))

    @pl.loop(0, n_ch)
    def _(c):
        kcopy(c).wait()
        for r in range(CH):
            b = c * CH + r
            s = jnp.dot(qd_ref[b].astype(jnp.bfloat16), kbuf[lax.rem(c, SLOTS), r], preferred_element_type=jnp.float32)
            own_lo[b] = s[:, :LOW]
            for j in range(up_blocks):
                own_up[b * up_blocks + j] = s[:, LOW + j * BLK:LOW + (j + 1) * BLK]

        @pl.when(c + SLOTS < n_ch)
        def _():
            kcopy(c + SLOTS).start()

        @pl.when((c >= 1) & (c <= FIRST))
        def _():
            lo_copy(c - 1).start()

    def fill(c, row):
        for r in range(UCH):
            j = c * UCH + r
            block = None
            for k in range(per_blk):
                unit = j * per_blk + k
                following = jnp.minimum(row + 1, rows - 1)
                row = jnp.where(unit >= off_ref[following], following, row)
                src = jnp.minimum(unit - off_ref[row], row_units - 1)
                piece = pltpu.roll(own_up[row * up_blocks + src // per_blk], (k + per_blk - src % per_blk) % per_blk * UNIT, 1)
                block = piece if k == 0 else jnp.where(lane_up >= k * UNIT, piece, block)
            pack[j] = block

        @pl.when(c >= 1)
        def _():
            up_copy(c - 1).start()
        return row

    lax.fori_loop(0, n_uch, fill, jnp.int32(0))
    up_copy(n_uch - 1).start()

    @pl.loop(FIRST, FIRST + LEAD)
    def _(c):
        lo_copy(c).start()

    @pl.loop(0, n_uch)
    def _(c):
        up_copy(c).wait_recv()

    lane = lax.broadcasted_iota(jnp.int32, (8, 2 * 64), 1)
    first = lax.broadcasted_iota(jnp.int32, (8, 2 * 64), 0) < 4
    t_up = lane_up + LOW

    @pl.loop(0, n_ch)
    def _(c):
        @pl.when(c + FIRST + LEAD < n_ch)
        def _():
            lo_copy(c + FIRST + LEAD).start()

        vcopy(c).wait()
        lo_copy(c).wait_recv()
        for r in range(CH):
            b = c * CH + r
            pos = pos_ref[b]
            off = off_ref[b]
            parts = [(own_lo[b] + rlo[b]) * scale]
            skew = off % per_blk * UNIT
            slots = [pltpu.roll(rup[jnp.minimum(off // per_blk + j, n_up - 1)], (BLK - skew) % BLK, 1) for j in range(up_blocks + 1)]
            for j in range(up_blocks):
                got = jnp.where(lane_up < BLK - skew, slots[j], slots[j + 1])
                total = (own_up[b * up_blocks + j] + got) * scale
                parts.append(jnp.where(t_up + j * BLK < pos, total, -jnp.inf))
            s = jnp.concatenate(parts, axis=1)
            s_new = sn_ref[b][:, 0:1] * scale
            m = jnp.maximum(jnp.max(s, axis=1, keepdims=True), s_new)
            e = jnp.exp(s - m)
            e_new = jnp.exp(s_new - m)
            inv = 1.0 / (jnp.sum(e, axis=1, keepdims=True) + e_new)
            p = (e * inv).astype(jnp.bfloat16)
            p_new = (e_new * inv).astype(jnp.bfloat16).astype(jnp.float32)
            o = lax.dot_general(p, vbuf[lax.rem(c, SLOTS), r], (((1,), (1,)), ((), ())), preferred_element_type=jnp.float32)
            o = o + p_new * vn_ref[pl.ds(b, 1), :]
            even, odd = o[0:8], o[8:16]
            o_ref[b] = jnp.where(lane < 64, jnp.where(first, even, pltpu.roll(even, 64, 1)), jnp.where(first, pltpu.roll(odd, 64, 1), odd))

        @pl.when(c + SLOTS < n_ch)
        def _():
            vcopy(c + SLOTS).start()

    pltpu.make_async_remote_copy(src_ref=own_lo, dst_ref=rlo, send_sem=send.at[0], recv_sem=slo_r.at[0],
                                 device_id=partner, device_id_type=MESH).wait_send()
    pltpu.make_async_remote_copy(src_ref=pack, dst_ref=rup, send_sem=send.at[1], recv_sem=sup_r.at[0],
                                 device_id=partner, device_id_type=MESH).wait_send()


def attend(n_up, cid, scale, pos, qd, sn, vn, k_t, v_t):
    rows = qd.shape[0]
    n_ch = rows // CH
    n_uch = n_up // UCH
    cache_len = k_t.shape[2]
    up_blocks = (cache_len - LOW) // BLK
    smem = pl.BlockSpec(memory_space=pltpu.SMEM)
    vmem = pl.BlockSpec(memory_space=pltpu.VMEM)
    hbm = pl.BlockSpec(memory_space=pl.ANY)
    return pl.pallas_call(
        functools.partial(attn_kernel, n_up, scale),
        out_shape=jax.ShapeDtypeStruct((rows, 8, 128), jnp.float32),
        in_specs=[smem, vmem, vmem, vmem, hbm, hbm],
        out_specs=vmem,
        scratch_shapes=[
            pltpu.SMEM((rows,), jnp.int32),
            pltpu.VMEM((SLOTS, CH, 128, cache_len), jnp.bfloat16),
            pltpu.VMEM((SLOTS, CH, 128, cache_len), jnp.bfloat16),
            pltpu.VMEM((rows, 16, LOW), jnp.float32),
            pltpu.VMEM((rows * up_blocks, 16, BLK), jnp.float32),
            pltpu.VMEM((n_up, 16, BLK), jnp.float32),
            pltpu.VMEM((rows, 16, LOW), jnp.float32),
            pltpu.VMEM((n_up, 16, BLK), jnp.float32),
            pltpu.SemaphoreType.DMA((SLOTS,)),
            pltpu.SemaphoreType.DMA((SLOTS,)),
            pltpu.SemaphoreType.DMA((2,)),
            pltpu.SemaphoreType.DMA((n_ch,)),
            pltpu.SemaphoreType.DMA((n_uch,)),
        ],
        compiler_params=pltpu.CompilerParams(collective_id=cid, has_side_effects=True, vmem_limit_bytes=40 * 1024 * 1024),
        name=f"attend_{n_up}",
    )(pos, qd, sn, vn, k_t, v_t)


Q = 10
HOP = 3
WO_SLOTS = 4
GU_SLOTS = 4
WD_SLOTS = 3


def tail_kernel(attn_ref, tok_hbm, ln_ref, wo_hbm, wg_hbm, wu_hbm, wd_hbm, out_ref,
                x_ref, tok_ref, part, r1, r2, r3, full, xres, acc_g, acc_u, mact, wo, wg, wu, wd,
                tok_s, wo_s, wg_s, wu_s, wd_s, snd, rcv):
    heads = lax.axis_index("heads")
    core, cx, cy = lax.rem(heads, 2), heads // 2, lax.axis_index("dim")
    sib = {"heads": 2 * cx + 1 - core}
    xn = {"heads": 2 * (1 - cx) + core}
    yn = {"dim": 1 - cy}
    width = part.shape[3]
    rows = 16 * 8
    f32 = jnp.float32

    def cols(q):
        return pl.ds(pl.multiple_of(q * width, width), width)

    def wo_copy(q):
        s = lax.rem(q, WO_SLOTS)
        return [pltpu.make_async_copy(wo_hbm.at[:, cols(q)], wo.at[s], wo_s.at[s])]

    def gu_copy(q):
        s = lax.rem(q, GU_SLOTS)
        return [pltpu.make_async_copy(wg_hbm.at[cols(q)], wg.at[s], wg_s.at[s]),
                pltpu.make_async_copy(wu_hbm.at[cols(q)], wu.at[s], wu_s.at[s])]

    def wd_copy(q):
        s = lax.rem(q, WD_SLOTS)
        return [pltpu.make_async_copy(wd_hbm.at[:, cols(q)], wd.at[s], wd_s.at[s])]

    def start(copies):
        for cp in copies:
            cp.start()

    def wait(copies):
        for cp in copies:
            cp.wait()

    def remote(ph, st, q, src, dst, dev):
        return pltpu.make_async_remote_copy(src_ref=src, dst_ref=dst, send_sem=snd.at[ph, st], recv_sem=rcv.at[ph, st, q],
                                            device_id=dev, device_id_type=MESH)

    def stage(ph, k, q, sem_q):
        if k == 0:
            return [remote(ph, 0, sem_q, part.at[q, pl.ds(8 * (1 - core), 8)], r1.at[q], sib)]
        if k == 1:
            return [remote(ph, 1, sem_q, r1.at[q, pl.ds(2 * (1 - cx), 2)], r2.at[q, pl.ds(0, 2)], xn),
                    remote(ph, 2, sem_q, r1.at[q, pl.ds(4 + 2 * (1 - cy), 2)], r2.at[q, pl.ds(2, 2)], yn)]
        if k == 2:
            return [remote(ph, 3, sem_q, r2.at[q, pl.ds(1 - cy, 1)], r3.at[q, pl.ds(0, 1)], yn),
                    remote(ph, 4, sem_q, r2.at[q, pl.ds(2 + 1 - cx, 1)], r3.at[q, pl.ds(1, 1)], xn)]
        blk_a, blk_b = core * 8, core * 8 + 4
        if k == 3:
            a, b = full.at[q, pl.ds(blk_a + 2 * cx + cy, 1)], full.at[q, pl.ds(blk_b + 2 * cy + cx, 1)]
            return [remote(ph, 5, sem_q, a, a, yn), remote(ph, 6, sem_q, b, b, xn)]
        if k == 4:
            a, b = full.at[q, pl.ds(blk_a + 2 * cx, 2)], full.at[q, pl.ds(blk_b + 2 * cy, 2)]
            return [remote(ph, 7, sem_q, a, a, xn), remote(ph, 8, sem_q, b, b, yn)]
        a = full.at[q, pl.ds(blk_a, 8)]
        return [remote(ph, 9, sem_q, a, a, sib)]

    def one(ph, k, q):
        return stage(ph, k, q, q)

    def drain(ph, ks):
        for k in ks:
            for cp in stage(ph, k, slice(None), 0):
                cp.wait_send()

    def arrived(ph, k, q):
        for cp in one(ph, k, q):
            cp.wait_recv()

    def when(t, lo):
        return pl.when((t >= lo) & (t < lo + Q))

    def reduce_steps(ph, t, finish):
        @when(t, 2)
        def _():
            u = t - 2
            arrived(ph, 0, u)
            r1[u] = r1[u] + part[u, pl.ds(8 * core, 8)]
            start(one(ph, 1, u))

        @when(t, 0)
        def _():
            start(one(ph, 0, t))

        @when(t, 2 + HOP)
        def _():
            u = t - 2 - HOP
            arrived(ph, 1, u)
            r2[u, pl.ds(0, 2)] = r2[u, pl.ds(0, 2)] + r1[u, pl.ds(2 * cx, 2)]
            r2[u, pl.ds(2, 2)] = r2[u, pl.ds(2, 2)] + r1[u, pl.ds(4 + 2 * cy, 2)]
            start(one(ph, 2, u))

        @when(t, 2 + 2 * HOP)
        def _():
            u = t - 2 - 2 * HOP
            arrived(ph, 2, u)
            finish(u, r3[u, 0] + r2[u, cy], r3[u, 1] + r2[u, 2 + cx])

    def gather_start(ph, t):
        @when(t, 0)
        def _():
            start(one(ph, 3, t))

    def gather_steps(ph, t, finish):
        @when(t, HOP)
        def _():
            arrived(ph, 3, t - HOP)
            start(one(ph, 4, t - HOP))

        @when(t, 2 * HOP)
        def _():
            arrived(ph, 4, t - 2 * HOP)
            start(one(ph, 5, t - 2 * HOP))

        @when(t, 2 * HOP + 2)
        def _():
            arrived(ph, 5, t - 2 * HOP - 2)
            finish(t - 2 * HOP - 2)

    blk_a, blk_b = core * 8 + 2 * cx + cy, core * 8 + 4 + 2 * cy + cx
    tok_loads = [pltpu.make_async_copy(tok_hbm.at[blk], tok_ref.at[i], tok_s.at[i]) for i, blk in enumerate((blk_a, blk_b))]
    for q in range(WO_SLOTS):
        start(wo_copy(q))
    start(tok_loads)
    barrier = pltpu.get_barrier_semaphore()
    for dev in (sib, xn, yn):
        pl.semaphore_signal(barrier, inc=1, device_id=dev, device_id_type=MESH)
    pl.semaphore_wait(barrier, 3)
    acc_g[...] = jnp.zeros_like(acc_g)
    acc_u[...] = jnp.zeros_like(acc_u)
    for i in range(attn_ref.shape[1]):
        x_ref[:, i * BLK:(i + 1) * BLK] = attn_ref[:, i, :].astype(jnp.bfloat16)
    wait(tok_loads)

    def finish_attn(u, a, b):
        xres[u, 0] = (tok_ref[0, :, cols(u)].astype(f32) + a).astype(jnp.bfloat16).astype(f32)
        xres[u, 1] = (tok_ref[1, :, cols(u)].astype(f32) + b).astype(jnp.bfloat16).astype(f32)

    @pl.loop(0, Q + 2 + 2 * HOP)
    def _(t):
        @when(t, 0)
        def _():
            wait(wo_copy(t))
            part[t] = jnp.dot(x_ref[...], wo[lax.rem(t, WO_SLOTS)], preferred_element_type=f32).reshape(16, 8, width)

            @pl.when(t + WO_SLOTS < Q)
            def _():
                start(wo_copy(t + WO_SLOTS))

            @pl.when(t < GU_SLOTS)
            def _():
                start(gu_copy(t))

            @pl.when((t >= GU_SLOTS) & (t < GU_SLOTS + WD_SLOTS))
            def _():
                start(wd_copy(t - GU_SLOTS))
        reduce_steps(0, t, finish_attn)

    drain(0, (0, 1, 2))
    sq = jnp.zeros((2, 8, 1), f32)
    for q in range(Q):
        sq = sq + jnp.sum(xres[q] * xres[q], axis=-1, keepdims=True)
    inv = lax.rsqrt(sq / (Q * width) + EPS)
    for q in range(Q):
        h = (xres[q] * inv * ln_ref[q]).astype(jnp.bfloat16).astype(f32)
        full[q, blk_a] = h[0]
        full[q, blk_b] = h[1]

    def finish_gather(u):
        wait(gu_copy(u))
        s = lax.rem(u, GU_SLOTS)
        h = full[u].reshape(rows, width).astype(jnp.bfloat16)
        acc_g[...] += jnp.dot(h, wg[s], preferred_element_type=f32)
        acc_u[...] += jnp.dot(h, wu[s], preferred_element_type=f32)

        @pl.when(u + GU_SLOTS < Q)
        def _():
            start(gu_copy(u + GU_SLOTS))

    @pl.loop(0, Q + 2 + 2 * HOP)
    def _(t):
        gather_start(0, t)
        gather_steps(0, t, finish_gather)

    drain(0, (3, 4, 5))

    @pl.loop(0, acc_g.shape[1] // 640)
    def _(n):
        c = pl.ds(pl.multiple_of(n * 640, 640), 640)
        mact[:, c] = (jax.nn.silu(acc_g[:, c]) * acc_u[:, c]).astype(jnp.bfloat16)

    def finish_mlp(u, a, b):
        full[u, blk_a] = (xres[u, 0] + a).astype(jnp.bfloat16).astype(f32)
        full[u, blk_b] = (xres[u, 1] + b).astype(jnp.bfloat16).astype(f32)

    def finish_out(u):
        out_ref[:, cols(u)] = full[u].reshape(rows, width).astype(jnp.bfloat16)

    lag = 3 + 2 * HOP

    @pl.loop(0, Q + lag + 2 + 2 * HOP)
    def _(t):
        gather_start(1, t - lag)

        @when(t, 0)
        def _():
            wait(wd_copy(t))
            part[t] = jnp.dot(mact[...], wd[lax.rem(t, WD_SLOTS)], preferred_element_type=f32).reshape(16, 8, width)

            @pl.when(t + WD_SLOTS < Q)
            def _():
                start(wd_copy(t + WD_SLOTS))
        reduce_steps(1, t, finish_mlp)
        gather_steps(1, t - lag, finish_out)

    drain(1, (0, 1, 2, 3, 4, 5))


def tail(cid, attn, tok_blocks, ln, w_out, w_gate, w_up, w_down):
    rows = attn.shape[0]
    depth = w_out.shape[0]
    d_model, inner = w_gate.shape
    width = d_model // Q
    vmem = pl.BlockSpec(memory_space=pltpu.VMEM)
    hbm = pl.BlockSpec(memory_space=pl.ANY)
    f32, bf16 = jnp.float32, jnp.bfloat16
    dma = pltpu.SemaphoreType.DMA
    return pl.pallas_call(
        tail_kernel,
        out_shape=jax.ShapeDtypeStruct((rows, d_model), bf16),
        in_specs=[vmem, hbm, vmem, hbm, hbm, hbm, hbm],
        out_specs=vmem,
        scratch_shapes=[
            pltpu.VMEM((rows, depth), bf16),
            pltpu.VMEM((2, 8, d_model), bf16),
            pltpu.VMEM((Q, 16, 8, width), f32),
            pltpu.VMEM((Q, 8, 8, width), f32),
            pltpu.VMEM((Q, 4, 8, width), f32),
            pltpu.VMEM((Q, 2, 8, width), f32),
            pltpu.VMEM((Q, 16, 8, width), f32),
            pltpu.VMEM((Q, 2, 8, width), f32),
            pltpu.VMEM((rows, inner), f32),
            pltpu.VMEM((rows, inner), f32),
            pltpu.VMEM((rows, inner), bf16),
            pltpu.VMEM((WO_SLOTS, depth, width), bf16),
            pltpu.VMEM((GU_SLOTS, width, inner), bf16),
            pltpu.VMEM((GU_SLOTS, width, inner), bf16),
            pltpu.VMEM((WD_SLOTS, inner, width), bf16),
            dma((2,)), dma((WO_SLOTS,)), dma((GU_SLOTS,)), dma((GU_SLOTS,)), dma((WD_SLOTS,)),
            dma((2, 10)), dma((2, 10, Q)),
        ],
        compiler_params=pltpu.CompilerParams(collective_id=cid, has_side_effects=True, vmem_limit_bytes=55 * 1024 * 1024),
        name="tail",
    )(attn, tok_blocks, ln, w_out, w_gate, w_up, w_down)


def solution(mesh):
    dim_count = mesh.shape['dim']
    mlp_axes = ('heads', 'dim')

    def layer_body(tokens, ln_attn, w_query, w_key, w_value, q_gain, k_gain, w_out, ln_mlp, w_gate, w_up, w_down, k_cache, v_cache, positions):
        rows = tokens.shape[0]
        heads_local = w_query.shape[1]
        kv_local = w_key.shape[1]
        slice_len = w_query.shape[2]
        head_dim = slice_len * dim_count
        half_dim = head_dim // 2
        q_group = heads_local // kv_local
        cache_len = k_cache.shape[1]
        dim_index = lax.axis_index('dim')

        inv_freq = np.tile(ROPE_BASE ** (-np.arange(half_dim) * 2.0 / head_dim), 2).astype(np.float32)

        def by_column(w):
            return w.transpose(1, 2, 0).reshape(-1, w.shape[0])

        qd, sn, vn, kt, vt = qkv(len(UP_SIZES) + 1, q_group, tokens, ln_attn[None], positions[None], inv_freq[None], q_gain[None], k_gain[None],
                             by_column(w_query), by_column(w_key), by_column(w_value))
        k_new = kt.reshape(kv_local, slice_len, rows).transpose(2, 0, 1)
        v_new = vt.reshape(kv_local, slice_len, rows).transpose(2, 0, 1)

        n_units = jnp.maximum((positions - LOW + UNIT - 1) // UNIT, 1)
        k_t = k_cache.transpose(0, 2, 3, 1).reshape(rows, kv_local * slice_len, cache_len)
        v_t = v_cache.transpose(0, 2, 3, 1).reshape(rows, kv_local * slice_len, cache_len)
        total = jnp.sum(n_units)
        which = sum((total > n * (BLK // UNIT)).astype(jnp.int32) for n in UP_SIZES[:-1])
        branches = [functools.partial(attend, n, i, head_dim ** -0.5) for i, n in enumerate(UP_SIZES)]
        attn = lax.switch(which, branches, positions, qd, sn, vn, k_t, v_t)
        out = tail(len(UP_SIZES), attn, tokens.reshape(16, 8, -1), ln_mlp.reshape(Q, 1, -1), w_out.reshape(heads_local * slice_len, -1), w_gate, w_up, w_down)
        return out, k_new, v_new

    row_spec = P('dp', None)
    head_spec = P(None, 'heads', 'dim')
    cache_spec = P('dp', None, 'heads', 'dim')
    new_spec = P('dp', 'heads', 'dim')
    in_specs = (row_spec, P(None), head_spec, head_spec, head_spec, P('dim'), P('dim'), P('heads', 'dim', None), P(None), P(None, mlp_axes), P(None, mlp_axes), P(mlp_axes, None), cache_spec, cache_spec, P('dp'))
    out_specs = (row_spec, new_spec, new_spec)
    return jax.shard_map(layer_body, mesh=mesh, in_specs=in_specs, out_specs=out_specs, check_vma=False)
```

```python
import functools

import jax
import jax.numpy as jnp
import numpy as np
from jax import lax
from jax.experimental import pallas as pl
from jax.experimental.pallas import tpu as pltpu
from jax.sharding import PartitionSpec as P

EPS = 1e-6
ROPE_BASE = 1000000.0
MESH = pl.DeviceIdType.MESH

BLK = 128
LOW = 512
CH = 4
UCH = 8
UNIT = 16
SLOTS = 4
FIRST = 8
LEAD = 4
UP_FIRST = 232
UP_SIZES = tuple(UP_FIRST + UCH * i for i in range(9)) + (512,)


def qkv_kernel(group, tok_ref, ln_ref, pos_ref, freq_ref, qg_ref, kg_ref, wq_hbm, wk_hbm, wv_hbm, qd_ref, vn_ref, kt_ref, vt_ref,
               hid, wq, wk, wv, own, other, gain_ref, gain_other, wsem, snd, rcv):
    partner = {"dim": 1 - lax.axis_index("dim")}
    rows, depth = tok_ref.shape
    n_q = own.shape[0] - 1
    steps = n_q // 2
    f32, bf16 = jnp.float32, jnp.bfloat16
    half = BLK // 2
    per_step = wq.shape[0] // steps

    def wq_copy(c):
        part = pl.ds(pl.multiple_of(c * per_step, per_step), per_step)
        return pltpu.make_async_copy(wq_hbm.at[part], wq.at[part], wsem.at[c])

    k_load = pltpu.make_async_copy(wk_hbm, wk, wsem.at[steps])
    v_load = pltpu.make_async_copy(wv_hbm, wv, wsem.at[steps + 1])

    def remote(src, dst, i):
        return pltpu.make_async_remote_copy(src_ref=src, dst_ref=dst, send_sem=snd.at[i], recv_sem=rcv.at[i],
                                            device_id=partner, device_id_type=MESH)

    def q_copy(c):
        part = pl.ds(2 * c, 2)
        return remote(own.at[part], other.at[part], c)

    k_copy = remote(own.at[pl.ds(n_q, 1)], other.at[pl.ds(n_q, 1)], steps)
    g_copy = remote(gain_ref, gain_other, steps + 1)

    k_load.start()
    for c in range(steps):
        wq_copy(c).start()
    v_load.start()
    barrier = pltpu.get_barrier_semaphore()
    pl.semaphore_signal(barrier, inc=1, device_id=partner, device_id_type=MESH)
    gain_ref[...] = jnp.zeros_like(gain_ref)
    for row, ref in enumerate((qg_ref, kg_ref)):
        gain_ref[row:row + 1, :half] = ref[...]
        gain_ref[row:row + 1, half:] = ref[...]
    pl.semaphore_wait(barrier, 1)

    @pl.loop(0, rows // 16, unroll=4)
    def _(i):
        part = pl.ds(pl.multiple_of(i * 16, 16), 16)
        x = tok_ref[part, :].astype(f32)
        inv = lax.rsqrt(jnp.mean(x * x, axis=-1, keepdims=True) + EPS)
        hid[part, :] = (x * inv * ln_ref[...]).astype(bf16)

    def project(w):
        return lax.dot_general(hid[...], w, (((1,), (1,)), ((), ())), preferred_element_type=f32)

    g_copy.start()
    k_load.wait()
    own[n_q] = project(wk[...])
    k_copy.start()

    @pl.loop(0, steps)
    def _(c):
        wq_copy(c).wait()
        u = project(wq[pl.ds(pl.multiple_of(c * per_step, per_step), per_step), :])

        own[2 * c] = u[:, :BLK]
        own[2 * c + 1] = u[:, BLK:]
        q_copy(c).start()

    v_load.wait()
    v_row = project(wv[...]).astype(bf16).astype(f32)
    vn_ref[...] = v_row
    vt_ref[...] = v_row.T.astype(bf16)
    low = lax.broadcasted_iota(jnp.int32, (rows, BLK), 1) < half
    angle = jnp.broadcast_to(pos_ref[...].astype(f32), (rows, rows)).T * freq_ref[...]
    cos_t = jnp.cos(angle)
    sin_t = jnp.sin(angle) * jnp.where(lax.axis_index("dim") == 0, -1.0, 1.0)

    def halves(x):
        return (jnp.sum(jnp.where(low, x, 0.0), axis=-1, keepdims=True), jnp.sum(jnp.where(low, 0.0, x), axis=-1, keepdims=True))

    def rotate(i, g):
        a, b = own[i], other[i]
        s_lo, s_hi = halves(a * a + b * b)
        inv = jnp.where(low, lax.rsqrt(s_lo / BLK + EPS), lax.rsqrt(s_hi / BLK + EPS))
        a, b = a * inv * gain_ref[g:g + 1, :], b * inv * gain_other[g:g + 1, :]
        return (a * cos_t + b * sin_t).astype(bf16).astype(f32), (b * cos_t - a * sin_t).astype(bf16).astype(f32)

    g_copy.wait_recv()
    k_copy.wait_recv()
    k_own, k_oth = rotate(n_q, 1)
    kt_ref[...] = k_own.T.astype(bf16)
    kr_own, kr_oth = pltpu.roll(k_own, half, 1), pltpu.roll(k_oth, half, 1)
    kk = [(jnp.where(low, k_own, kr_own), jnp.where(low, k_oth, kr_oth)),
          (jnp.where(low, kr_own, k_own), jnp.where(low, kr_oth, k_oth))]
    for i in range(n_q):
        if i % 2 == 0:
            q_copy(i // 2).wait_recv()
        q_own, q_oth = rotate(i, 0)
        kv = 2 * i // group
        new = halves(q_own * kk[kv][0] + q_oth * kk[kv][1])
        turned = pltpu.roll(q_own, half, 1)
        for e in range(2):
            row = i + n_q * e
            val = q_own if e == kv else turned
            qd_ref[:, row, :] = jnp.where(low, val, new[e]) if kv == 0 else jnp.where(low, new[e], val)
    for c in range(steps):
        q_copy(c).wait_send()
    k_copy.wait_send()
    g_copy.wait_send()


def qkv(cid, group, tokens, ln, pos, freq, q_gain, k_gain, w_q, w_k, w_v):
    rows, depth = tokens.shape
    n_q = w_q.shape[0] // BLK
    steps = n_q // 2
    vmem = pl.BlockSpec(memory_space=pltpu.VMEM)
    hbm = pl.BlockSpec(memory_space=pl.ANY)
    f32, bf16 = jnp.float32, jnp.bfloat16
    heads = 2 * n_q
    dma = pltpu.SemaphoreType.DMA
    return pl.pallas_call(
        functools.partial(qkv_kernel, group),
        out_shape=(jax.ShapeDtypeStruct((rows, heads, BLK), f32), jax.ShapeDtypeStruct((rows, BLK), f32), jax.ShapeDtypeStruct((BLK, rows), bf16), jax.ShapeDtypeStruct((BLK, rows), bf16)),
        in_specs=[vmem] * 6 + [hbm] * 3,
        out_specs=(vmem,) * 4,
        scratch_shapes=[
            pltpu.VMEM((rows, depth), bf16),
            pltpu.VMEM(w_q.shape, bf16),
            pltpu.VMEM(w_k.shape, bf16),
            pltpu.VMEM(w_v.shape, bf16),
            pltpu.VMEM((n_q + 1, rows, BLK), f32),
            pltpu.VMEM((n_q + 1, rows, BLK), f32),
            pltpu.VMEM((8, BLK), f32),
            pltpu.VMEM((8, BLK), f32),
            dma((steps + 2,)), dma((steps + 2,)), dma((steps + 2,)),
        ],
        compiler_params=pltpu.CompilerParams(collective_id=cid, has_side_effects=True, vmem_limit_bytes=62 * 1024 * 1024),
        name="qkv",
    )(tokens, ln, pos, freq, q_gain, k_gain, w_q, w_k, w_v)


def attn_kernel(n_up, scale, pos_ref, qd_ref, vn_ref, k_hbm, v_hbm, o_ref,
                off_ref, kbuf, vbuf, own_lo, own_up, pack, rlo, rup, ksem, vsem, send, slo_r, sup_r):
    partner = {"dim": 1 - lax.axis_index("dim")}
    rows = qd_ref.shape[0]
    n_ch = rows // CH
    n_uch = n_up // UCH
    up_blocks = own_up.shape[0] // rows
    per_blk = BLK // UNIT
    lane_up = lax.broadcasted_iota(jnp.int32, (16, BLK), 1)
    kv_row = lax.broadcasted_iota(jnp.int32, (16, BLK), 0) // 4 % 2
    q_lanes = kv_row == lane_up // 64

    def kcopy(c):
        return pltpu.make_async_copy(k_hbm.at[pl.ds(c * CH, CH)], kbuf.at[lax.rem(c, SLOTS)], ksem.at[lax.rem(c, SLOTS)])

    def vcopy(c):
        return pltpu.make_async_copy(v_hbm.at[pl.ds(c * CH, CH)], vbuf.at[lax.rem(c, SLOTS)], vsem.at[lax.rem(c, SLOTS)])

    def lo_copy(c):
        part = pl.ds(c * CH, CH)
        return pltpu.make_async_remote_copy(src_ref=own_lo.at[part], dst_ref=rlo.at[part], send_sem=send.at[0],
                                            recv_sem=slo_r.at[c], device_id=partner, device_id_type=MESH)

    def up_copy(c):
        part = pl.ds(c * UCH, UCH)
        return pltpu.make_async_remote_copy(src_ref=pack.at[part], dst_ref=rup.at[part], send_sem=send.at[1],
                                            recv_sem=sup_r.at[c], device_id=partner, device_id_type=MESH)

    for c in range(SLOTS):
        kcopy(c).start()
    barrier = pltpu.get_barrier_semaphore()
    pl.semaphore_signal(barrier, inc=1, device_id=partner, device_id_type=MESH)
    pl.semaphore_wait(barrier, 1)
    for c in range(SLOTS):
        vcopy(c).start()
    row_units = up_blocks * per_blk

    @pl.loop(0, n_ch)
    def _(c):
        kcopy(c).wait()
        for r in range(CH):
            b = c * CH + r
            s = jnp.dot(jnp.where(q_lanes, qd_ref[b], 0.0).astype(jnp.bfloat16), kbuf[lax.rem(c, SLOTS), r], preferred_element_type=jnp.float32)
            own_lo[b] = s[:, :LOW]
            for j in range(up_blocks):
                own_up[b * up_blocks + j] = s[:, LOW + j * BLK:LOW + (j + 1) * BLK]

        @pl.when(c + SLOTS < n_ch)
        def _():
            kcopy(c + SLOTS).start()

        @pl.when((c >= 1) & (c <= FIRST))
        def _():
            lo_copy(c - 1).start()

    def place(b, total):
        off_ref[b] = total
        return total + jnp.maximum((pos_ref[b] - LOW + UNIT - 1) // UNIT, 1)

    lax.fori_loop(0, rows, place, jnp.int32(0))

    def fill(c, row):
        for r in range(UCH):
            j = c * UCH + r
            block = None
            for k in range(per_blk):
                unit = j * per_blk + k
                following = jnp.minimum(row + 1, rows - 1)
                row = jnp.where(unit >= off_ref[following], following, row)
                src = jnp.minimum(unit - off_ref[row], row_units - 1)
                piece = pltpu.roll(own_up[row * up_blocks + src // per_blk], (k + per_blk - src % per_blk) % per_blk * UNIT, 1)
                block = piece if k == 0 else jnp.where(lane_up >= k * UNIT, piece, block)
            pack[j] = block

        @pl.when(c >= 1)
        def _():
            up_copy(c - 1).start()
        return row

    lax.fori_loop(0, n_uch, fill, jnp.int32(0))
    up_copy(n_uch - 1).start()

    @pl.loop(FIRST, FIRST + LEAD)
    def _(c):
        lo_copy(c).start()

    @pl.loop(0, n_uch)
    def _(c):
        up_copy(c).wait_recv()

    lane = lax.broadcasted_iota(jnp.int32, (8, 2 * 64), 1)
    first = lax.broadcasted_iota(jnp.int32, (8, 2 * 64), 0) < 4
    t_up = lane_up + LOW

    @pl.loop(0, n_ch)
    def _(c):
        @pl.when(c + FIRST + LEAD < n_ch)
        def _():
            lo_copy(c + FIRST + LEAD).start()

        vcopy(c).wait()
        lo_copy(c).wait_recv()
        for r in range(CH):
            b = c * CH + r
            pos = pos_ref[b]
            off = off_ref[b]
            parts = [(own_lo[b] + rlo[b]) * scale]
            skew = off % per_blk * UNIT
            slots = [pltpu.roll(rup[jnp.minimum(off // per_blk + j, n_up - 1)], (BLK - skew) % BLK, 1) for j in range(up_blocks + 1)]
            for j in range(up_blocks):
                got = jnp.where(lane_up < BLK - skew, slots[j], slots[j + 1])
                total = (own_up[b * up_blocks + j] + got) * scale
                parts.append(jnp.where(t_up + j * BLK < pos, total, -jnp.inf))
            s = jnp.concatenate(parts, axis=1)
            q_row = qd_ref[b]
            s_new = jnp.where(kv_row[:, 0:1] == 0, q_row[:, BLK - 1:], q_row[:, 0:1]) * scale
            m = jnp.maximum(jnp.max(s, axis=1, keepdims=True), s_new)
            e = jnp.exp(s - m)
            e_new = jnp.exp(s_new - m)
            inv = 1.0 / (jnp.sum(e, axis=1, keepdims=True) + e_new)
            p = (e * inv).astype(jnp.bfloat16)
            p_new = (e_new * inv).astype(jnp.bfloat16).astype(jnp.float32)
            o = lax.dot_general(p, vbuf[lax.rem(c, SLOTS), r], (((1,), (1,)), ((), ())), preferred_element_type=jnp.float32)
            o = o + p_new * vn_ref[pl.ds(b, 1), :]
            even, odd = o[0:8], o[8:16]
            o_ref[b] = jnp.where(lane < 64, jnp.where(first, even, pltpu.roll(even, 64, 1)), jnp.where(first, pltpu.roll(odd, 64, 1), odd))

        @pl.when(c + SLOTS < n_ch)
        def _():
            vcopy(c + SLOTS).start()

    pltpu.make_async_remote_copy(src_ref=own_lo, dst_ref=rlo, send_sem=send.at[0], recv_sem=slo_r.at[0],
                                 device_id=partner, device_id_type=MESH).wait_send()
    pltpu.make_async_remote_copy(src_ref=pack, dst_ref=rup, send_sem=send.at[1], recv_sem=sup_r.at[0],
                                 device_id=partner, device_id_type=MESH).wait_send()


def attend(n_up, cid, scale, pos, qd, vn, k_t, v_t):
    rows = qd.shape[0]
    n_ch = rows // CH
    n_uch = n_up // UCH
    cache_len = k_t.shape[2]
    up_blocks = (cache_len - LOW) // BLK
    smem = pl.BlockSpec(memory_space=pltpu.SMEM)
    vmem = pl.BlockSpec(memory_space=pltpu.VMEM)
    hbm = pl.BlockSpec(memory_space=pl.ANY)
    return pl.pallas_call(
        functools.partial(attn_kernel, n_up, scale),
        out_shape=jax.ShapeDtypeStruct((rows, 8, 128), jnp.float32),
        in_specs=[smem, vmem, vmem, hbm, hbm],
        out_specs=vmem,
        scratch_shapes=[
            pltpu.SMEM((rows,), jnp.int32),
            pltpu.VMEM((SLOTS, CH, 128, cache_len), jnp.bfloat16),
            pltpu.VMEM((SLOTS, CH, 128, cache_len), jnp.bfloat16),
            pltpu.VMEM((rows, 16, LOW), jnp.float32),
            pltpu.VMEM((rows * up_blocks, 16, BLK), jnp.float32),
            pltpu.VMEM((n_up, 16, BLK), jnp.float32),
            pltpu.VMEM((rows, 16, LOW), jnp.float32),
            pltpu.VMEM((n_up, 16, BLK), jnp.float32),
            pltpu.SemaphoreType.DMA((SLOTS,)),
            pltpu.SemaphoreType.DMA((SLOTS,)),
            pltpu.SemaphoreType.DMA((2,)),
            pltpu.SemaphoreType.DMA((n_ch,)),
            pltpu.SemaphoreType.DMA((n_uch,)),
        ],
        compiler_params=pltpu.CompilerParams(collective_id=cid, has_side_effects=True, vmem_limit_bytes=40 * 1024 * 1024),
        name=f"attend_{n_up}",
    )(pos, qd, vn, k_t, v_t)


Q = 10
HOP = 3
WO_SLOTS = 4
GU_SLOTS = 4
WD_SLOTS = 3


def tail_kernel(attn_ref, tok_hbm, ln_ref, wo_hbm, wg_hbm, wu_hbm, wd_hbm, out_ref,
                x_ref, tok_ref, part, r1, r2, r3, full, xres, acc_g, acc_u, mact, wo, wg, wu, wd,
                tok_s, wo_s, wg_s, wu_s, wd_s, snd, rcv):
    heads = lax.axis_index("heads")
    core, cx, cy = lax.rem(heads, 2), heads // 2, lax.axis_index("dim")
    sib = {"heads": 2 * cx + 1 - core}
    xn = {"heads": 2 * (1 - cx) + core}
    yn = {"dim": 1 - cy}
    width = part.shape[3]
    rows = 16 * 8
    f32 = jnp.float32

    def cols(q):
        return pl.ds(pl.multiple_of(q * width, width), width)

    def wo_copy(q):
        s = lax.rem(q, WO_SLOTS)
        return [pltpu.make_async_copy(wo_hbm.at[:, cols(q)], wo.at[s], wo_s.at[s])]

    def gu_copy(q):
        s = lax.rem(q, GU_SLOTS)
        return [pltpu.make_async_copy(wg_hbm.at[cols(q)], wg.at[s], wg_s.at[s]),
                pltpu.make_async_copy(wu_hbm.at[cols(q)], wu.at[s], wu_s.at[s])]

    def wd_copy(q):
        s = lax.rem(q, WD_SLOTS)
        return [pltpu.make_async_copy(wd_hbm.at[:, cols(q)], wd.at[s], wd_s.at[s])]

    def start(copies):
        for cp in copies:
            cp.start()

    def wait(copies):
        for cp in copies:
            cp.wait()

    def remote(ph, st, q, src, dst, dev):
        return pltpu.make_async_remote_copy(src_ref=src, dst_ref=dst, send_sem=snd.at[ph, st], recv_sem=rcv.at[ph, st, q],
                                            device_id=dev, device_id_type=MESH)

    def stage(ph, k, q, sem_q):
        if k == 0:
            return [remote(ph, 0, sem_q, part.at[q, pl.ds(8 * (1 - core), 8)], r1.at[q], sib)]
        if k == 1:
            return [remote(ph, 1, sem_q, r1.at[q, pl.ds(2 * (1 - cx), 2)], r2.at[q, pl.ds(0, 2)], xn),
                    remote(ph, 2, sem_q, r1.at[q, pl.ds(4 + 2 * (1 - cy), 2)], r2.at[q, pl.ds(2, 2)], yn)]
        if k == 2:
            return [remote(ph, 3, sem_q, r2.at[q, pl.ds(1 - cy, 1)], r3.at[q, pl.ds(0, 1)], yn),
                    remote(ph, 4, sem_q, r2.at[q, pl.ds(2 + 1 - cx, 1)], r3.at[q, pl.ds(1, 1)], xn)]
        blk_a, blk_b = core * 8, core * 8 + 4
        if k == 3:
            a, b = full.at[q, pl.ds(blk_a + 2 * cx + cy, 1)], full.at[q, pl.ds(blk_b + 2 * cy + cx, 1)]
            return [remote(ph, 5, sem_q, a, a, yn), remote(ph, 6, sem_q, b, b, xn)]
        if k == 4:
            a, b = full.at[q, pl.ds(blk_a + 2 * cx, 2)], full.at[q, pl.ds(blk_b + 2 * cy, 2)]
            return [remote(ph, 7, sem_q, a, a, xn), remote(ph, 8, sem_q, b, b, yn)]
        a = full.at[q, pl.ds(blk_a, 8)]
        return [remote(ph, 9, sem_q, a, a, sib)]

    def one(ph, k, q):
        return stage(ph, k, q, q)

    def drain(ph, ks):
        for k in ks:
            for cp in stage(ph, k, slice(None), 0):
                cp.wait_send()

    def arrived(ph, k, q):
        for cp in one(ph, k, q):
            cp.wait_recv()

    def when(t, lo):
        return pl.when((t >= lo) & (t < lo + Q))

    def reduce_steps(ph, t, finish):
        @when(t, 2)
        def _():
            u = t - 2
            arrived(ph, 0, u)
            r1[u] = r1[u] + part[u, pl.ds(8 * core, 8)]
            start(one(ph, 1, u))

        @when(t, 0)
        def _():
            start(one(ph, 0, t))

        @when(t, 2 + HOP)
        def _():
            u = t - 2 - HOP
            arrived(ph, 1, u)
            r2[u, pl.ds(0, 2)] = r2[u, pl.ds(0, 2)] + r1[u, pl.ds(2 * cx, 2)]
            r2[u, pl.ds(2, 2)] = r2[u, pl.ds(2, 2)] + r1[u, pl.ds(4 + 2 * cy, 2)]
            start(one(ph, 2, u))

        @when(t, 2 + 2 * HOP)
        def _():
            u = t - 2 - 2 * HOP
            arrived(ph, 2, u)
            finish(u, r3[u, 0] + r2[u, cy], r3[u, 1] + r2[u, 2 + cx])

    def gather_start(ph, t):
        @when(t, 0)
        def _():
            start(one(ph, 3, t))

    def gather_steps(ph, t, finish):
        @when(t, HOP)
        def _():
            arrived(ph, 3, t - HOP)
            start(one(ph, 4, t - HOP))

        @when(t, 2 * HOP)
        def _():
            arrived(ph, 4, t - 2 * HOP)
            start(one(ph, 5, t - 2 * HOP))

        @when(t, 2 * HOP + 2)
        def _():
            arrived(ph, 5, t - 2 * HOP - 2)
            finish(t - 2 * HOP - 2)

    blk_a, blk_b = core * 8 + 2 * cx + cy, core * 8 + 4 + 2 * cy + cx
    tok_loads = [pltpu.make_async_copy(tok_hbm.at[blk], tok_ref.at[i], tok_s.at[i]) for i, blk in enumerate((blk_a, blk_b))]
    for q in range(WO_SLOTS):
        start(wo_copy(q))
    start(tok_loads)
    barrier = pltpu.get_barrier_semaphore()
    for dev in (sib, xn, yn):
        pl.semaphore_signal(barrier, inc=1, device_id=dev, device_id_type=MESH)
    acc_g[...] = jnp.zeros_like(acc_g)
    acc_u[...] = jnp.zeros_like(acc_u)
    for i in range(attn_ref.shape[1]):
        x_ref[:, i * BLK:(i + 1) * BLK] = attn_ref[:, i, :].astype(jnp.bfloat16)
    wait(tok_loads)
    pl.semaphore_wait(barrier, 3)
    def finish_attn(u, a, b):
        xres[u, 0] = (tok_ref[0, :, cols(u)].astype(f32) + a).astype(jnp.bfloat16).astype(f32)
        xres[u, 1] = (tok_ref[1, :, cols(u)].astype(f32) + b).astype(jnp.bfloat16).astype(f32)

    @pl.loop(0, Q + 2 + 2 * HOP)
    def _(t):
        @when(t, 0)
        def _():
            wait(wo_copy(t))
            part[t] = jnp.dot(x_ref[...], wo[lax.rem(t, WO_SLOTS)], preferred_element_type=f32).reshape(16, 8, width)

            @pl.when(t + WO_SLOTS < Q)
            def _():
                start(wo_copy(t + WO_SLOTS))

            @pl.when(t < GU_SLOTS)
            def _():
                start(gu_copy(t))

            @pl.when((t >= GU_SLOTS) & (t < GU_SLOTS + WD_SLOTS))
            def _():
                start(wd_copy(t - GU_SLOTS))
        reduce_steps(0, t, finish_attn)

    drain(0, (0, 1, 2))
    sq = jnp.zeros((2, 8, 1), f32)
    for q in range(Q):
        sq = sq + jnp.sum(xres[q] * xres[q], axis=-1, keepdims=True)
    inv = lax.rsqrt(sq / (Q * width) + EPS)
    for q in range(Q):
        h = (xres[q] * inv * ln_ref[q]).astype(jnp.bfloat16).astype(f32)
        full[q, blk_a] = h[0]
        full[q, blk_b] = h[1]

    def finish_gather(u):
        wait(gu_copy(u))
        s = lax.rem(u, GU_SLOTS)
        h = full[u].reshape(rows, width).astype(jnp.bfloat16)
        acc_g[...] += jnp.dot(h, wg[s], preferred_element_type=f32)
        acc_u[...] += jnp.dot(h, wu[s], preferred_element_type=f32)

        @pl.when(u + GU_SLOTS < Q)
        def _():
            start(gu_copy(u + GU_SLOTS))

    @pl.loop(0, Q + 2 + 2 * HOP)
    def _(t):
        gather_start(0, t)
        gather_steps(0, t, finish_gather)

    drain(0, (3, 4, 5))

    @pl.loop(0, acc_g.shape[1] // 640)
    def _(n):
        c = pl.ds(pl.multiple_of(n * 640, 640), 640)
        mact[:, c] = (jax.nn.silu(acc_g[:, c]) * acc_u[:, c]).astype(jnp.bfloat16)

    def finish_mlp(u, a, b):
        full[u, blk_a] = (xres[u, 0] + a).astype(jnp.bfloat16).astype(f32)
        full[u, blk_b] = (xres[u, 1] + b).astype(jnp.bfloat16).astype(f32)

    def finish_out(u):
        out_ref[:, cols(u)] = full[u].reshape(rows, width).astype(jnp.bfloat16)

    lag = 3 + 2 * HOP

    @pl.loop(0, Q + lag + 2 + 2 * HOP)
    def _(t):
        gather_start(1, t - lag)

        @when(t, 0)
        def _():
            wait(wd_copy(t))
            part[t] = jnp.dot(mact[...], wd[lax.rem(t, WD_SLOTS)], preferred_element_type=f32).reshape(16, 8, width)

            @pl.when(t + WD_SLOTS < Q)
            def _():
                start(wd_copy(t + WD_SLOTS))
        reduce_steps(1, t, finish_mlp)
        gather_steps(1, t - lag, finish_out)

    drain(1, (0, 1, 2, 3, 4, 5))


def tail(cid, attn, tok_blocks, ln, w_out, w_gate, w_up, w_down):
    rows = attn.shape[0]
    depth = w_out.shape[0]
    d_model, inner = w_gate.shape
    width = d_model // Q
    vmem = pl.BlockSpec(memory_space=pltpu.VMEM)
    hbm = pl.BlockSpec(memory_space=pl.ANY)
    f32, bf16 = jnp.float32, jnp.bfloat16
    dma = pltpu.SemaphoreType.DMA
    return pl.pallas_call(
        tail_kernel,
        out_shape=jax.ShapeDtypeStruct((rows, d_model), bf16),
        in_specs=[vmem, hbm, vmem, hbm, hbm, hbm, hbm],
        out_specs=vmem,
        scratch_shapes=[
            pltpu.VMEM((rows, depth), bf16),
            pltpu.VMEM((2, 8, d_model), bf16),
            pltpu.VMEM((Q, 16, 8, width), f32),
            pltpu.VMEM((Q, 8, 8, width), f32),
            pltpu.VMEM((Q, 4, 8, width), f32),
            pltpu.VMEM((Q, 2, 8, width), f32),
            pltpu.VMEM((Q, 16, 8, width), f32),
            pltpu.VMEM((Q, 2, 8, width), f32),
            pltpu.VMEM((rows, inner), f32),
            pltpu.VMEM((rows, inner), f32),
            pltpu.VMEM((rows, inner), bf16),
            pltpu.VMEM((WO_SLOTS, depth, width), bf16),
            pltpu.VMEM((GU_SLOTS, width, inner), bf16),
            pltpu.VMEM((GU_SLOTS, width, inner), bf16),
            pltpu.VMEM((WD_SLOTS, inner, width), bf16),
            dma((2,)), dma((WO_SLOTS,)), dma((GU_SLOTS,)), dma((GU_SLOTS,)), dma((WD_SLOTS,)),
            dma((2, 10)), dma((2, 10, Q)),
        ],
        compiler_params=pltpu.CompilerParams(collective_id=cid, has_side_effects=True, vmem_limit_bytes=55 * 1024 * 1024),
        name="tail",
    )(attn, tok_blocks, ln, w_out, w_gate, w_up, w_down)


def solution(mesh):
    dim_count = mesh.shape['dim']
    mlp_axes = ('heads', 'dim')

    def layer_body(tokens, ln_attn, w_query, w_key, w_value, q_gain, k_gain, w_out, ln_mlp, w_gate, w_up, w_down, k_cache, v_cache, positions):
        rows = tokens.shape[0]
        heads_local = w_query.shape[1]
        kv_local = w_key.shape[1]
        slice_len = w_query.shape[2]
        head_dim = slice_len * dim_count
        half_dim = head_dim // 2
        q_group = heads_local // kv_local
        cache_len = k_cache.shape[1]
        dim_index = lax.axis_index('dim')

        inv_freq = np.tile(ROPE_BASE ** (-np.arange(half_dim) * 2.0 / head_dim), 2).astype(np.float32)

        def by_column(w):
            return w.transpose(1, 2, 0).reshape(-1, w.shape[0])

        qd, vn, kt, vt = qkv(len(UP_SIZES) + 1, q_group, tokens, ln_attn[None], positions[None], inv_freq[None], q_gain[None], k_gain[None],
                             by_column(w_query), by_column(w_key), by_column(w_value))
        k_new = kt.reshape(kv_local, slice_len, rows).transpose(2, 0, 1)
        v_new = vt.reshape(kv_local, slice_len, rows).transpose(2, 0, 1)

        n_units = jnp.maximum((positions - LOW + UNIT - 1) // UNIT, 1)
        per_blk = BLK // UNIT
        k_t = k_cache.transpose(0, 2, 3, 1).reshape(rows, kv_local * slice_len, cache_len)
        v_t = v_cache.transpose(0, 2, 3, 1).reshape(rows, kv_local * slice_len, cache_len)
        spare = (UP_FIRST - UCH) * per_blk // rows
        assert spare * rows == (UP_FIRST - UCH) * per_blk
        which = lax.shift_right_arithmetic(jnp.sum(n_units - spare), (UCH * per_blk).bit_length() - 1)
        branches = [functools.partial(attend, n, i, head_dim ** -0.5) for i, n in enumerate(UP_SIZES)]
        attn = lax.switch(which, branches, positions, qd, vn, k_t, v_t)
        out = tail(len(UP_SIZES), attn, tokens.reshape(16, 8, -1), ln_mlp.reshape(Q, 1, -1), w_out.reshape(heads_local * slice_len, -1), w_gate, w_up, w_down)
        return out, k_new, v_new

    row_spec = P('dp', None)
    head_spec = P(None, 'heads', 'dim')
    cache_spec = P('dp', None, 'heads', 'dim')
    new_spec = P('dp', 'heads', 'dim')
    in_specs = (row_spec, P(None), head_spec, head_spec, head_spec, P('dim'), P('dim'), P('heads', 'dim', None), P(None), P(None, mlp_axes), P(None, mlp_axes), P(mlp_axes, None), cache_spec, cache_spec, P('dp'))
    out_specs = (row_spec, new_spec, new_spec)
    return jax.shard_map(layer_body, mesh=mesh, in_specs=in_specs, out_specs=out_specs, check_vma=False)
```

```python
import functools

import jax
import jax.numpy as jnp
import numpy as np
from jax import lax
from jax.experimental import pallas as pl
from jax.experimental.pallas import tpu as pltpu
from jax.sharding import PartitionSpec as P

EPS = 1e-6
ROPE_BASE = 1000000.0
MESH = pl.DeviceIdType.MESH

BLK = 128
LOW = 512
CH = 4
UCH = 8
UNIT = 16
SLOTS = 4
FIRST = 8
LEAD = 4
UP_FIRST = 232
UP_SIZES = tuple(UP_FIRST + UCH * i for i in range(9)) + (512,)


def qkv_kernel(group, tok_ref, ln_ref, pos_ref, freq_ref, qg_ref, kg_ref, wq_hbm, wk_hbm, wv_hbm, qd_ref, vn_ref, kt_ref, vt_ref,
               hid, wq, wk, wv, own, other, gain_ref, gain_other, wsem, snd, rcv):
    partner = {"dim": 1 - lax.axis_index("dim")}
    rows, depth = tok_ref.shape
    n_q = own.shape[0] - 1
    steps = n_q // 2
    f32, bf16 = jnp.float32, jnp.bfloat16
    half = BLK // 2
    per_step = wq.shape[0] // steps

    def wq_copy(c):
        part = pl.ds(pl.multiple_of(c * per_step, per_step), per_step)
        return pltpu.make_async_copy(wq_hbm.at[part], wq.at[part], wsem.at[c])

    k_load = pltpu.make_async_copy(wk_hbm, wk, wsem.at[steps])
    v_load = pltpu.make_async_copy(wv_hbm, wv, wsem.at[steps + 1])

    def remote(src, dst, i):
        return pltpu.make_async_remote_copy(src_ref=src, dst_ref=dst, send_sem=snd.at[i], recv_sem=rcv.at[i],
                                            device_id=partner, device_id_type=MESH)

    def q_copy(c):
        part = pl.ds(2 * c, 2)
        return remote(own.at[part], other.at[part], c)

    k_copy = remote(own.at[pl.ds(n_q, 1)], other.at[pl.ds(n_q, 1)], steps)
    g_copy = remote(gain_ref, gain_other, steps + 1)

    k_load.start()
    for c in range(steps):
        wq_copy(c).start()
    v_load.start()
    barrier = pltpu.get_barrier_semaphore()
    pl.semaphore_signal(barrier, inc=1, device_id=partner, device_id_type=MESH)
    gain_ref[...] = jnp.zeros_like(gain_ref)
    for row, ref in enumerate((qg_ref, kg_ref)):
        gain_ref[row:row + 1, :half] = ref[...]
        gain_ref[row:row + 1, half:] = ref[...]
    pl.semaphore_wait(barrier, 1)

    @pl.loop(0, rows // 16, unroll=4)
    def _(i):
        part = pl.ds(pl.multiple_of(i * 16, 16), 16)
        x = tok_ref[part, :].astype(f32)
        inv = lax.rsqrt(jnp.mean(x * x, axis=-1, keepdims=True) + EPS)
        hid[part, :] = (x * inv * ln_ref[...]).astype(bf16)

    def project(w):
        return lax.dot_general(hid[...], w, (((1,), (1,)), ((), ())), preferred_element_type=f32)

    g_copy.start()
    k_load.wait()
    own[n_q] = project(wk[...])
    k_copy.start()

    @pl.loop(0, steps)
    def _(c):
        wq_copy(c).wait()
        u = project(wq[pl.ds(pl.multiple_of(c * per_step, per_step), per_step), :])

        own[2 * c] = u[:, :BLK]
        own[2 * c + 1] = u[:, BLK:]
        q_copy(c).start()

    v_load.wait()
    v_row = project(wv[...]).astype(bf16).astype(f32)
    vn_ref[...] = v_row
    vt_ref[...] = v_row.T.astype(bf16)
    low = lax.broadcasted_iota(jnp.int32, (rows, BLK), 1) < half
    angle = jnp.broadcast_to(pos_ref[...].astype(f32), (rows, rows)).T * freq_ref[...]
    cos_t = jnp.cos(angle)
    sin_t = jnp.sin(angle) * jnp.where(lax.axis_index("dim") == 0, -1.0, 1.0)

    def halves(x):
        return (jnp.sum(jnp.where(low, x, 0.0), axis=-1, keepdims=True), jnp.sum(jnp.where(low, 0.0, x), axis=-1, keepdims=True))

    def rotate(i, g):
        a, b = own[i], other[i]
        s_lo, s_hi = halves(a * a + b * b)
        inv = jnp.where(low, lax.rsqrt(s_lo / BLK + EPS), lax.rsqrt(s_hi / BLK + EPS))
        a, b = a * inv * gain_ref[g:g + 1, :], b * inv * gain_other[g:g + 1, :]
        return (a * cos_t + b * sin_t).astype(bf16).astype(f32), (b * cos_t - a * sin_t).astype(bf16).astype(f32)

    g_copy.wait_recv()
    k_copy.wait_recv()
    k_own, k_oth = rotate(n_q, 1)
    kt_ref[...] = k_own.T.astype(bf16)
    kr_own, kr_oth = pltpu.roll(k_own, half, 1), pltpu.roll(k_oth, half, 1)
    kk = [(jnp.where(low, k_own, kr_own), jnp.where(low, k_oth, kr_oth)),
          (jnp.where(low, kr_own, k_own), jnp.where(low, kr_oth, k_oth))]
    for i in range(n_q):
        if i % 2 == 0:
            q_copy(i // 2).wait_recv()
        q_own, q_oth = rotate(i, 0)
        kv = 2 * i // group
        new = halves(q_own * kk[kv][0] + q_oth * kk[kv][1])
        turned = pltpu.roll(q_own, half, 1)
        for e in range(2):
            row = i + n_q * e
            val = q_own if e == kv else turned
            qd_ref[:, row, :] = jnp.where(low, val, new[e]) if kv == 0 else jnp.where(low, new[e], val)
    for c in range(steps):
        q_copy(c).wait_send()
    k_copy.wait_send()
    g_copy.wait_send()


def qkv(cid, group, tokens, ln, pos, freq, q_gain, k_gain, w_q, w_k, w_v):
    rows, depth = tokens.shape
    n_q = w_q.shape[0] // BLK
    steps = n_q // 2
    vmem = pl.BlockSpec(memory_space=pltpu.VMEM)
    hbm = pl.BlockSpec(memory_space=pl.ANY)
    f32, bf16 = jnp.float32, jnp.bfloat16
    heads = 2 * n_q
    dma = pltpu.SemaphoreType.DMA
    return pl.pallas_call(
        functools.partial(qkv_kernel, group),
        out_shape=(jax.ShapeDtypeStruct((rows, heads, BLK), f32), jax.ShapeDtypeStruct((rows, BLK), f32), jax.ShapeDtypeStruct((BLK, rows), bf16), jax.ShapeDtypeStruct((BLK, rows), bf16)),
        in_specs=[vmem] * 6 + [hbm] * 3,
        out_specs=(vmem,) * 4,
        scratch_shapes=[
            pltpu.VMEM((rows, depth), bf16),
            pltpu.VMEM(w_q.shape, bf16),
            pltpu.VMEM(w_k.shape, bf16),
            pltpu.VMEM(w_v.shape, bf16),
            pltpu.VMEM((n_q + 1, rows, BLK), f32),
            pltpu.VMEM((n_q + 1, rows, BLK), f32),
            pltpu.VMEM((8, BLK), f32),
            pltpu.VMEM((8, BLK), f32),
            dma((steps + 2,)), dma((steps + 2,)), dma((steps + 2,)),
        ],
        compiler_params=pltpu.CompilerParams(collective_id=cid, has_side_effects=True, vmem_limit_bytes=62 * 1024 * 1024),
        name="qkv",
    )(tokens, ln, pos, freq, q_gain, k_gain, w_q, w_k, w_v)


def attn_kernel(n_up, scale, pos_ref, qd_ref, vn_ref, k_hbm, v_hbm, o_ref,
                off_ref, kbuf, vbuf, own_lo, own_up, pack, rlo, rup, ksem, vsem, send, slo_r, sup_r):
    partner = {"dim": 1 - lax.axis_index("dim")}
    rows = qd_ref.shape[0]
    n_ch = rows // CH
    n_uch = n_up // UCH
    up_blocks = own_up.shape[0] // rows
    per_blk = BLK // UNIT
    lane_up = lax.broadcasted_iota(jnp.int32, (16, BLK), 1)
    kv_row = lax.broadcasted_iota(jnp.int32, (16, BLK), 0) // 4 % 2
    q_lanes = kv_row == lane_up // 64

    def kcopy(c):
        return pltpu.make_async_copy(k_hbm.at[pl.ds(c * CH, CH)], kbuf.at[lax.rem(c, SLOTS)], ksem.at[lax.rem(c, SLOTS)])

    def vcopy(c):
        return pltpu.make_async_copy(v_hbm.at[pl.ds(c * CH, CH)], vbuf.at[lax.rem(c, SLOTS)], vsem.at[lax.rem(c, SLOTS)])

    def lo_copy(c):
        part = pl.ds(c * CH, CH)
        return pltpu.make_async_remote_copy(src_ref=own_lo.at[part], dst_ref=rlo.at[part], send_sem=send.at[0],
                                            recv_sem=slo_r.at[c], device_id=partner, device_id_type=MESH)

    def up_copy(c):
        part = pl.ds(c * UCH, UCH)
        return pltpu.make_async_remote_copy(src_ref=pack.at[part], dst_ref=rup.at[part], send_sem=send.at[1],
                                            recv_sem=sup_r.at[c], device_id=partner, device_id_type=MESH)

    kcopy(0).start()
    barrier = pltpu.get_barrier_semaphore()
    pl.semaphore_signal(barrier, inc=1, device_id=partner, device_id_type=MESH)
    pl.semaphore_wait(barrier, 1)
    for c in range(1, SLOTS):
        kcopy(c).start()
    row_units = up_blocks * per_blk

    @pl.loop(0, n_ch)
    def _(c):
        @pl.when((c >= 1) & (c <= FIRST))
        def _():
            lo_copy(c - 1).start()

        kcopy(c).wait()
        for r in range(CH):
            b = c * CH + r
            s = jnp.dot(jnp.where(q_lanes, qd_ref[b], 0.0).astype(jnp.bfloat16), kbuf[lax.rem(c, SLOTS), r], preferred_element_type=jnp.float32)
            own_lo[b] = s[:, :LOW]
            for j in range(up_blocks):
                own_up[b * up_blocks + j] = s[:, LOW + j * BLK:LOW + (j + 1) * BLK]

        @pl.when(c + SLOTS < n_ch)
        def _():
            kcopy(c + SLOTS).start()

    for c in range(SLOTS):
        vcopy(c).start()

    def place(b, total):
        off_ref[b] = total
        return total + jnp.maximum((pos_ref[b] - LOW + UNIT - 1) // UNIT, 1)

    lax.fori_loop(0, rows, place, jnp.int32(0))

    def fill(c, row):
        for r in range(UCH):
            j = c * UCH + r
            block = None
            for k in range(per_blk):
                unit = j * per_blk + k
                following = jnp.minimum(row + 1, rows - 1)
                row = jnp.where(unit >= off_ref[following], following, row)
                src = jnp.minimum(unit - off_ref[row], row_units - 1)
                piece = pltpu.roll(own_up[row * up_blocks + src // per_blk], (k + per_blk - src % per_blk) % per_blk * UNIT, 1)
                block = piece if k == 0 else jnp.where(lane_up >= k * UNIT, piece, block)
            pack[j] = block

        @pl.when(c >= 1)
        def _():
            up_copy(c - 1).start()
        return row

    lax.fori_loop(0, n_uch, fill, jnp.int32(0))
    up_copy(n_uch - 1).start()

    @pl.loop(FIRST, FIRST + LEAD)
    def _(c):
        lo_copy(c).start()

    @pl.loop(0, n_uch)
    def _(c):
        up_copy(c).wait_recv()

    lane = lax.broadcasted_iota(jnp.int32, (8, 2 * 64), 1)
    first = lax.broadcasted_iota(jnp.int32, (8, 2 * 64), 0) < 4
    t_up = lane_up + LOW

    @pl.loop(0, n_ch)
    def _(c):
        @pl.when(c + FIRST + LEAD < n_ch)
        def _():
            lo_copy(c + FIRST + LEAD).start()

        vcopy(c).wait()
        lo_copy(c).wait_recv()
        for r in range(CH):
            b = c * CH + r
            pos = pos_ref[b]
            off = off_ref[b]
            parts = [(own_lo[b] + rlo[b]) * scale]
            skew = off % per_blk * UNIT
            slots = [pltpu.roll(rup[jnp.minimum(off // per_blk + j, n_up - 1)], (BLK - skew) % BLK, 1) for j in range(up_blocks + 1)]
            for j in range(up_blocks):
                got = jnp.where(lane_up < BLK - skew, slots[j], slots[j + 1])
                total = (own_up[b * up_blocks + j] + got) * scale
                parts.append(jnp.where(t_up + j * BLK < pos, total, -jnp.inf))
            s = jnp.concatenate(parts, axis=1)
            q_row = qd_ref[b]
            s_new = jnp.where(kv_row[:, 0:1] == 0, q_row[:, BLK - 1:], q_row[:, 0:1]) * scale
            m = jnp.maximum(jnp.max(s, axis=1, keepdims=True), s_new)
            e = jnp.exp(s - m)
            e_new = jnp.exp(s_new - m)
            inv = 1.0 / (jnp.sum(e, axis=1, keepdims=True) + e_new)
            p = (e * inv).astype(jnp.bfloat16)
            p_new = (e_new * inv).astype(jnp.bfloat16).astype(jnp.float32)
            o = lax.dot_general(p, vbuf[lax.rem(c, SLOTS), r], (((1,), (1,)), ((), ())), preferred_element_type=jnp.float32)
            o = o + p_new * vn_ref[pl.ds(b, 1), :]
            even, odd = o[0:8], o[8:16]
            o_ref[b] = jnp.where(lane < 64, jnp.where(first, even, pltpu.roll(even, 64, 1)), jnp.where(first, pltpu.roll(odd, 64, 1), odd))

        @pl.when(c + SLOTS < n_ch)
        def _():
            vcopy(c + SLOTS).start()

    pltpu.make_async_remote_copy(src_ref=own_lo, dst_ref=rlo, send_sem=send.at[0], recv_sem=slo_r.at[0],
                                 device_id=partner, device_id_type=MESH).wait_send()
    pltpu.make_async_remote_copy(src_ref=pack, dst_ref=rup, send_sem=send.at[1], recv_sem=sup_r.at[0],
                                 device_id=partner, device_id_type=MESH).wait_send()


def attend(n_up, cid, scale, pos, qd, vn, k_t, v_t):
    rows = qd.shape[0]
    n_ch = rows // CH
    n_uch = n_up // UCH
    cache_len = k_t.shape[2]
    up_blocks = (cache_len - LOW) // BLK
    smem = pl.BlockSpec(memory_space=pltpu.SMEM)
    vmem = pl.BlockSpec(memory_space=pltpu.VMEM)
    hbm = pl.BlockSpec(memory_space=pl.ANY)
    return pl.pallas_call(
        functools.partial(attn_kernel, n_up, scale),
        out_shape=jax.ShapeDtypeStruct((rows, 8, 128), jnp.float32),
        in_specs=[smem, vmem, vmem, hbm, hbm],
        out_specs=vmem,
        scratch_shapes=[
            pltpu.SMEM((rows,), jnp.int32),
            pltpu.VMEM((SLOTS, CH, 128, cache_len), jnp.bfloat16),
            pltpu.VMEM((SLOTS, CH, 128, cache_len), jnp.bfloat16),
            pltpu.VMEM((rows, 16, LOW), jnp.float32),
            pltpu.VMEM((rows * up_blocks, 16, BLK), jnp.float32),
            pltpu.VMEM((n_up, 16, BLK), jnp.float32),
            pltpu.VMEM((rows, 16, LOW), jnp.float32),
            pltpu.VMEM((n_up, 16, BLK), jnp.float32),
            pltpu.SemaphoreType.DMA((SLOTS,)),
            pltpu.SemaphoreType.DMA((SLOTS,)),
            pltpu.SemaphoreType.DMA((2,)),
            pltpu.SemaphoreType.DMA((n_ch,)),
            pltpu.SemaphoreType.DMA((n_uch,)),
        ],
        compiler_params=pltpu.CompilerParams(collective_id=cid, has_side_effects=True, vmem_limit_bytes=40 * 1024 * 1024),
        name=f"attend_{n_up}",
    )(pos, qd, vn, k_t, v_t)


Q = 10
REDUCE_LAGS = ((3, 6, 6), (2, 5, 6))
GATHER_LAGS = ((4, 3, 2), (6, 4, 2))
WO_SLOTS = 3
GU_SLOTS = 5
WD_SLOTS = 4


def tail_kernel(attn_ref, tok_hbm, ln_ref, wo_hbm, wg_hbm, wu_hbm, wd_hbm, out_ref,
                x_ref, tok_ref, part, r1, r2, r3, full, xres, acc_g, acc_u, mact, wo, wg, wu, wd,
                tok_s, wo_s, wg_s, wu_s, wd_s, snd, rcv):
    heads = lax.axis_index("heads")
    core, cx, cy = lax.rem(heads, 2), heads // 2, lax.axis_index("dim")
    sib = {"heads": 2 * cx + 1 - core}
    xn = {"heads": 2 * (1 - cx) + core}
    yn = {"dim": 1 - cy}
    width = part.shape[3]
    rows = 16 * 8
    f32 = jnp.float32

    def cols(q):
        return pl.ds(pl.multiple_of(q * width, width), width)

    def wo_copy(q):
        s = lax.rem(q, WO_SLOTS)
        return [pltpu.make_async_copy(wo_hbm.at[:, cols(q)], wo.at[s], wo_s.at[s])]

    def gu_copy(q):
        s = lax.rem(q, GU_SLOTS)
        return [pltpu.make_async_copy(wg_hbm.at[cols(q)], wg.at[s], wg_s.at[s]),
                pltpu.make_async_copy(wu_hbm.at[cols(q)], wu.at[s], wu_s.at[s])]

    def wd_copy(q):
        s = lax.rem(q, WD_SLOTS)
        return [pltpu.make_async_copy(wd_hbm.at[:, cols(q)], wd.at[s], wd_s.at[s])]

    def start(copies):
        for cp in copies:
            cp.start()

    def wait(copies):
        for cp in copies:
            cp.wait()

    def remote(ph, st, q, src, dst, dev):
        return pltpu.make_async_remote_copy(src_ref=src, dst_ref=dst, send_sem=snd.at[ph, st], recv_sem=rcv.at[ph, st, q],
                                            device_id=dev, device_id_type=MESH)

    def stage(ph, k, q, sem_q):
        if k == 0:
            return [remote(ph, 0, sem_q, part.at[q, pl.ds(8 * (1 - core), 8)], r1.at[q], sib)]
        if k == 1:
            return [remote(ph, 1, sem_q, r1.at[q, pl.ds(2 * (1 - cx), 2)], r2.at[q, pl.ds(0, 2)], xn),
                    remote(ph, 2, sem_q, r1.at[q, pl.ds(4 + 2 * (1 - cy), 2)], r2.at[q, pl.ds(2, 2)], yn)]
        if k == 2:
            return [remote(ph, 3, sem_q, r2.at[q, pl.ds(1 - cy, 1)], r3.at[q, pl.ds(0, 1)], yn),
                    remote(ph, 4, sem_q, r2.at[q, pl.ds(2 + 1 - cx, 1)], r3.at[q, pl.ds(1, 1)], xn)]
        blk_a, blk_b = core * 8, core * 8 + 4
        if k == 3:
            a, b = full.at[q, pl.ds(blk_a + 2 * cx + cy, 1)], full.at[q, pl.ds(blk_b + 2 * cy + cx, 1)]
            return [remote(ph, 5, sem_q, a, a, yn), remote(ph, 6, sem_q, b, b, xn)]
        if k == 4:
            a, b = full.at[q, pl.ds(blk_a + 2 * cx, 2)], full.at[q, pl.ds(blk_b + 2 * cy, 2)]
            return [remote(ph, 7, sem_q, a, a, xn), remote(ph, 8, sem_q, b, b, yn)]
        a = full.at[q, pl.ds(blk_a, 8)]
        return [remote(ph, 9, sem_q, a, a, sib)]

    def one(ph, k, q):
        return stage(ph, k, q, q)

    def drain(ph, ks):
        for k in ks:
            for cp in stage(ph, k, slice(None), 0):
                cp.wait_send()

    def arrived(ph, k, q):
        for cp in one(ph, k, q):
            cp.wait_recv()

    def when(t, lo):
        return pl.when((t >= lo) & (t < lo + Q))

    def reduce_steps(ph, t, finish):
        first, second, third = np.cumsum(REDUCE_LAGS[ph]).tolist()

        @when(t, first)
        def _():
            u = t - first
            arrived(ph, 0, u)
            r1[u] = r1[u] + part[u, pl.ds(8 * core, 8)]
            start(one(ph, 1, u))

        @when(t, 0)
        def _():
            start(one(ph, 0, t))

        @when(t, second)
        def _():
            u = t - second
            arrived(ph, 1, u)
            r2[u, pl.ds(0, 2)] = r2[u, pl.ds(0, 2)] + r1[u, pl.ds(2 * cx, 2)]
            r2[u, pl.ds(2, 2)] = r2[u, pl.ds(2, 2)] + r1[u, pl.ds(4 + 2 * cy, 2)]
            start(one(ph, 2, u))

        @when(t, third)
        def _():
            u = t - third
            arrived(ph, 2, u)
            finish(u, r3[u, 0] + r2[u, cy], r3[u, 1] + r2[u, 2 + cx])

    def gather_start(ph, t):
        @when(t, 0)
        def _():
            start(one(ph, 3, t))

    def gather_steps(ph, t, finish):
        first, second, third = np.cumsum(GATHER_LAGS[ph]).tolist()

        @when(t, first)
        def _():
            arrived(ph, 3, t - first)
            start(one(ph, 4, t - first))

        @when(t, second)
        def _():
            arrived(ph, 4, t - second)
            start(one(ph, 5, t - second))

        @when(t, third)
        def _():
            arrived(ph, 5, t - third)
            finish(t - third)

    blk_a, blk_b = core * 8 + 2 * cx + cy, core * 8 + 4 + 2 * cy + cx
    tok_loads = [pltpu.make_async_copy(tok_hbm.at[blk], tok_ref.at[i], tok_s.at[i]) for i, blk in enumerate((blk_a, blk_b))]
    for q in range(WO_SLOTS):
        start(wo_copy(q))
    start(tok_loads)
    barrier = pltpu.get_barrier_semaphore()
    for dev in (sib, xn, yn):
        pl.semaphore_signal(barrier, inc=1, device_id=dev, device_id_type=MESH)
    acc_g[...] = jnp.zeros_like(acc_g)
    acc_u[...] = jnp.zeros_like(acc_u)
    for i in range(attn_ref.shape[1]):
        x_ref[:, i * BLK:(i + 1) * BLK] = attn_ref[:, i, :].astype(jnp.bfloat16)
    wait(tok_loads)
    pl.semaphore_wait(barrier, 3)
    def finish_attn(u, a, b):
        xres[u, 0] = (tok_ref[0, :, cols(u)].astype(f32) + a).astype(jnp.bfloat16).astype(f32)
        xres[u, 1] = (tok_ref[1, :, cols(u)].astype(f32) + b).astype(jnp.bfloat16).astype(f32)

    @pl.loop(0, Q + sum(REDUCE_LAGS[0]))
    def _(t):
        @when(t, 0)
        def _():
            wait(wo_copy(t))
            part[t] = jnp.dot(x_ref[...], wo[lax.rem(t, WO_SLOTS)], preferred_element_type=f32).reshape(16, 8, width)

            @pl.when(t + WO_SLOTS < Q)
            def _():
                start(wo_copy(t + WO_SLOTS))

        @pl.when((t >= WO_SLOTS) & (t < WO_SLOTS + GU_SLOTS))
        def _():
            start(gu_copy(t - WO_SLOTS))

        @pl.when((t >= WO_SLOTS + GU_SLOTS) & (t < WO_SLOTS + GU_SLOTS + WD_SLOTS))
        def _():
            start(wd_copy(t - WO_SLOTS - GU_SLOTS))

        reduce_steps(0, t, finish_attn)

    drain(0, (0, 1, 2))
    sq = jnp.zeros((2, 8, 1), f32)
    for q in range(Q):
        sq = sq + jnp.sum(xres[q] * xres[q], axis=-1, keepdims=True)
    inv = lax.rsqrt(sq / (Q * width) + EPS)
    for q in range(Q):
        h = (xres[q] * inv * ln_ref[q]).astype(jnp.bfloat16).astype(f32)
        full[q, blk_a] = h[0]
        full[q, blk_b] = h[1]

    def finish_gather(u):
        wait(gu_copy(u))
        s = lax.rem(u, GU_SLOTS)
        h = full[u].reshape(rows, width).astype(jnp.bfloat16)
        acc_g[...] += jnp.dot(h, wg[s], preferred_element_type=f32)
        acc_u[...] += jnp.dot(h, wu[s], preferred_element_type=f32)

        @pl.when(u + GU_SLOTS < Q)
        def _():
            start(gu_copy(u + GU_SLOTS))

    @pl.loop(0, Q + sum(GATHER_LAGS[0]))
    def _(t):
        gather_start(0, t)
        gather_steps(0, t, finish_gather)

    drain(0, (3, 4, 5))

    @pl.loop(0, acc_g.shape[1] // 640)
    def _(n):
        c = pl.ds(pl.multiple_of(n * 640, 640), 640)
        mact[:, c] = (jax.nn.silu(acc_g[:, c]) * acc_u[:, c]).astype(jnp.bfloat16)

    def finish_mlp(u, a, b):
        full[u, blk_a] = (xres[u, 0] + a).astype(jnp.bfloat16).astype(f32)
        full[u, blk_b] = (xres[u, 1] + b).astype(jnp.bfloat16).astype(f32)

    def finish_out(u):
        out_ref[:, cols(u)] = full[u].reshape(rows, width).astype(jnp.bfloat16)

    lag = 1 + sum(REDUCE_LAGS[1])

    @pl.loop(0, Q + lag + sum(GATHER_LAGS[1]))
    def _(t):
        gather_start(1, t - lag)

        @when(t, 0)
        def _():
            wait(wd_copy(t))
            part[t] = jnp.dot(mact[...], wd[lax.rem(t, WD_SLOTS)], preferred_element_type=f32).reshape(16, 8, width)

            @pl.when(t + WD_SLOTS < Q)
            def _():
                start(wd_copy(t + WD_SLOTS))
        reduce_steps(1, t, finish_mlp)
        gather_steps(1, t - lag, finish_out)

    drain(1, (0, 1, 2, 3, 4, 5))


def tail(cid, attn, tok_blocks, ln, w_out, w_gate, w_up, w_down):
    rows = attn.shape[0]
    depth = w_out.shape[0]
    d_model, inner = w_gate.shape
    width = d_model // Q
    vmem = pl.BlockSpec(memory_space=pltpu.VMEM)
    hbm = pl.BlockSpec(memory_space=pl.ANY)
    f32, bf16 = jnp.float32, jnp.bfloat16
    dma = pltpu.SemaphoreType.DMA
    return pl.pallas_call(
        tail_kernel,
        out_shape=jax.ShapeDtypeStruct((rows, d_model), bf16),
        in_specs=[vmem, hbm, vmem, hbm, hbm, hbm, hbm],
        out_specs=vmem,
        scratch_shapes=[
            pltpu.VMEM((rows, depth), bf16),
            pltpu.VMEM((2, 8, d_model), bf16),
            pltpu.VMEM((Q, 16, 8, width), f32),
            pltpu.VMEM((Q, 8, 8, width), f32),
            pltpu.VMEM((Q, 4, 8, width), f32),
            pltpu.VMEM((Q, 2, 8, width), f32),
            pltpu.VMEM((Q, 16, 8, width), f32),
            pltpu.VMEM((Q, 2, 8, width), f32),
            pltpu.VMEM((rows, inner), f32),
            pltpu.VMEM((rows, inner), f32),
            pltpu.VMEM((rows, inner), bf16),
            pltpu.VMEM((WO_SLOTS, depth, width), bf16),
            pltpu.VMEM((GU_SLOTS, width, inner), bf16),
            pltpu.VMEM((GU_SLOTS, width, inner), bf16),
            pltpu.VMEM((WD_SLOTS, inner, width), bf16),
            dma((2,)), dma((WO_SLOTS,)), dma((GU_SLOTS,)), dma((GU_SLOTS,)), dma((WD_SLOTS,)),
            dma((2, 10)), dma((2, 10, Q)),
        ],
        compiler_params=pltpu.CompilerParams(collective_id=cid, has_side_effects=True, vmem_limit_bytes=62 * 1024 * 1024),
        name="tail",
    )(attn, tok_blocks, ln, w_out, w_gate, w_up, w_down)


def solution(mesh):
    dim_count = mesh.shape['dim']
    mlp_axes = ('heads', 'dim')

    def layer_body(tokens, ln_attn, w_query, w_key, w_value, q_gain, k_gain, w_out, ln_mlp, w_gate, w_up, w_down, k_cache, v_cache, positions):
        rows = tokens.shape[0]
        heads_local = w_query.shape[1]
        kv_local = w_key.shape[1]
        slice_len = w_query.shape[2]
        head_dim = slice_len * dim_count
        half_dim = head_dim // 2
        q_group = heads_local // kv_local
        cache_len = k_cache.shape[1]
        dim_index = lax.axis_index('dim')

        inv_freq = np.tile(ROPE_BASE ** (-np.arange(half_dim) * 2.0 / head_dim), 2).astype(np.float32)

        def by_column(w):
            return w.transpose(1, 2, 0).reshape(-1, w.shape[0])

        qd, vn, kt, vt = qkv(len(UP_SIZES) + 1, q_group, tokens, ln_attn[None], positions[None], inv_freq[None], q_gain[None], k_gain[None],
                             by_column(w_query), by_column(w_key), by_column(w_value))
        k_new = kt.reshape(kv_local, slice_len, rows).transpose(2, 0, 1)
        v_new = vt.reshape(kv_local, slice_len, rows).transpose(2, 0, 1)

        n_units = jnp.maximum((positions - LOW + UNIT - 1) // UNIT, 1)
        per_blk = BLK // UNIT
        k_t = k_cache.transpose(0, 2, 3, 1).reshape(rows, kv_local * slice_len, cache_len)
        v_t = v_cache.transpose(0, 2, 3, 1).reshape(rows, kv_local * slice_len, cache_len)
        spare = (UP_FIRST - UCH) * per_blk // rows
        assert spare * rows == (UP_FIRST - UCH) * per_blk
        which = lax.shift_right_arithmetic(jnp.sum(n_units - spare), (UCH * per_blk).bit_length() - 1)
        branches = [functools.partial(attend, n, i, head_dim ** -0.5) for i, n in enumerate(UP_SIZES)]
        attn = lax.switch(which, branches, positions, qd, vn, k_t, v_t)
        out = tail(len(UP_SIZES), attn, tokens.reshape(16, 8, -1), ln_mlp.reshape(Q, 1, -1), w_out.reshape(heads_local * slice_len, -1), w_gate, w_up, w_down)
        return out, k_new, v_new

    row_spec = P('dp', None)
    head_spec = P(None, 'heads', 'dim')
    cache_spec = P('dp', None, 'heads', 'dim')
    new_spec = P('dp', 'heads', 'dim')
    in_specs = (row_spec, P(None), head_spec, head_spec, head_spec, P('dim'), P('dim'), P('heads', 'dim', None), P(None), P(None, mlp_axes), P(None, mlp_axes), P(mlp_axes, None), cache_spec, cache_spec, P('dp'))
    out_specs = (row_spec, new_spec, new_spec)
    return jax.shard_map(layer_body, mesh=mesh, in_specs=in_specs, out_specs=out_specs, check_vma=False)
```

```python
import functools

import jax
import jax.numpy as jnp
import numpy as np
from jax import lax
from jax.experimental import pallas as pl
from jax.experimental.pallas import tpu as pltpu
from jax.sharding import PartitionSpec as P

EPS = 1e-6
ROPE_BASE = 1000000.0
MESH = pl.DeviceIdType.MESH

BLK = 128
LOW = 512
CH = 4
UCH = 8
UNIT = 16
SLOTS = 4
FIRST = 8
LEAD = 4
UP_FIRST = 232
UP_SIZES = tuple(UP_FIRST + UCH * i for i in range(9)) + (512,)


def qkv_kernel(group, tok_ref, ln_ref, pos_ref, freq_ref, qg_ref, kg_ref, wq_hbm, wk_hbm, wv_hbm, qd_ref, vn_ref, kt_ref, vt_ref,
               hid, wq, wk, wv, own, other, gain_ref, gain_other, wsem, snd, rcv):
    partner = {"dim": 1 - lax.axis_index("dim")}
    rows, depth = tok_ref.shape
    n_q = own.shape[0] - 1
    steps = n_q // 2
    f32, bf16 = jnp.float32, jnp.bfloat16
    half = BLK // 2
    per_step = wq.shape[0] // steps

    def wq_copy(c):
        part = pl.ds(pl.multiple_of(c * per_step, per_step), per_step)
        return pltpu.make_async_copy(wq_hbm.at[part], wq.at[part], wsem.at[c])

    k_load = pltpu.make_async_copy(wk_hbm, wk, wsem.at[steps])
    v_load = pltpu.make_async_copy(wv_hbm, wv, wsem.at[steps + 1])

    def remote(src, dst, i):
        return pltpu.make_async_remote_copy(src_ref=src, dst_ref=dst, send_sem=snd.at[i], recv_sem=rcv.at[i],
                                            device_id=partner, device_id_type=MESH)

    def q_copy(c):
        part = pl.ds(2 * c, 2)
        return remote(own.at[part], other.at[part], c)

    k_copy = remote(own.at[pl.ds(n_q, 1)], other.at[pl.ds(n_q, 1)], steps)
    g_copy = remote(gain_ref, gain_other, steps + 1)

    k_load.start()
    for c in range(steps):
        wq_copy(c).start()
    v_load.start()
    barrier = pltpu.get_barrier_semaphore()
    pl.semaphore_signal(barrier, inc=1, device_id=partner, device_id_type=MESH)
    gain_ref[...] = jnp.zeros_like(gain_ref)
    for row, ref in enumerate((qg_ref, kg_ref)):
        gain_ref[row:row + 1, :half] = ref[...]
        gain_ref[row:row + 1, half:] = ref[...]
    pl.semaphore_wait(barrier, 1)

    @pl.loop(0, rows // 16, unroll=4)
    def _(i):
        part = pl.ds(pl.multiple_of(i * 16, 16), 16)
        x = tok_ref[part, :].astype(f32)
        inv = lax.rsqrt(jnp.mean(x * x, axis=-1, keepdims=True) + EPS)
        hid[part, :] = (x * inv * ln_ref[...]).astype(bf16)

    def project(w):
        return lax.dot_general(hid[...], w, (((1,), (1,)), ((), ())), preferred_element_type=f32)

    g_copy.start()
    k_load.wait()
    own[n_q] = project(wk[...])
    k_copy.start()

    @pl.loop(0, steps)
    def _(c):
        wq_copy(c).wait()
        u = project(wq[pl.ds(pl.multiple_of(c * per_step, per_step), per_step), :])

        own[2 * c] = u[:, :BLK]
        own[2 * c + 1] = u[:, BLK:]
        q_copy(c).start()

    v_load.wait()
    v_row = project(wv[...]).astype(bf16).astype(f32)
    vn_ref[...] = v_row
    vt_ref[...] = v_row.T.astype(bf16)
    low = lax.broadcasted_iota(jnp.int32, (rows, BLK), 1) < half
    angle = jnp.broadcast_to(pos_ref[...].astype(f32), (rows, rows)).T * freq_ref[...]
    cos_t = jnp.cos(angle)
    sin_t = jnp.sin(angle) * jnp.where(lax.axis_index("dim") == 0, -1.0, 1.0)

    def halves(x):
        return (jnp.sum(jnp.where(low, x, 0.0), axis=-1, keepdims=True), jnp.sum(jnp.where(low, 0.0, x), axis=-1, keepdims=True))

    def rotate(i, g):
        a, b = own[i], other[i]
        s_lo, s_hi = halves(a * a + b * b)
        inv = jnp.where(low, lax.rsqrt(s_lo / BLK + EPS), lax.rsqrt(s_hi / BLK + EPS))
        a, b = a * inv * gain_ref[g:g + 1, :], b * inv * gain_other[g:g + 1, :]
        return (a * cos_t + b * sin_t).astype(bf16).astype(f32), (b * cos_t - a * sin_t).astype(bf16).astype(f32)

    g_copy.wait_recv()
    k_copy.wait_recv()
    k_own, k_oth = rotate(n_q, 1)
    kt_ref[...] = k_own.T.astype(bf16)
    kr_own, kr_oth = pltpu.roll(k_own, half, 1), pltpu.roll(k_oth, half, 1)
    kk = [(jnp.where(low, k_own, kr_own), jnp.where(low, k_oth, kr_oth)),
          (jnp.where(low, kr_own, k_own), jnp.where(low, kr_oth, k_oth))]
    for i in range(n_q):
        if i % 2 == 0:
            q_copy(i // 2).wait_recv()
        q_own, q_oth = rotate(i, 0)
        kv = 2 * i // group
        new = halves(q_own * kk[kv][0] + q_oth * kk[kv][1])
        turned = pltpu.roll(q_own, half, 1)
        for e in range(2):
            row = i + n_q * e
            val = q_own if e == kv else turned
            qd_ref[:, row, :] = jnp.where(low, val, new[e]) if kv == 0 else jnp.where(low, new[e], val)
    for c in range(steps):
        q_copy(c).wait_send()
    k_copy.wait_send()
    g_copy.wait_send()


def qkv(cid, group, tokens, ln, pos, freq, q_gain, k_gain, w_q, w_k, w_v):
    rows, depth = tokens.shape
    n_q = w_q.shape[0] // BLK
    steps = n_q // 2
    vmem = pl.BlockSpec(memory_space=pltpu.VMEM)
    hbm = pl.BlockSpec(memory_space=pl.ANY)
    f32, bf16 = jnp.float32, jnp.bfloat16
    heads = 2 * n_q
    dma = pltpu.SemaphoreType.DMA
    return pl.pallas_call(
        functools.partial(qkv_kernel, group),
        out_shape=(jax.ShapeDtypeStruct((rows, heads, BLK), f32), jax.ShapeDtypeStruct((rows, BLK), f32), jax.ShapeDtypeStruct((BLK, rows), bf16), jax.ShapeDtypeStruct((BLK, rows), bf16)),
        in_specs=[vmem] * 6 + [hbm] * 3,
        out_specs=(vmem,) * 4,
        scratch_shapes=[
            pltpu.VMEM((rows, depth), bf16),
            pltpu.VMEM(w_q.shape, bf16),
            pltpu.VMEM(w_k.shape, bf16),
            pltpu.VMEM(w_v.shape, bf16),
            pltpu.VMEM((n_q + 1, rows, BLK), f32),
            pltpu.VMEM((n_q + 1, rows, BLK), f32),
            pltpu.VMEM((8, BLK), f32),
            pltpu.VMEM((8, BLK), f32),
            dma((steps + 2,)), dma((steps + 2,)), dma((steps + 2,)),
        ],
        compiler_params=pltpu.CompilerParams(collective_id=cid, has_side_effects=True, vmem_limit_bytes=62 * 1024 * 1024),
        name="qkv",
    )(tokens, ln, pos, freq, q_gain, k_gain, w_q, w_k, w_v)


def attn_kernel(n_up, scale, pos_ref, qd_ref, vn_ref, k_hbm, v_hbm, o_ref,
                off_ref, kbuf, vbuf, own_lo, own_up, pack, rlo, rup, ksem, vsem, send, slo_r, sup_r):
    partner = {"dim": 1 - lax.axis_index("dim")}
    rows = qd_ref.shape[0]
    n_ch = rows // CH
    n_uch = n_up // UCH
    up_blocks = own_up.shape[0] // rows
    per_blk = BLK // UNIT
    lane_up = lax.broadcasted_iota(jnp.int32, (16, BLK), 1)
    kv_row = lax.broadcasted_iota(jnp.int32, (16, BLK), 0) // 4 % 2
    q_lanes = kv_row == lane_up // 64

    def kcopy(c):
        return pltpu.make_async_copy(k_hbm.at[pl.ds(c * CH, CH)], kbuf.at[lax.rem(c, SLOTS)], ksem.at[lax.rem(c, SLOTS)])

    def vcopy(c):
        return pltpu.make_async_copy(v_hbm.at[pl.ds(c * CH, CH)], vbuf.at[lax.rem(c, SLOTS)], vsem.at[lax.rem(c, SLOTS)])

    def lo_copy(c):
        part = pl.ds(c * CH, CH)
        return pltpu.make_async_remote_copy(src_ref=own_lo.at[part], dst_ref=rlo.at[part], send_sem=send.at[0],
                                            recv_sem=slo_r.at[c], device_id=partner, device_id_type=MESH)

    def up_copy(c):
        part = pl.ds(c * UCH, UCH)
        return pltpu.make_async_remote_copy(src_ref=pack.at[part], dst_ref=rup.at[part], send_sem=send.at[1],
                                            recv_sem=sup_r.at[c], device_id=partner, device_id_type=MESH)

    kcopy(0).start()
    barrier = pltpu.get_barrier_semaphore()
    pl.semaphore_signal(barrier, inc=1, device_id=partner, device_id_type=MESH)
    pl.semaphore_wait(barrier, 1)
    for c in range(1, SLOTS):
        kcopy(c).start()
    row_units = up_blocks * per_blk

    @pl.loop(0, n_ch)
    def _(c):
        @pl.when((c >= 1) & (c <= FIRST))
        def _():
            lo_copy(c - 1).start()

        kcopy(c).wait()
        for r in range(CH):
            b = c * CH + r
            s = jnp.dot(jnp.where(q_lanes, qd_ref[b], 0.0).astype(jnp.bfloat16), kbuf[lax.rem(c, SLOTS), r], preferred_element_type=jnp.float32)
            own_lo[b] = s[:, :LOW]
            for j in range(up_blocks):
                own_up[b * up_blocks + j] = s[:, LOW + j * BLK:LOW + (j + 1) * BLK]

        @pl.when(c + SLOTS < n_ch)
        def _():
            kcopy(c + SLOTS).start()

    for c in range(SLOTS):
        vcopy(c).start()

    def place(b, total):
        off_ref[b] = total
        return total + jnp.maximum((pos_ref[b] - LOW + UNIT - 1) // UNIT, 1)

    lax.fori_loop(0, rows, place, jnp.int32(0))

    def fill(c, row):
        for r in range(UCH):
            j = c * UCH + r
            block = None
            for k in range(per_blk):
                unit = j * per_blk + k
                following = jnp.minimum(row + 1, rows - 1)
                row = jnp.where(unit >= off_ref[following], following, row)
                src = jnp.minimum(unit - off_ref[row], row_units - 1)
                piece = pltpu.roll(own_up[row * up_blocks + src // per_blk], (k + per_blk - src % per_blk) % per_blk * UNIT, 1)
                block = piece if k == 0 else jnp.where(lane_up >= k * UNIT, piece, block)
            pack[j] = block

        @pl.when(c >= 1)
        def _():
            up_copy(c - 1).start()
        return row

    lax.fori_loop(0, n_uch, fill, jnp.int32(0))
    up_copy(n_uch - 1).start()

    @pl.loop(FIRST, FIRST + LEAD)
    def _(c):
        lo_copy(c).start()

    @pl.loop(0, n_uch)
    def _(c):
        up_copy(c).wait_recv()

    lane = lax.broadcasted_iota(jnp.int32, (8, 2 * 64), 1)
    first = lax.broadcasted_iota(jnp.int32, (8, 2 * 64), 0) < 4
    t_up = lane_up + LOW

    @pl.loop(0, n_ch)
    def _(c):
        @pl.when(c + FIRST + LEAD < n_ch)
        def _():
            lo_copy(c + FIRST + LEAD).start()

        vcopy(c).wait()
        lo_copy(c).wait_recv()
        for r in range(CH):
            b = c * CH + r
            pos = pos_ref[b]
            off = off_ref[b]
            parts = [(own_lo[b] + rlo[b]) * scale]
            skew = off % per_blk * UNIT
            slots = [pltpu.roll(rup[jnp.minimum(off // per_blk + j, n_up - 1)], (BLK - skew) % BLK, 1) for j in range(up_blocks + 1)]
            for j in range(up_blocks):
                got = jnp.where(lane_up < BLK - skew, slots[j], slots[j + 1])
                total = (own_up[b * up_blocks + j] + got) * scale
                parts.append(jnp.where(t_up + j * BLK < pos, total, -jnp.inf))
            s = jnp.concatenate(parts, axis=1)
            q_row = qd_ref[b]
            s_new = jnp.where(kv_row[:, 0:1] == 0, q_row[:, BLK - 1:], q_row[:, 0:1]) * scale
            m = jnp.maximum(jnp.max(s, axis=1, keepdims=True), s_new)
            e = jnp.exp(s - m)
            e_new = jnp.exp(s_new - m)
            inv = 1.0 / (jnp.sum(e, axis=1, keepdims=True) + e_new)
            p = (e * inv).astype(jnp.bfloat16)
            p_new = (e_new * inv).astype(jnp.bfloat16).astype(jnp.float32)
            o = lax.dot_general(p, vbuf[lax.rem(c, SLOTS), r], (((1,), (1,)), ((), ())), preferred_element_type=jnp.float32)
            o = o + p_new * vn_ref[pl.ds(b, 1), :]
            even, odd = o[0:8], o[8:16]
            o_ref[b] = jnp.where(lane < 64, jnp.where(first, even, pltpu.roll(even, 64, 1)), jnp.where(first, pltpu.roll(odd, 64, 1), odd))

        @pl.when(c + SLOTS < n_ch)
        def _():
            vcopy(c + SLOTS).start()

    pltpu.make_async_remote_copy(src_ref=own_lo, dst_ref=rlo, send_sem=send.at[0], recv_sem=slo_r.at[0],
                                 device_id=partner, device_id_type=MESH).wait_send()
    pltpu.make_async_remote_copy(src_ref=pack, dst_ref=rup, send_sem=send.at[1], recv_sem=sup_r.at[0],
                                 device_id=partner, device_id_type=MESH).wait_send()


def attend(n_up, cid, scale, pos, qd, vn, k_t, v_t):
    rows = qd.shape[0]
    n_ch = rows // CH
    n_uch = n_up // UCH
    cache_len = k_t.shape[2]
    up_blocks = (cache_len - LOW) // BLK
    smem = pl.BlockSpec(memory_space=pltpu.SMEM)
    vmem = pl.BlockSpec(memory_space=pltpu.VMEM)
    hbm = pl.BlockSpec(memory_space=pl.ANY)
    return pl.pallas_call(
        functools.partial(attn_kernel, n_up, scale),
        out_shape=jax.ShapeDtypeStruct((rows, 8, 128), jnp.float32),
        in_specs=[smem, vmem, vmem, hbm, hbm],
        out_specs=vmem,
        scratch_shapes=[
            pltpu.SMEM((rows,), jnp.int32),
            pltpu.VMEM((SLOTS, CH, 128, cache_len), jnp.bfloat16),
            pltpu.VMEM((SLOTS, CH, 128, cache_len), jnp.bfloat16),
            pltpu.VMEM((rows, 16, LOW), jnp.float32),
            pltpu.VMEM((rows * up_blocks, 16, BLK), jnp.float32),
            pltpu.VMEM((n_up, 16, BLK), jnp.float32),
            pltpu.VMEM((rows, 16, LOW), jnp.float32),
            pltpu.VMEM((n_up, 16, BLK), jnp.float32),
            pltpu.SemaphoreType.DMA((SLOTS,)),
            pltpu.SemaphoreType.DMA((SLOTS,)),
            pltpu.SemaphoreType.DMA((2,)),
            pltpu.SemaphoreType.DMA((n_ch,)),
            pltpu.SemaphoreType.DMA((n_uch,)),
        ],
        compiler_params=pltpu.CompilerParams(collective_id=cid, has_side_effects=True, vmem_limit_bytes=40 * 1024 * 1024),
        name=f"attend_{n_up}",
    )(pos, qd, vn, k_t, v_t)


Q = 10
REDUCE_LAGS = ((3, 6, 6), (2, 5, 6))
GATHER_LAGS = ((4, 3, 2), (6, 4, 2))
PARTS = 4
WO_SLOTS = 3
GU_SLOTS = 5
WD_SLOTS = 4


def tail_kernel(attn_ref, tok_hbm, ln_ref, wo_hbm, wg_hbm, wu_hbm, wd_hbm, out_ref,
                x_ref, tok_ref, part, r1, r2, r3, full, xres, acc_g, acc_u, mact, wo, wg, wu, wd,
                tok_s, wo_s, wg_s, wu_s, wd_s, snd, rcv):
    heads = lax.axis_index("heads")
    core, cx, cy = lax.rem(heads, 2), heads // 2, lax.axis_index("dim")
    sib = {"heads": 2 * cx + 1 - core}
    xn = {"heads": 2 * (1 - cx) + core}
    yn = {"dim": 1 - cy}
    width = part.shape[3]
    rows = 16 * 8
    f32 = jnp.float32

    def cols(q):
        return pl.ds(pl.multiple_of(q * width, width), width)

    def wo_copy(q):
        s = lax.rem(q, WO_SLOTS)
        return [pltpu.make_async_copy(wo_hbm.at[:, cols(q)], wo.at[s], wo_s.at[s])]

    def gu_copy(q):
        s = lax.rem(q, GU_SLOTS)
        return [pltpu.make_async_copy(wg_hbm.at[cols(q)], wg.at[s], wg_s.at[s]),
                pltpu.make_async_copy(wu_hbm.at[cols(q)], wu.at[s], wu_s.at[s])]

    def wd_copy(q):
        s = lax.rem(q, WD_SLOTS)
        return [pltpu.make_async_copy(wd_hbm.at[:, cols(q)], wd.at[s], wd_s.at[s])]

    def start(copies):
        for cp in copies:
            cp.start()

    def wait(copies):
        for cp in copies:
            cp.wait()

    def remote(ph, st, q, src, dst, dev):
        return pltpu.make_async_remote_copy(src_ref=src, dst_ref=dst, send_sem=snd.at[ph, st], recv_sem=rcv.at[ph, st, q],
                                            device_id=dev, device_id_type=MESH)

    def stage(ph, k, q, sem_q):
        if k == 0:
            return [remote(ph, 0, sem_q, part.at[q, pl.ds(8 * (1 - core), 8)], r1.at[q], sib)]
        if k == 1:
            return [remote(ph, 1, sem_q, r1.at[q, pl.ds(2 * (1 - cx), 2)], r2.at[q, pl.ds(0, 2)], xn),
                    remote(ph, 2, sem_q, r1.at[q, pl.ds(4 + 2 * (1 - cy), 2)], r2.at[q, pl.ds(2, 2)], yn)]
        if k == 2:
            return [remote(ph, 3, sem_q, r2.at[q, pl.ds(1 - cy, 1)], r3.at[q, pl.ds(0, 1)], yn),
                    remote(ph, 4, sem_q, r2.at[q, pl.ds(2 + 1 - cx, 1)], r3.at[q, pl.ds(1, 1)], xn)]
        blk_a, blk_b = core * 8, core * 8 + 4
        if k == 3:
            a, b = full.at[q, pl.ds(blk_a + 2 * cx + cy, 1)], full.at[q, pl.ds(blk_b + 2 * cy + cx, 1)]
            return [remote(ph, 5, sem_q, a, a, yn), remote(ph, 6, sem_q, b, b, xn)]
        if k == 4:
            a, b = full.at[q, pl.ds(blk_a + 2 * cx, 2)], full.at[q, pl.ds(blk_b + 2 * cy, 2)]
            return [remote(ph, 7, sem_q, a, a, xn), remote(ph, 8, sem_q, b, b, yn)]
        a = full.at[q, pl.ds(blk_a, 8)]
        return [remote(ph, 9, sem_q, a, a, sib)]

    def one(ph, k, q):
        return stage(ph, k, q, q)

    def drain(ph, ks):
        for k in ks:
            for cp in stage(ph, k, slice(None), 0):
                cp.wait_send()

    def arrived(ph, k, q):
        for cp in one(ph, k, q):
            cp.wait_recv()

    def when(t, lo):
        return pl.when((t >= lo) & (t < lo + Q))

    def reduce_steps(ph, t, finish):
        first, second, third = np.cumsum(REDUCE_LAGS[ph]).tolist()

        @when(t, first)
        def _():
            u = t - first
            arrived(ph, 0, u)
            r1[u] = r1[u] + part[u, pl.ds(8 * core, 8)]
            start(one(ph, 1, u))

        @when(t, 0)
        def _():
            start(one(ph, 0, t))

        @when(t, second)
        def _():
            u = t - second
            arrived(ph, 1, u)
            r2[u, pl.ds(0, 2)] = r2[u, pl.ds(0, 2)] + r1[u, pl.ds(2 * cx, 2)]
            r2[u, pl.ds(2, 2)] = r2[u, pl.ds(2, 2)] + r1[u, pl.ds(4 + 2 * cy, 2)]
            start(one(ph, 2, u))

        @when(t, third)
        def _():
            u = t - third
            arrived(ph, 2, u)
            finish(u, r3[u, 0] + r2[u, cy], r3[u, 1] + r2[u, 2 + cx])

    def gather_start(ph, t):
        @when(t, 0)
        def _():
            start(one(ph, 3, t))

    def gather_steps(ph, t, finish):
        first, second, third = np.cumsum(GATHER_LAGS[ph]).tolist()

        @when(t, first)
        def _():
            arrived(ph, 3, t - first)
            start(one(ph, 4, t - first))

        @when(t, second)
        def _():
            arrived(ph, 4, t - second)
            start(one(ph, 5, t - second))

        @when(t, third)
        def _():
            arrived(ph, 5, t - third)
            finish(t - third)

    blk_a, blk_b = core * 8 + 2 * cx + cy, core * 8 + 4 + 2 * cy + cx
    tok_loads = [pltpu.make_async_copy(tok_hbm.at[blk], tok_ref.at[i], tok_s.at[i]) for i, blk in enumerate((blk_a, blk_b))]
    for q in range(WO_SLOTS):
        start(wo_copy(q))
    start(tok_loads)
    barrier = pltpu.get_barrier_semaphore()
    for dev in (sib, xn, yn):
        pl.semaphore_signal(barrier, inc=1, device_id=dev, device_id_type=MESH)
    acc_g[...] = jnp.zeros_like(acc_g)
    acc_u[...] = jnp.zeros_like(acc_u)
    for i in range(attn_ref.shape[1]):
        x_ref[:, i * BLK:(i + 1) * BLK] = attn_ref[:, i, :].astype(jnp.bfloat16)
    wait(tok_loads)
    pl.semaphore_wait(barrier, 3)
    def finish_attn(u, a, b):
        xres[u, 0] = (tok_ref[0, :, cols(u)].astype(f32) + a).astype(jnp.bfloat16).astype(f32)
        xres[u, 1] = (tok_ref[1, :, cols(u)].astype(f32) + b).astype(jnp.bfloat16).astype(f32)

    @pl.loop(0, Q + sum(REDUCE_LAGS[0]))
    def _(t):
        @when(t, 0)
        def _():
            wait(wo_copy(t))
            part[t] = jnp.dot(x_ref[...], wo[lax.rem(t, WO_SLOTS)], preferred_element_type=f32).reshape(16, 8, width)

            @pl.when(t + WO_SLOTS < Q)
            def _():
                start(wo_copy(t + WO_SLOTS))

        @pl.when((t >= WO_SLOTS) & (t < WO_SLOTS + GU_SLOTS))
        def _():
            start(gu_copy(t - WO_SLOTS))

        @pl.when((t >= WO_SLOTS + GU_SLOTS) & (t < WO_SLOTS + GU_SLOTS + WD_SLOTS))
        def _():
            start(wd_copy(t - WO_SLOTS - GU_SLOTS))

        reduce_steps(0, t, finish_attn)

    drain(0, (0, 1, 2))
    sq = jnp.zeros((2, 8, 1), f32)
    for q in range(Q):
        sq = sq + jnp.sum(xres[q] * xres[q], axis=-1, keepdims=True)
    inv = lax.rsqrt(sq / (Q * width) + EPS)
    for q in range(Q):
        h = (xres[q] * inv * ln_ref[q]).astype(jnp.bfloat16).astype(f32)
        full[q, blk_a] = h[0]
        full[q, blk_b] = h[1]

    def finish_gather(u):
        wait(gu_copy(u))
        s = lax.rem(u, GU_SLOTS)
        h = full[u].reshape(rows, width).astype(jnp.bfloat16)
        acc_g[...] += jnp.dot(h, wg[s], preferred_element_type=f32)
        acc_u[...] += jnp.dot(h, wu[s], preferred_element_type=f32)

        @pl.when(u + GU_SLOTS < Q)
        def _():
            start(gu_copy(u + GU_SLOTS))

    @pl.loop(0, Q + sum(GATHER_LAGS[0]))
    def _(t):
        gather_start(0, t)
        gather_steps(0, t, finish_gather)

    drain(0, (3, 4, 5))

    @pl.loop(0, acc_g.shape[1] // 640)
    def _(n):
        c = pl.ds(pl.multiple_of(n * 640, 640), 640)
        mact[:, c] = (jax.nn.silu(acc_g[:, c]) * acc_u[:, c]).astype(jnp.bfloat16)

    def finish_mlp(u, a, b):
        full[u, blk_a] = (xres[u, 0] + a).astype(jnp.bfloat16).astype(f32)
        full[u, blk_b] = (xres[u, 1] + b).astype(jnp.bfloat16).astype(f32)

    def finish_out(u):
        out_ref[:, cols(u)] = full[u].reshape(rows, width).astype(jnp.bfloat16)

    lag = 1 + sum(REDUCE_LAGS[1])

    @pl.loop(0, Q + lag + sum(GATHER_LAGS[1]))
    def _(t):
        gather_start(1, t - lag)

        @when(t, 0)
        def _():
            wait(wd_copy(t))
            part[t] = jnp.dot(mact[...], wd[lax.rem(t, WD_SLOTS)], preferred_element_type=f32).reshape(16, 8, width)

            @pl.when(t + WD_SLOTS < Q)
            def _():
                start(wd_copy(t + WD_SLOTS))
        reduce_steps(1, t, finish_mlp)
        gather_steps(1, t - lag, finish_out)

    drain(1, (0, 1, 2, 3, 4, 5))


def tail(cid, attn, tok_blocks, ln, w_out, w_gate, w_up, w_down):
    rows = attn.shape[0]
    depth = w_out.shape[0]
    d_model, inner = w_gate.shape
    width = d_model // Q
    vmem = pl.BlockSpec(memory_space=pltpu.VMEM)
    hbm = pl.BlockSpec(memory_space=pl.ANY)
    f32, bf16 = jnp.float32, jnp.bfloat16
    dma = pltpu.SemaphoreType.DMA
    return pl.pallas_call(
        tail_kernel,
        out_shape=jax.ShapeDtypeStruct((rows, d_model), bf16),
        in_specs=[vmem, hbm, vmem, hbm, hbm, hbm, hbm],
        out_specs=vmem,
        scratch_shapes=[
            pltpu.VMEM((rows, depth), bf16),
            pltpu.VMEM((2, 8, d_model), bf16),
            pltpu.VMEM((Q, 16, 8, width), f32),
            pltpu.VMEM((Q, 8, 8, width), f32),
            pltpu.VMEM((Q, 4, 8, width), f32),
            pltpu.VMEM((Q, 2, 8, width), f32),
            pltpu.VMEM((Q, 16, 8, width), f32),
            pltpu.VMEM((Q, 2, 8, width), f32),
            pltpu.VMEM((rows, inner), f32),
            pltpu.VMEM((rows, inner), f32),
            pltpu.VMEM((rows, inner), bf16),
            pltpu.VMEM((WO_SLOTS, depth, width), bf16),
            pltpu.VMEM((GU_SLOTS, width, inner), bf16),
            pltpu.VMEM((GU_SLOTS, width, inner), bf16),
            pltpu.VMEM((WD_SLOTS, inner, width), bf16),
            dma((2,)), dma((WO_SLOTS,)), dma((GU_SLOTS,)), dma((GU_SLOTS,)), dma((WD_SLOTS,)),
            dma((2, 10)), dma((2, 10, Q)),
        ],
        compiler_params=pltpu.CompilerParams(collective_id=cid, has_side_effects=True, vmem_limit_bytes=62 * 1024 * 1024),
        name="tail",
    )(attn, tok_blocks, ln, w_out, w_gate, w_up, w_down)


def place_kernel(out_hbm, k_hbm, v_hbm, out_dst, k_dst, v_dst, out_buf, k_buf, v_buf, sem_in, sem_out):
    rows = out_hbm.shape[0] // PARTS
    moves = [(k_hbm, k_buf, k_dst), (v_hbm, v_buf, v_dst)]
    for i in range(PARTS):
        part = pl.ds(i * rows, rows)
        moves.append((out_hbm.at[part], out_buf.at[part], out_dst.at[part]))
    loads = [pltpu.make_async_copy(src, buf, sem_in.at[i]) for i, (src, buf, dst) in enumerate(moves)]
    stores = [pltpu.make_async_copy(buf, dst, sem_out.at[i]) for i, (src, buf, dst) in enumerate(moves)]
    for load in loads:
        load.start()
    for load, store in zip(loads, stores):
        load.wait()
        store.start()
    for store in stores:
        store.wait()


def place_results(out, k_t, v_t):
    hbm = pl.BlockSpec(memory_space=pl.ANY)
    arrays = (out, k_t, v_t)
    return pl.pallas_call(
        place_kernel,
        out_shape=tuple(jax.ShapeDtypeStruct(x.shape, x.dtype) for x in arrays),
        in_specs=[hbm] * 3,
        out_specs=(hbm,) * 3,
        scratch_shapes=[pltpu.VMEM(x.shape, x.dtype) for x in arrays] + [pltpu.SemaphoreType.DMA((PARTS + 2,))] * 2,
        name="place",
    )(*arrays)


def solution(mesh):
    dim_count = mesh.shape['dim']
    mlp_axes = ('heads', 'dim')

    def layer_body(tokens, ln_attn, w_query, w_key, w_value, q_gain, k_gain, w_out, ln_mlp, w_gate, w_up, w_down, k_cache, v_cache, positions):
        rows = tokens.shape[0]
        heads_local = w_query.shape[1]
        kv_local = w_key.shape[1]
        slice_len = w_query.shape[2]
        head_dim = slice_len * dim_count
        half_dim = head_dim // 2
        q_group = heads_local // kv_local
        cache_len = k_cache.shape[1]
        dim_index = lax.axis_index('dim')

        inv_freq = np.tile(ROPE_BASE ** (-np.arange(half_dim) * 2.0 / head_dim), 2).astype(np.float32)

        def by_column(w):
            return w.transpose(1, 2, 0).reshape(-1, w.shape[0])

        qd, vn, kt, vt = qkv(len(UP_SIZES) + 1, q_group, tokens, ln_attn[None], positions[None], inv_freq[None], q_gain[None], k_gain[None],
                             by_column(w_query), by_column(w_key), by_column(w_value))
        n_units = jnp.maximum((positions - LOW + UNIT - 1) // UNIT, 1)
        per_blk = BLK // UNIT
        k_t = k_cache.transpose(0, 2, 3, 1).reshape(rows, kv_local * slice_len, cache_len)
        v_t = v_cache.transpose(0, 2, 3, 1).reshape(rows, kv_local * slice_len, cache_len)
        spare = (UP_FIRST - UCH) * per_blk // rows
        assert spare * rows == (UP_FIRST - UCH) * per_blk
        which = lax.shift_right_arithmetic(jnp.sum(n_units - spare), (UCH * per_blk).bit_length() - 1)
        branches = [functools.partial(attend, n, i, head_dim ** -0.5) for i, n in enumerate(UP_SIZES)]
        attn = lax.switch(which, branches, positions, qd, vn, k_t, v_t)
        out = tail(len(UP_SIZES), attn, tokens.reshape(16, 8, -1), ln_mlp.reshape(Q, 1, -1), w_out.reshape(heads_local * slice_len, -1), w_gate, w_up, w_down)
        out, kt, vt = place_results(out, kt, vt)
        k_new = kt.reshape(kv_local, slice_len, rows).transpose(2, 0, 1)
        v_new = vt.reshape(kv_local, slice_len, rows).transpose(2, 0, 1)
        return out, k_new, v_new

    row_spec = P('dp', None)
    head_spec = P(None, 'heads', 'dim')
    cache_spec = P('dp', None, 'heads', 'dim')
    new_spec = P('dp', 'heads', 'dim')
    in_specs = (row_spec, P(None), head_spec, head_spec, head_spec, P('dim'), P('dim'), P('heads', 'dim', None), P(None), P(None, mlp_axes), P(None, mlp_axes), P(mlp_axes, None), cache_spec, cache_spec, P('dp'))
    out_specs = (row_spec, new_spec, new_spec)
    return jax.shard_map(layer_body, mesh=mesh, in_specs=in_specs, out_specs=out_specs, check_vma=False)
```
